32 devices in a mesh: expert: 4 (over y, x), shard: 8 (over z, core).
Axes of the slice: x: 2, y: 2, z: 4, core: 2. Of those that a mesh axis runs over, the one named last changes fastest.
Arguments:
- inputs: bfloat16 [4096, 1536], P(('expert', 'shard')), may hold values from -6 to 6
- cotangent: bfloat16 [4096, 1536], P(('expert', 'shard')), may hold values from -6 to 6
- routes: int32 [4096, 8], P(('expert', 'shard')), may hold values from 0 to 39, all different within a row; in each aligned block of 128 rows (0 to 127, 128 to 255, ...) at most 38 rows name the same one
- attn_gain: bfloat16 [1536], P('shard'), may hold values from 0.5 to 1.5
- w_query: bfloat16 [1536, 1536], P('shard'), may hold values from -0.22963966 to 0.22963966
- key_matrix: bfloat16 [1536, 512], P('shard'), may hold values from -0.22963966 to 0.22963966
- value_matrix: bfloat16 [1536, 512], P('shard'), may hold values from -0.15625 to 0.15625
- w_output: bfloat16 [1536, 1536], P('shard'), may hold values from -2.5 to 2.5
- moe_gain: bfloat16 [1536], P('shard'), may hold values from 0.5 to 1.5
- w_router: bfloat16 [1536, 40], P('shard'), may hold values from -0.38273277 to 0.38273277
- w_experts: bfloat16 [1536, 40, 1536], P('shard', 'expert'), may hold values from -0.25 to 0.25
Outputs:
- outputs: bfloat16 [4096, 1536], P(('expert', 'shard'))
- grad_inputs: float32 [4096, 1536], P(('expert', 'shard'))
- grad_attn_gain: float32 [1536], P('shard')
- grad_w_query: float32 [1536, 1536], P('shard')
- grad_w_key: float32 [1536, 512], P('shard')
- grad_w_value: float32 [1536, 512], P('shard')
- grad_w_output: float32 [1536, 1536], P('shard')
- grad_moe_gain: float32 [1536], P('shard')
- grad_w_router: float32 [1536, 40], P('shard')
- grad_w_experts: float32 [1536, 40, 1536], P('shard', 'expert')
The draws below stay inside these ranges and needn't reach their ends.
Inputs may be any that keep to these rules, and one draw needn't show every extreme that they name: `routes`: each token names 8 different experts. Among the 128 tokens of one device at most 38 name the same expert, and 38 is reached. Every expert is named by some token.
All inputs are finite; a program needn't handle non-finite values.
Results may differ from the reference program's by a relative error of at most 0.028.
Values may be sent and summed in bfloat16 or wider, within the bound.
A program may use at most 320 MiB of HBM per device.

```python
import math
import jax
import jax.numpy as jnp
import numpy as np
from jax import lax

MODEL_WIDTH = 1536
QUERY_HEADS = 24
KEY_VALUE_HEADS = 8
HEAD_SIZE = 64
FF = 512
E = 40
TOP = 8
DEVICE_TOKENS = 64
TOK_DEV = 128
CAP = 38
SEQ_LEN = 512
TOKENS = 4096
N_SHARD = 8


def weight_drawn(key, salt, heads):
    base_draw = jax.random.truncated_normal(jax.random.fold_in(key, salt), -6.0, 6.0, (MODEL_WIDTH, heads * HEAD_SIZE), jnp.float32) * MODEL_WIDTH ** (-0.5)
    return base_draw.astype(jnp.bfloat16)


def draw_inputs(key, part):
    noise_rows = jax.random.truncated_normal(jax.random.fold_in(key, 11), -6.0, 6.0, (TOKENS, MODEL_WIDTH), jnp.float32)
    return noise_rows.astype(jnp.bfloat16)


def draw_w_query(key, part):
    return weight_drawn(key, 21, QUERY_HEADS)


def draw_key_matrix(key, part):
    return weight_drawn(key, 22, KEY_VALUE_HEADS)


def draw_w_router(key, part):
    base_draw = jax.random.truncated_normal(jax.random.fold_in(key, 41), -6.0, 6.0, (MODEL_WIDTH, E), jnp.float32) * MODEL_WIDTH ** (-0.5)
    return base_draw.astype(jnp.bfloat16)


def steps_of(key, dims, shards, low, high):
    factor_of = 1.0
    for dim, shards_of in shards:
        draws = jax.random.uniform(jax.random.fold_in(jax.random.fold_in(key, 6), dim), (shards_of,), jnp.float32, low / len(shards), high / len(shards))
        factor_of = factor_of * jnp.repeat(jnp.exp(draws), dims[dim] // shards_of).reshape((-1,) + (1,) * (len(dims) - 1 - dim))
    return factor_of


def shared_out(stream_key, own, number, rows, number_of, top, bound, skew):
    order = jax.random.permutation(stream_key, number_of)
    heavy_load, common = portions_of(number_of, rows * top, bound, skew, True), portions_of(number_of, rows * top, bound, skew, False)
    places = jnp.arange(number_of)

    def named(lengths, rotation):
        used = int((lengths > 0).sum())
        fixed = max(1, used // 4)
        passed = fixed + (places - fixed + rotation * (used - fixed)) % max(1, number_of - fixed)
        return jnp.zeros((number_of,), jnp.int32).at[order[jnp.where(places < fixed, places, passed)]].set(jnp.asarray(lengths, jnp.int32))

    lengths = jnp.where(number % 4 == 0, named(heavy_load, number // 4), named(common, number - number // 4 - 1))
    mixed = jax.random.permutation(jax.random.fold_in(own, 3), number_of)
    source_of, sink = mixed[0:number_of // 2 * 2:2], mixed[1:number_of // 2 * 2:2]
    slack = jnp.minimum(lengths[source_of] - 1, bound - lengths[sink]) // 2
    slack = jnp.where((source_of == order[0]) | (sink == order[0]) | (lengths[sink] == 0), 0, jnp.maximum(slack, 0))
    passed = jax.random.randint(jax.random.fold_in(own, 4), (number_of // 2,), 0, 1 << 20) % (slack + 1)
    lengths = lengths.at[source_of].add(-passed).at[sink].add(passed)
    items = jnp.searchsorted(jnp.cumsum(lengths), jnp.arange(rows * top), side="right").astype(jnp.int32)
    table = items.reshape(top, rows).T
    table = table[jax.random.permutation(jax.random.fold_in(own, 1), rows)]
    rotation = jax.random.randint(jax.random.fold_in(own, 2), (rows, 1), 0, top)
    return jnp.take_along_axis(table, (jnp.arange(top)[None, :] + rotation) % top, axis=1)


def portions_of(number_of, total, most, slope, full):
    loads = [(1 << 20) // math.isqrt(standing ** slope) + 1 for standing in range(1, number_of + 1)]
    largest = most if full else min(most, max(-(-total // number_of), total * loads[0] // sum(loads)))
    least = 1 if total - largest >= number_of - 1 else 0
    given, surplus = [largest] + [least] * (number_of - 1), total - largest - least * (number_of - 1)
    while surplus > 0:
        movable = [i for i in range(1, number_of) if given[i] < largest] or [i for i in range(1, number_of) if given[i] < most]
        pool, remaining = sum([loads[i] for i in movable]), surplus
        for i in movable:
            more = min(most - given[i], max(1, remaining * loads[i] // pool), surplus)
            given[i] = given[i] + more
            surplus = surplus - more
    return np.array(given)


def normal_values(key, extent, deviation, limit, pieces=(), kind=jnp.bfloat16):
    level = steps_of(key, extent, pieces, -0.22, 0.18) if pieces else 1.0
    result = jax.random.normal(key, extent, jnp.float32) * deviation * level
    return jnp.minimum(jnp.maximum(result, -limit), limit).astype(kind)


def setup_inputs(seed: int = 0) -> dict:
    key_of = jax.random.split(jax.random.key(seed), 12)
    inputs = draw_inputs(jax.random.fold_in(key_of[11], 71), 0)
    cotangent = normal_values(key_of[1], (TOKENS, MODEL_WIDTH), 1.0, 6.0, ((0, 32),))
    routes_keys = jax.random.split(jax.random.fold_in(key_of[2], 1), TOKENS // TOK_DEV)
    routes_turns = jax.random.permutation(jax.random.fold_in(key_of[2], 3), TOKENS // TOK_DEV)
    routes = jax.vmap(lambda own, number: shared_out(jax.random.fold_in(key_of[2], 2), own, number, TOK_DEV, E, TOP, CAP, 2))(routes_keys, routes_turns).reshape((TOKENS, TOP))
    attn_gain = jnp.clip(1.0 + 0.1 * jax.random.normal(key_of[3], (MODEL_WIDTH,), jnp.float32), 0.5, 1.5).astype(jnp.bfloat16)
    w_query = draw_w_query(jax.random.fold_in(key_of[11], 71), 0)
    key_matrix = draw_key_matrix(jax.random.fold_in(key_of[11], 71), 0)
    value_matrix = normal_values(key_of[6], (MODEL_WIDTH, KEY_VALUE_HEADS * HEAD_SIZE), MODEL_WIDTH ** -0.5, 0.15625, ((0, 8),))
    w_output = normal_values(key_of[7], (QUERY_HEADS * HEAD_SIZE, MODEL_WIDTH), (max(2 * QUERY_HEADS * HEAD_SIZE // SEQ_LEN, 1)) ** -0.5, 2.5, ((0, 8),))
    moe_gain = jnp.clip(1.0 + 0.1 * jax.random.normal(key_of[8], (MODEL_WIDTH,), jnp.float32), 0.5, 1.5).astype(jnp.bfloat16)
    w_router = draw_w_router(jax.random.fold_in(key_of[11], 71), 0)
    w_experts = normal_values(key_of[10], (MODEL_WIDTH, E, 3 * FF), FF ** -0.5, 0.25, ((0, 8), (1, 4)))
    return {"inputs": inputs, "cotangent": cotangent, "routes": routes, "attn_gain": attn_gain, "w_query": w_query, "key_matrix": key_matrix, "value_matrix": value_matrix, "w_output": w_output, "moe_gain": moe_gain, "w_router": w_router, "w_experts": w_experts}


EPSILON = 1e-06
ROPE_BASE = 10000.0
MASKED = -1e+30

def to_narrow(values):
    return lax.optimization_barrier(values.astype(jnp.bfloat16)).astype(jnp.float32)

def to_sequences(values):
    seqs_here = TOK_DEV // DEVICE_TOKENS
    groups = values.shape[0] // (N_SHARD * TOK_DEV)
    trailing = values.shape[1:]
    shaped = values.reshape((groups, N_SHARD, seqs_here, DEVICE_TOKENS) + trailing)
    axes_order = (0, 2, 1, 3) + tuple(range(4, 4 + len(trailing)))
    return jnp.transpose(shaped, axes_order).reshape((groups * seqs_here, N_SHARD * DEVICE_TOKENS) + trailing)

def gathered_sequences(values):
    seqs_here = TOK_DEV // DEVICE_TOKENS
    groups = values.shape[0] // seqs_here
    trailing = values.shape[2:]
    shaped = values.reshape((groups, seqs_here, N_SHARD, DEVICE_TOKENS) + trailing)
    axes_order = (0, 2, 1, 3) + tuple(range(4, 4 + len(trailing)))
    return jnp.transpose(shaped, axes_order).reshape((groups * N_SHARD * seqs_here * DEVICE_TOKENS,) + trailing)

def angle_tables(positions):
    half_width = HEAD_SIZE // 2
    frequency = jnp.power(ROPE_BASE, -(jnp.arange(half_width, dtype=jnp.float32) * (2.0 / HEAD_SIZE)))
    angles = positions[:, None] * frequency[None, :]
    return (jnp.cos(angles), jnp.sin(angles))

def apply_rotation(values, cosine_table, sines_table):
    half_width = values.shape[-1] // 2
    first_half, second_half = (values[..., :half_width], values[..., half_width:])
    cosine_table, sines_table = (cosine_table[:, None, :], sines_table[:, None, :])
    return jnp.concatenate([first_half * cosine_table - second_half * sines_table, second_half * cosine_table + first_half * sines_table], axis=-1)

def reverse_rotation(values, cosine_table, sines_table):
    half_width = values.shape[-1] // 2
    first_half, second_half = (values[..., :half_width], values[..., half_width:])
    cosine_table, sines_table = (cosine_table[:, None, :], sines_table[:, None, :])
    return jnp.concatenate([first_half * cosine_table + second_half * sines_table, second_half * cosine_table - first_half * sines_table], axis=-1)

def block_scores(queries_block, row_start, keys_in):
    group_width = QUERY_HEADS // KEY_VALUE_HEADS
    rows_of_block = queries_block.shape[0]
    query_four_dims = queries_block.astype(jnp.float32).reshape(rows_of_block, KEY_VALUE_HEADS, group_width, HEAD_SIZE)
    scores = jnp.einsum('qjgd,kjd->jgqk', query_four_dims, keys_in.astype(jnp.float32)) * (1.0 / HEAD_SIZE)
    query_pos = row_start + jnp.arange(rows_of_block, dtype=jnp.int32)
    key_pos = jnp.arange(keys_in.shape[0], dtype=jnp.int32)
    allowed = key_pos[None, :] <= query_pos[:, None]
    return (jnp.where(allowed, scores, MASKED), query_four_dims)

def forward_block(queries_block, row_start, keys_in, values):
    scores, query_four_dims = block_scores(queries_block, row_start, keys_in)
    row_max = lax.optimization_barrier(jnp.max(scores, axis=-1, keepdims=True))
    log_total = row_max + jnp.log(lax.optimization_barrier(jnp.sum(jnp.exp(scores - row_max), axis=-1, keepdims=True)))
    attn_probs = to_narrow(jnp.exp(scores - log_total))
    attention_mixed = jnp.einsum('jgqk,kjd->qjgd', attn_probs, values.astype(jnp.float32))
    return (attention_mixed.reshape(queries_block.shape[0], QUERY_HEADS * HEAD_SIZE).astype(jnp.bfloat16), log_total[..., 0])

def backward_block(queries_block, row_start, log_total, output_gradient, output_block, keys_in, values):
    scores, query_four_dims = block_scores(queries_block, row_start, keys_in)
    rows_of_block = queries_block.shape[0]
    group_width = QUERY_HEADS // KEY_VALUE_HEADS
    attn_probs = jnp.exp(scores - log_total[..., None])
    grad_four_dims = output_gradient.astype(jnp.float32).reshape(rows_of_block, KEY_VALUE_HEADS, group_width, HEAD_SIZE)
    row_difference = lax.optimization_barrier(jnp.sum(grad_four_dims * output_block.astype(jnp.float32).reshape(rows_of_block, KEY_VALUE_HEADS, group_width, HEAD_SIZE), axis=-1))
    row_difference = jnp.transpose(row_difference, (1, 2, 0))
    d_probs = jnp.einsum('qjgd,kjd->jgqk', grad_four_dims, values.astype(jnp.float32))
    dscore = to_narrow(attn_probs * (d_probs - row_difference[..., None]))
    keys_wide = keys_in.astype(jnp.float32)
    dquery = jnp.einsum('jgqk,kjd->qjgd', dscore, keys_wide) * (1.0 / HEAD_SIZE)
    key_gradient = jnp.einsum('jgqk,qjgd->kjd', dscore, query_four_dims) * (1.0 / HEAD_SIZE)
    dvalue = jnp.einsum('jgqk,qjgd->kjd', to_narrow(attn_probs), grad_four_dims)
    return (dquery.reshape(rows_of_block, QUERY_HEADS, HEAD_SIZE), key_gradient, dvalue)

def sequence_forward(qseq, kseq, vseq):
    total_length = qseq.shape[0]
    query_block = min(256, total_length)
    block_count = total_length // query_block
    blocks = qseq.reshape(block_count, query_block, QUERY_HEADS, HEAD_SIZE)
    begins = jnp.arange(block_count, dtype=jnp.int32) * query_block
    outcomes, log_totals = lax.map(lambda element: forward_block(element[0], element[1], kseq, vseq), (blocks, begins))
    return (outcomes.reshape(total_length, QUERY_HEADS * HEAD_SIZE), log_totals)

def sequence_backward(qseq, kseq, vseq, log_totals, dseq, oseq):
    total_length = qseq.shape[0]
    query_block = min(256, total_length)
    block_count = total_length // query_block
    blocks = qseq.reshape(block_count, query_block, QUERY_HEADS, HEAD_SIZE)
    begins = jnp.arange(block_count, dtype=jnp.int32) * query_block

    def scan_step(loop_state, element):
        dquery, key_gradient, dvalue = backward_block(element[0], element[1], element[2], element[3], element[4], kseq, vseq)
        return ((loop_state[0] + key_gradient, loop_state[1] + dvalue), dquery)
    initial_state = (jnp.zeros((total_length, KEY_VALUE_HEADS, HEAD_SIZE), jnp.float32), jnp.zeros((total_length, KEY_VALUE_HEADS, HEAD_SIZE), jnp.float32))
    (keys_gradient, values_gradient), d_queries = lax.scan(scan_step, initial_state, (blocks, begins, log_totals, dseq.reshape(block_count, query_block, QUERY_HEADS * HEAD_SIZE), oseq.reshape(block_count, query_block, QUERY_HEADS * HEAD_SIZE)))
    return (d_queries.reshape(total_length, QUERY_HEADS, HEAD_SIZE), keys_gradient, values_gradient)

def reference(inputs, cotangent, routes, attn_gain, w_query, key_matrix, value_matrix, w_output, moe_gain, w_router, w_experts):
    token_list = inputs.shape[0]
    total_length = DEVICE_TOKENS * N_SHARD
    inputs_wide = inputs.astype(jnp.float32)
    r_one = lax.rsqrt(lax.optimization_barrier(jnp.mean(inputs_wide * inputs_wide, axis=-1, keepdims=True)) + EPSILON)
    z_one = inputs_wide * r_one
    normed_first = (z_one * attn_gain.astype(jnp.float32)).astype(jnp.bfloat16)
    row_ids = jnp.arange(token_list, dtype=jnp.int32)
    positions = (row_ids // TOK_DEV % N_SHARD * DEVICE_TOKENS + row_ids % DEVICE_TOKENS).astype(jnp.float32)
    cosine_table, sines_table = angle_tables(positions)
    query_rotated = apply_rotation(jnp.dot(normed_first, w_query, preferred_element_type=jnp.float32).reshape(token_list, QUERY_HEADS, HEAD_SIZE), cosine_table, sines_table).astype(jnp.bfloat16)
    key_rotated = apply_rotation(jnp.dot(normed_first, key_matrix, preferred_element_type=jnp.float32).reshape(token_list, KEY_VALUE_HEADS, HEAD_SIZE), cosine_table, sines_table).astype(jnp.bfloat16)
    value_second = jnp.dot(normed_first, value_matrix, preferred_element_type=jnp.float32).astype(jnp.bfloat16).reshape(token_list, KEY_VALUE_HEADS, HEAD_SIZE)
    query_seq = to_sequences(query_rotated)
    key_seq = to_sequences(key_rotated)
    value_seq = to_sequences(value_second)
    mixed_seq, log_totals = lax.map(lambda element: sequence_forward(element[0], element[1], element[2]), (query_seq, key_seq, value_seq))
    attention_mixed = gathered_sequences(mixed_seq)
    h_one = inputs_wide + jnp.dot(attention_mixed, w_output, preferred_element_type=jnp.float32)
    r_two = lax.rsqrt(lax.optimization_barrier(jnp.mean(h_one * h_one, axis=-1, keepdims=True)) + EPSILON)
    z_two = h_one * r_two
    n_two = (z_two * moe_gain.astype(jnp.float32)).astype(jnp.bfloat16)
    logits = jnp.dot(n_two, w_router, preferred_element_type=jnp.float32)
    expert_ids = jnp.arange(E, dtype=jnp.int32)
    route_picks = (routes[:, :, None] == expert_ids[None, None, :]).astype(jnp.float32)
    chosen = lax.optimization_barrier(jnp.sum(route_picks * logits[:, None, :], axis=-1))
    weights = jax.nn.softmax(chosen, axis=-1)
    route_total = token_list * TOP
    devices = token_list // TOK_DEV
    groups = devices // N_SHARD
    local_routes = routes.reshape(devices, TOK_DEV * TOP)
    route_hits = (local_routes[:, :, None] == expert_ids[None, None, :]).astype(jnp.int32)
    route_ranks = lax.optimization_barrier(jnp.sum(jnp.cumsum(route_hits, axis=1) * route_hits, axis=2)) - 1
    expert_room = devices * CAP
    device_ids = jnp.arange(devices, dtype=jnp.int32)[:, None]
    slot_index = (local_routes * expert_room + device_ids * CAP + route_ranks).reshape(-1)
    route_ids = jnp.arange(route_total, dtype=jnp.int32)
    token_of = route_ids // TOP
    token_table = jnp.full((E * expert_room,), token_list, jnp.int32).at[slot_index].set(token_of).reshape(E, expert_room)
    route_table = jnp.full((E * expert_room,), route_total, jnp.int32).at[slot_index].set(route_ids).reshape(E, expert_room)
    n_two_pad = jnp.concatenate([n_two, jnp.zeros((1, MODEL_WIDTH), jnp.bfloat16)], axis=0)
    dy_pad = jnp.concatenate([cotangent.astype(jnp.float32), jnp.zeros((1, MODEL_WIDTH), jnp.float32)], axis=0)
    weight_pad = jnp.concatenate([weights.reshape(-1), jnp.zeros((1,), jnp.float32)])

    def expert_step(loop_state, element):
        moe_sum, dweights, row_grads = loop_state
        token_rows, route_rows, weight_block = element
        rows_in = n_two_pad[token_rows]
        dy_rows = dy_pad[token_rows]
        slot_weight = weight_pad[route_rows]
        gate_and_up = weight_block[:, :2 * FF]
        down_part = weight_block[:, 2 * FF:]
        both_parts = jnp.dot(rows_in, gate_and_up, preferred_element_type=jnp.float32)
        gate_part = both_parts[:, :FF]
        upper_part = both_parts[:, FF:]
        sigmoid_gate = jax.nn.sigmoid(gate_part)
        activated = (gate_part * sigmoid_gate * upper_part).astype(jnp.bfloat16)
        expert_out = jnp.dot(activated, down_part.T, preferred_element_type=jnp.float32).astype(jnp.bfloat16)
        out_wide = expert_out.astype(jnp.float32)
        moe_sum = moe_sum.at[token_rows].add(slot_weight[:, None] * out_wide)
        dweights = dweights.at[route_rows].set(lax.optimization_barrier(jnp.sum(dy_rows * out_wide, axis=-1)))
        dexpert = (slot_weight[:, None] * dy_rows).astype(jnp.bfloat16)
        d_act = jnp.dot(dexpert, down_part, preferred_element_type=jnp.float32)
        d_gate_up = jnp.concatenate([d_act * upper_part * sigmoid_gate * (1.0 + gate_part * (1.0 - sigmoid_gate)), d_act * gate_part * sigmoid_gate], axis=-1).astype(jnp.bfloat16)
        row_grad = jnp.dot(d_gate_up, gate_and_up.T, preferred_element_type=jnp.float32).astype(jnp.bfloat16)
        row_grads = row_grads.at[token_rows].add(row_grad.astype(jnp.float32))
        rows_four = rows_in.astype(jnp.float32).reshape(groups, N_SHARD, CAP, MODEL_WIDTH)
        gate_grad_four = d_gate_up.astype(jnp.float32).reshape(groups, N_SHARD, CAP, 2 * FF)
        dexpert_four = dexpert.astype(jnp.float32).reshape(groups, N_SHARD, CAP, MODEL_WIDTH)
        act_four = activated.astype(jnp.float32).reshape(groups, N_SHARD, CAP, FF)
        first_part = lax.optimization_barrier(jnp.sum(to_narrow(jnp.einsum('gscd,gscf->sdf', rows_four, gate_grad_four)), axis=0))
        second_part = lax.optimization_barrier(jnp.sum(to_narrow(jnp.einsum('gscd,gscf->sdf', dexpert_four, act_four)), axis=0))
        grad_block = jnp.concatenate([first_part, second_part], axis=1)
        return ((moe_sum, dweights, row_grads), grad_block)
    initial_state = (jnp.zeros((token_list + 1, MODEL_WIDTH), jnp.float32), jnp.zeros((route_total + 1,), jnp.float32), jnp.zeros((token_list + 1, MODEL_WIDTH), jnp.float32))
    (moe_sum, dweights, row_grads), grad_blocks = lax.scan(expert_step, initial_state, (token_table, route_table, jnp.transpose(w_experts, (1, 0, 2))))
    grad_w_experts = jnp.transpose(grad_blocks, (1, 0, 2))
    outputs = (h_one + moe_sum[:token_list]).astype(jnp.bfloat16)
    dweights = dweights[:route_total].reshape(token_list, TOP)
    d_chosen = weights * (dweights - lax.optimization_barrier(jnp.sum(weights * dweights, axis=-1, keepdims=True)))
    d_logits = lax.optimization_barrier(jnp.sum(route_picks * d_chosen[:, :, None], axis=1)).astype(jnp.bfloat16)
    grad_w_router = jnp.dot(n_two.T, d_logits, preferred_element_type=jnp.float32)
    d_n_two = jnp.dot(d_logits, w_router.T, preferred_element_type=jnp.float32) + row_grads[:token_list]
    grad_moe_gain = lax.optimization_barrier(jnp.sum(d_n_two * z_two, axis=0))
    dz_two = d_n_two * moe_gain.astype(jnp.float32)
    dh_one = cotangent.astype(jnp.float32) + r_two * (dz_two - z_two * lax.optimization_barrier(jnp.mean(dz_two * z_two, axis=-1, keepdims=True)))
    dh_narrow = dh_one.astype(jnp.bfloat16)
    grad_w_output = jnp.dot(attention_mixed.T, dh_narrow, preferred_element_type=jnp.float32)
    mixed_gradient = jnp.dot(dh_narrow, w_output.T, preferred_element_type=jnp.float32).astype(jnp.bfloat16)
    d_queries, keys_gradient, values_gradient = lax.map(lambda element: sequence_backward(element[0], element[1], element[2], element[3], element[4], element[5]), (query_seq, key_seq, value_seq, log_totals, to_sequences(mixed_gradient), mixed_seq))
    d_query = reverse_rotation(gathered_sequences(d_queries), cosine_table, sines_table).reshape(token_list, QUERY_HEADS * HEAD_SIZE).astype(jnp.bfloat16)
    key_gradient = reverse_rotation(gathered_sequences(keys_gradient), cosine_table, sines_table).reshape(token_list, KEY_VALUE_HEADS * HEAD_SIZE).astype(jnp.bfloat16)
    value_gradient = gathered_sequences(values_gradient).reshape(token_list, KEY_VALUE_HEADS * HEAD_SIZE).astype(jnp.bfloat16)
    grad_w_query = jnp.dot(normed_first.T, d_query, preferred_element_type=jnp.float32)
    grad_w_key = jnp.dot(normed_first.T, key_gradient, preferred_element_type=jnp.float32)
    grad_w_value = jnp.dot(normed_first.T, value_gradient, preferred_element_type=jnp.float32)
    d_n_one = jnp.dot(d_query, w_query.T, preferred_element_type=jnp.float32) + jnp.dot(key_gradient, key_matrix.T, preferred_element_type=jnp.float32) + jnp.dot(value_gradient, value_matrix.T, preferred_element_type=jnp.float32)
    grad_attn_gain = lax.optimization_barrier(jnp.sum(d_n_one * z_one, axis=0))
    dz_one = d_n_one * attn_gain.astype(jnp.float32)
    grad_inputs = dh_one + r_one * (dz_one - z_one * lax.optimization_barrier(jnp.mean(dz_one * z_one, axis=-1, keepdims=True)))
    return (outputs, grad_inputs, grad_attn_gain, grad_w_query, grad_w_key, grad_w_value, grad_w_output, grad_moe_gain, grad_w_router, grad_w_experts)
```

```python
import functools

import jax
import jax.numpy as jnp
from jax import lax
from jax.experimental import pallas as pl
from jax.experimental.pallas import tpu as pltpu
from jax.sharding import PartitionSpec as P

MODEL_WIDTH = 1536
QUERY_HEADS = 24
KEY_VALUE_HEADS = 8
HEAD_SIZE = 64
FF = 512
E = 40
TOP = 8
DEVICE_TOKENS = 64
CAP = 38


EPSILON = 1e-06
ROPE_BASE = 10000.0
MASKED = -1e30
LANES = 128


def angle_tables(positions):
    half_width = HEAD_SIZE // 2
    frequency = jnp.power(
        ROPE_BASE, -(jnp.arange(half_width, dtype=jnp.float32) * (2.0 / HEAD_SIZE))
    )
    angles = positions[:, None] * frequency[None, :]
    return (jnp.cos(angles), jnp.sin(angles))


def apply_rotation(values, cosine_table, sines_table):
    half_width = values.shape[-1] // 2
    first_half, second_half = (values[..., :half_width], values[..., half_width:])
    cosine_table, sines_table = (cosine_table[:, None, :], sines_table[:, None, :])
    return jnp.concatenate(
        [
            first_half * cosine_table - second_half * sines_table,
            second_half * cosine_table + first_half * sines_table,
        ],
        axis=-1,
    )


def reverse_rotation(values, cosine_table, sines_table):
    half_width = values.shape[-1] // 2
    first_half, second_half = (values[..., :half_width], values[..., half_width:])
    cosine_table, sines_table = (cosine_table[:, None, :], sines_table[:, None, :])
    return jnp.concatenate(
        [
            first_half * cosine_table + second_half * sines_table,
            second_half * cosine_table - first_half * sines_table,
        ],
        axis=-1,
    )


def general(
    inputs,
    cotangent,
    routes,
    attn_gain,
    w_query,
    key_matrix,
    value_matrix,
    w_output,
    moe_gain,
    w_router,
    w_experts,
):
    rows_local = inputs.shape[0]
    group_count = lax.axis_size("expert")
    experts_here = E // group_count
    group_width = QUERY_HEADS // KEY_VALUE_HEADS
    key_value_width = KEY_VALUE_HEADS * HEAD_SIZE
    scale_factor = 1.0 / HEAD_SIZE
    sequence_count = rows_local // DEVICE_TOKENS
    gain_one, query_full, key_complete, value_full, output_full, router_full, gain_two = (
        lax.all_gather(attn_gain, "shard", axis=0, tiled=True),
        lax.all_gather(w_query, "shard", axis=0, tiled=True),
        lax.all_gather(key_matrix, "shard", axis=0, tiled=True),
        lax.all_gather(value_matrix, "shard", axis=0, tiled=True),
        lax.all_gather(w_output, "shard", axis=0, tiled=True),
        lax.all_gather(w_router, "shard", axis=0, tiled=True),
        lax.all_gather(moe_gain, "shard", axis=0, tiled=True),
    )
    inputs_wide = inputs.astype(jnp.float32)
    r_one = lax.rsqrt(jnp.mean(inputs_wide * inputs_wide, axis=-1, keepdims=True) + EPSILON)
    z_one = inputs_wide * r_one
    normed_first = (z_one * gain_one.astype(jnp.float32)).astype(jnp.bfloat16)
    offset = lax.axis_index("shard") * DEVICE_TOKENS
    positions = offset + jnp.arange(DEVICE_TOKENS, dtype=jnp.int32)
    row_positions = jnp.tile(positions, sequence_count)
    cosine_table, sines_table = angle_tables(row_positions.astype(jnp.float32))
    query_rotated = apply_rotation(
        jnp.dot(normed_first, query_full, preferred_element_type=jnp.float32).reshape(
            rows_local, QUERY_HEADS, HEAD_SIZE
        ),
        cosine_table,
        sines_table,
    ).astype(jnp.bfloat16)
    keys_rot = apply_rotation(
        jnp.dot(normed_first, key_complete, preferred_element_type=jnp.float32).reshape(
            rows_local, KEY_VALUE_HEADS, HEAD_SIZE
        ),
        cosine_table,
        sines_table,
    ).astype(jnp.bfloat16)
    values_narrow = jnp.dot(normed_first, value_full, preferred_element_type=jnp.float32).astype(
        jnp.bfloat16
    )
    kv_local = jnp.concatenate(
        [keys_rot.reshape(rows_local, key_value_width), values_narrow], axis=1
    ).reshape(sequence_count, DEVICE_TOKENS, 2 * key_value_width)
    kv_all = lax.all_gather(kv_local, "shard", axis=1, tiled=True)
    seq_length = kv_all.shape[1]
    block_of_keys = min(512, seq_length)
    total_of_block = (offset + DEVICE_TOKENS + block_of_keys - 1) // block_of_keys
    query_four_dims = query_rotated.reshape(
        sequence_count, DEVICE_TOKENS, KEY_VALUE_HEADS, group_width, HEAD_SIZE
    )

    def scores_for(block_index):
        start_row = block_index * block_of_keys
        key_value_slice = lax.dynamic_slice_in_dim(kv_all, start_row, block_of_keys, 1)
        keys_block = key_value_slice[..., :key_value_width].reshape(
            sequence_count, block_of_keys, KEY_VALUE_HEADS, HEAD_SIZE
        )
        values_block = key_value_slice[..., key_value_width:].reshape(
            sequence_count, block_of_keys, KEY_VALUE_HEADS, HEAD_SIZE
        )
        scores = (
            jnp.einsum(
                "nqjgd,nkjd->njgqk", query_four_dims, keys_block, preferred_element_type=jnp.float32
            )
            * scale_factor
        )
        key_pos = start_row + jnp.arange(block_of_keys, dtype=jnp.int32)
        allowed = key_pos[None, :] <= positions[:, None]
        return (jnp.where(allowed, scores, MASKED), keys_block, values_block)

    def stats_step(block_index, loop_state):
        running_max, running_sum = loop_state
        scores = scores_for(block_index)[0]
        new_max = jnp.maximum(running_max, jnp.max(scores, axis=-1))
        running_sum = running_sum * jnp.exp(running_max - new_max) + jnp.sum(
            jnp.exp(scores - new_max[..., None]), axis=-1
        )
        return (new_max, running_sum)

    statistics_shape = (sequence_count, KEY_VALUE_HEADS, group_width, DEVICE_TOKENS)
    start_stats = (
        jnp.full(statistics_shape, MASKED, jnp.float32),
        jnp.zeros(statistics_shape, jnp.float32),
    )
    run_max, run_sum = lax.fori_loop(0, total_of_block, stats_step, start_stats)
    log_total = run_max + jnp.log(run_sum)

    def mixing_step(block_index, mixed_sum):
        scores, keys_block, values_block = scores_for(block_index)
        attn_probs = jnp.exp(scores - log_total[..., None]).astype(jnp.bfloat16)
        return mixed_sum + jnp.einsum(
            "njgqk,nkjd->nqjgd", attn_probs, values_block, preferred_element_type=jnp.float32
        )

    attention_mixed = lax.fori_loop(
        0,
        total_of_block,
        mixing_step,
        jnp.zeros(
            (sequence_count, DEVICE_TOKENS, KEY_VALUE_HEADS, group_width, HEAD_SIZE), jnp.float32
        ),
    )
    attention_mixed = attention_mixed.reshape(rows_local, QUERY_HEADS * HEAD_SIZE).astype(
        jnp.bfloat16
    )
    h_one = inputs_wide + jnp.dot(attention_mixed, output_full, preferred_element_type=jnp.float32)
    r_two = lax.rsqrt(jnp.mean(h_one * h_one, axis=-1, keepdims=True) + EPSILON)
    z_two = h_one * r_two
    n_two = (z_two * gain_two.astype(jnp.float32)).astype(jnp.bfloat16)
    logits = jnp.dot(n_two, router_full, preferred_element_type=jnp.float32)
    expert_ids = jnp.arange(E, dtype=jnp.int32)
    route_picks = (routes[:, :, None] == expert_ids[None, None, :]).astype(jnp.float32)
    chosen = jnp.sum(route_picks * logits[:, None, :], axis=-1)
    weights = jax.nn.softmax(chosen, axis=-1)
    flat_routes = routes.reshape(-1)
    route_hits = (flat_routes[:, None] == expert_ids[None, :]).astype(jnp.int32)
    route_ranks = jnp.sum(jnp.cumsum(route_hits, axis=0) * route_hits, axis=1) - 1
    targets = flat_routes * CAP + route_ranks
    token_of = jnp.arange(rows_local * TOP, dtype=jnp.int32) // TOP
    outgoing = jnp.zeros((E * CAP, MODEL_WIDTH), jnp.bfloat16).at[targets].set(n_two[token_of])
    arrived = lax.all_to_all(
        outgoing.reshape(group_count, experts_here, CAP, MODEL_WIDTH),
        "expert",
        split_axis=0,
        concat_axis=0,
        tiled=True,
    )
    expert_full = lax.all_gather(w_experts, "shard", axis=0, tiled=True)
    gate_and_up = expert_full[:, :, : 2 * FF]
    down_part = expert_full[:, :, 2 * FF :]
    both_parts = jnp.einsum(
        "sjcd,djf->sjcf", arrived, gate_and_up, preferred_element_type=jnp.float32
    )
    gate_part = both_parts[..., :FF]
    upper_part = both_parts[..., FF:]
    sigmoid_gate = jax.nn.sigmoid(gate_part)
    activated = (gate_part * sigmoid_gate * upper_part).astype(jnp.bfloat16)
    produced = jnp.einsum(
        "sjcf,djf->sjcd", activated, down_part, preferred_element_type=jnp.float32
    ).astype(jnp.bfloat16)
    returned = lax.all_to_all(produced, "expert", split_axis=0, concat_axis=0, tiled=True).reshape(
        E * CAP, MODEL_WIDTH
    )
    route_out = returned[targets].reshape(rows_local, TOP, MODEL_WIDTH).astype(jnp.float32)
    moe_sum = jnp.sum(weights[:, :, None] * route_out, axis=1)
    outputs = (h_one + moe_sum).astype(jnp.bfloat16)
    dy_wide = cotangent.astype(jnp.float32)
    d_routes = (
        (weights[:, :, None] * dy_wide[:, None, :])
        .astype(jnp.bfloat16)
        .reshape(rows_local * TOP, MODEL_WIDTH)
    )
    d_outgoing = jnp.zeros((E * CAP, MODEL_WIDTH), jnp.bfloat16).at[targets].set(d_routes)
    d_arrived = lax.all_to_all(
        d_outgoing.reshape(group_count, experts_here, CAP, MODEL_WIDTH),
        "expert",
        split_axis=0,
        concat_axis=0,
        tiled=True,
    )
    d_weights = jnp.sum(dy_wide[:, None, :] * route_out, axis=-1)
    d_chosen = weights * (d_weights - jnp.sum(weights * d_weights, axis=-1, keepdims=True))
    d_logits = jnp.sum(route_picks * d_chosen[:, :, None], axis=1).astype(jnp.bfloat16)
    grad_router = jnp.einsum("td,te->de", n_two, d_logits, preferred_element_type=jnp.float32)
    d_act = jnp.einsum("sjcd,djf->sjcf", d_arrived, down_part, preferred_element_type=jnp.float32)
    d_gate_up = jnp.concatenate(
        [
            d_act * upper_part * sigmoid_gate * (1.0 + gate_part * (1.0 - sigmoid_gate)),
            d_act * gate_part * sigmoid_gate,
        ],
        axis=-1,
    ).astype(jnp.bfloat16)
    d_rows = jnp.einsum(
        "sjcf,djf->sjcd", d_gate_up, gate_and_up, preferred_element_type=jnp.float32
    ).astype(jnp.bfloat16)
    d_returned = lax.all_to_all(d_rows, "expert", split_axis=0, concat_axis=0, tiled=True).reshape(
        E * CAP, MODEL_WIDTH
    )
    d_n_two = jnp.einsum(
        "te,de->td", d_logits, router_full, preferred_element_type=jnp.float32
    ) + jnp.sum(
        d_returned[targets].reshape(rows_local, TOP, MODEL_WIDTH).astype(jnp.float32), axis=1
    )
    first_part = jnp.einsum(
        "sjcd,sjcf->djf", arrived, d_gate_up, preferred_element_type=jnp.float32
    )
    second = jnp.einsum("sjcd,sjcf->djf", d_arrived, activated, preferred_element_type=jnp.float32)
    grad_experts = lax.psum_scatter(
        jnp.concatenate([first_part, second], axis=2).astype(jnp.bfloat16),
        "shard",
        scatter_dimension=0,
        tiled=True,
    ).astype(jnp.float32)
    grad_gain_two = jnp.sum(d_n_two * z_two, axis=0)
    dz_two = d_n_two * gain_two.astype(jnp.float32)
    dh_one = dy_wide + r_two * (dz_two - z_two * jnp.mean(dz_two * z_two, axis=-1, keepdims=True))
    dh_narrow = dh_one.astype(jnp.bfloat16)
    grad_output = jnp.einsum(
        "tk,td->kd", attention_mixed, dh_narrow, preferred_element_type=jnp.float32
    )
    mixed_gradient = jnp.einsum(
        "td,kd->tk", dh_narrow, output_full, preferred_element_type=jnp.float32
    ).astype(jnp.bfloat16)
    grad_four_dims = mixed_gradient.reshape(
        sequence_count, DEVICE_TOKENS, KEY_VALUE_HEADS, group_width, HEAD_SIZE
    )
    row_difference = jnp.sum(
        grad_four_dims.astype(jnp.float32)
        * attention_mixed.reshape(
            sequence_count, DEVICE_TOKENS, KEY_VALUE_HEADS, group_width, HEAD_SIZE
        ).astype(jnp.float32),
        axis=-1,
    )
    row_difference = jnp.transpose(row_difference, (0, 2, 3, 1))

    def grad_step(block_index, loop_state):
        d_query_sum, d_key_rows = loop_state
        scores, keys_block, values_block = scores_for(block_index)
        attn_probs = jnp.exp(scores - log_total[..., None])
        d_probs = jnp.einsum(
            "nqjgd,nkjd->njgqk", grad_four_dims, values_block, preferred_element_type=jnp.float32
        )
        d_scores = (attn_probs * (d_probs - row_difference[..., None])).astype(jnp.bfloat16)
        d_query_sum = (
            d_query_sum
            + jnp.einsum(
                "njgqk,nkjd->nqjgd", d_scores, keys_block, preferred_element_type=jnp.float32
            )
            * scale_factor
        )
        key_grad = (
            jnp.einsum(
                "njgqk,nqjgd->nkjd", d_scores, query_four_dims, preferred_element_type=jnp.float32
            )
            * scale_factor
        )
        value_grad = jnp.einsum(
            "njgqk,nqjgd->nkjd",
            attn_probs.astype(jnp.bfloat16),
            grad_four_dims,
            preferred_element_type=jnp.float32,
        )
        update = jnp.concatenate(
            [
                key_grad.reshape(sequence_count, block_of_keys, key_value_width),
                value_grad.reshape(sequence_count, block_of_keys, key_value_width),
            ],
            axis=2,
        )
        d_key_rows = lax.dynamic_update_slice_in_dim(
            d_key_rows, update, block_index * block_of_keys, 1
        )
        return (d_query_sum, d_key_rows)

    start_grads = (
        jnp.zeros(
            (sequence_count, DEVICE_TOKENS, KEY_VALUE_HEADS, group_width, HEAD_SIZE), jnp.float32
        ),
        jnp.zeros((sequence_count, seq_length, 2 * key_value_width), jnp.float32),
    )
    d_query_sum, d_key_rows = lax.fori_loop(0, total_of_block, grad_step, start_grads)
    owned_keys = (
        lax.psum_scatter(d_key_rows.astype(jnp.bfloat16), "shard", scatter_dimension=1, tiled=True)
        .astype(jnp.float32)
        .reshape(rows_local, 2 * key_value_width)
    )
    d_query = (
        reverse_rotation(
            d_query_sum.reshape(rows_local, QUERY_HEADS, HEAD_SIZE), cosine_table, sines_table
        )
        .reshape(rows_local, QUERY_HEADS * HEAD_SIZE)
        .astype(jnp.bfloat16)
    )
    key_gradient = (
        reverse_rotation(
            owned_keys[:, :key_value_width].reshape(rows_local, KEY_VALUE_HEADS, HEAD_SIZE),
            cosine_table,
            sines_table,
        )
        .reshape(rows_local, key_value_width)
        .astype(jnp.bfloat16)
    )
    value_gradient = owned_keys[:, key_value_width:].astype(jnp.bfloat16)
    grad_query = jnp.einsum("td,tk->dk", normed_first, d_query, preferred_element_type=jnp.float32)
    grad_key = jnp.einsum(
        "td,tk->dk", normed_first, key_gradient, preferred_element_type=jnp.float32
    )
    grad_value = jnp.einsum(
        "td,tk->dk", normed_first, value_gradient, preferred_element_type=jnp.float32
    )
    d_n_one = (
        jnp.einsum("tk,dk->td", d_query, query_full, preferred_element_type=jnp.float32)
        + jnp.einsum("tk,dk->td", key_gradient, key_complete, preferred_element_type=jnp.float32)
        + jnp.einsum("tk,dk->td", value_gradient, value_full, preferred_element_type=jnp.float32)
    )
    grad_gain_one = jnp.sum(d_n_one * z_one, axis=0)
    dz_one = d_n_one * gain_one.astype(jnp.float32)
    grad_inputs = dh_one + r_one * (
        dz_one - z_one * jnp.mean(dz_one * z_one, axis=-1, keepdims=True)
    )
    totals = (
        lax.psum_scatter(
            grad_gain_one.astype(jnp.bfloat16), "shard", scatter_dimension=0, tiled=True
        ).astype(jnp.float32),
        lax.psum_scatter(
            grad_query.astype(jnp.bfloat16), "shard", scatter_dimension=0, tiled=True
        ).astype(jnp.float32),
        lax.psum_scatter(
            grad_key.astype(jnp.bfloat16), "shard", scatter_dimension=0, tiled=True
        ).astype(jnp.float32),
        lax.psum_scatter(
            grad_value.astype(jnp.bfloat16), "shard", scatter_dimension=0, tiled=True
        ).astype(jnp.float32),
        lax.psum_scatter(
            grad_output.astype(jnp.bfloat16), "shard", scatter_dimension=0, tiled=True
        ).astype(jnp.float32),
        lax.psum_scatter(
            grad_router.astype(jnp.bfloat16), "shard", scatter_dimension=0, tiled=True
        ).astype(jnp.float32),
        lax.psum_scatter(
            grad_gain_two.astype(jnp.bfloat16), "shard", scatter_dimension=0, tiled=True
        ).astype(jnp.float32),
    )
    totals = (
        lax.psum(totals[0].astype(jnp.bfloat16), "expert").astype(jnp.float32),
        lax.psum(totals[1].astype(jnp.bfloat16), "expert").astype(jnp.float32),
        lax.psum(totals[2].astype(jnp.bfloat16), "expert").astype(jnp.float32),
        lax.psum(totals[3].astype(jnp.bfloat16), "expert").astype(jnp.float32),
        lax.psum(totals[4].astype(jnp.bfloat16), "expert").astype(jnp.float32),
        lax.psum(totals[5].astype(jnp.bfloat16), "expert").astype(jnp.float32),
        lax.psum(totals[6].astype(jnp.bfloat16), "expert").astype(jnp.float32),
    )
    return (
        outputs,
        grad_inputs,
        totals[0],
        totals[1],
        totals[2],
        totals[3],
        totals[4],
        totals[6],
        totals[5],
        grad_experts,
    )


def divides(shards, groups):
    experts_here = E // groups
    if groups != 4 or shards % 2 or shards < 4:
        return False
    if KEY_VALUE_HEADS % shards or shards > experts_here:
        return False
    extra = experts_here % shards
    return extra == 0 or (shards % extra == 0 and FF % (shards // extra) == 0)


def packed_experts(w_experts, shards):
    rows, experts_here, _ = w_experts.shape
    whole, extra = divmod(experts_here, shards)
    parts = [w_experts[:, : whole * shards].reshape(rows, shards, whole * 3 * FF)]
    if extra:
        cuts = shards // extra
        width = FF // cuts
        cut = w_experts[:, whole * shards :].reshape(rows, extra, 3, cuts, width)
        parts.append(jnp.transpose(cut, (0, 1, 3, 2, 4)).reshape(rows, shards, 3 * width))
    return jnp.transpose(jnp.concatenate(parts, axis=2), (1, 0, 2))


def unpacked_experts(blocks, experts_here):
    shards, rows, _ = blocks.shape
    whole, extra = divmod(experts_here, shards)
    blocks = jnp.transpose(blocks, (1, 0, 2))
    parts = [blocks[:, :, : whole * 3 * FF].reshape(rows, shards * whole, 3 * FF)]
    if extra:
        cuts = shards // extra
        width = FF // cuts
        cut = blocks[:, :, whole * 3 * FF :].reshape(rows, extra, cuts, 3, width)
        parts.append(jnp.transpose(cut, (0, 1, 3, 2, 4)).reshape(rows, extra, 3 * FF))
    return jnp.concatenate(parts, axis=1)


def rotated(values, cosine, sine):
    half = HEAD_SIZE // 2
    first, second = values[..., :half], values[..., half:]
    return jnp.concatenate([first * cosine - second * sine, second * cosine + first * sine], axis=-1)


def alternating(depth):
    order = []
    low, high = 0, depth - 1
    while low <= high:
        order.append(high)
        if low != high:
            order.append(low)
        low, high = low + 1, high - 1
    return order


def sent(source, target, send, receive, group, shard):
    return pltpu.make_async_remote_copy(
        src_ref=source,
        dst_ref=target,
        send_sem=send,
        recv_sem=receive,
        device_id=(group, shard),
        device_id_type=pl.DeviceIdType.MESH,
    )


class Place:
    def __init__(self, shards, groups):
        self.group, self.shard = lax.axis_index("expert"), lax.axis_index("shard")
        self.shards, self.groups = shards, groups
        self.depth = shards // 2
        self.spot, self.core = self.shard // 2, self.shard % 2
        self.first = self.group + 1 - 2 * (self.group % 2)
        self.second = (self.group + 2) % 4
        self.corner = (self.first + 2) % 4
        self.partner = self.shard + 1 - 2 * self.core

    def greet(self, wide, whole_line):
        barrier = pltpu.get_barrier_semaphore()

        def signal(group, shard):
            pl.semaphore_signal(
                barrier, inc=1, device_id=(group, shard), device_id_type=pl.DeviceIdType.MESH
            )

        more = 2 if wide else 0
        if wide:
            signal(self.first, self.shard)
            signal(self.second, self.shard)
        if whole_line:
            for i in range(1, self.shards):
                signal(self.group, (self.shard + i) % self.shards)
            pl.semaphore_wait(barrier, more + self.shards - 1)
            return
        signal(self.group, self.partner)
        inside = (self.spot > 0) & (self.spot < self.depth - 1)

        @pl.when(self.spot > 0)
        def _():
            signal(self.group, self.shard - 2)

        @pl.when(self.spot < self.depth - 1)
        def _():
            signal(self.group, self.shard + 2)

        @pl.when(inside)
        def _():
            pl.semaphore_wait(barrier, more + 3)

        @pl.when(jnp.logical_not(inside))
        def _():
            pl.semaphore_wait(barrier, more + 2)


class Exchange:
    @staticmethod
    def scratch(array):
        n = array.shape[0]
        dma = pltpu.SemaphoreType.DMA
        return [pltpu.VMEM(array.shape[1:], array.dtype), dma((2,)), dma((n,)), dma((n,))]

    def __init__(self, at, source, target, stage, own, out, come):
        self.at, self.source, self.target = at, source, target
        self.stage, self.own, self.out, self.come = stage, own, out, come

    def copy(self, i):
        at = self.at
        to = (at.shard + i) % at.shards
        return sent(
            self.source.at[to],
            self.target.at[at.shard],
            self.out.at[i],
            self.come.at[i],
            at.group,
            to,
        )

    def keep(self, i):
        here = self.at.shard
        if i == 0:
            return pltpu.make_async_copy(self.source.at[here], self.stage, self.own.at[0])
        return pltpu.make_async_copy(self.stage, self.target.at[here], self.own.at[1])

    def start(self):
        self.keep(0).start()
        for i in range(self.at.shards - 1, 0, -1):
            self.copy(i).start()
        self.keep(0).wait()
        self.keep(1).start()

    def finish(self):
        self.keep(1).wait()
        for i in range(1, self.at.shards):
            self.copy(i).wait()


class Gather:
    @staticmethod
    def scratch(array, wide, shards):
        steps = shards // 2 - 1
        marks = 1 + 2 * steps
        dma = pltpu.SemaphoreType.DMA
        turns = 2 if wide else 1
        return [
            dma((1,)),
            dma((2 * steps,)),
            dma((2 * steps,)),
            dma((turns, marks)),
            dma((turns, marks)),
            dma((turns, marks)),
            dma((turns, marks)),
            dma((5 if wide else 1, marks)),
            dma((5 if wide else 1, marks)),
        ]

    def __init__(self, at, wide, block, out, *sems):
        self.at, self.wide, self.block, self.out = at, wide, block, out
        self.own, self.z_out, self.z_in, self.p_out, self.p_in = sems[:5]
        self.h_out, self.h_in, self.c_out, self.c_in = sems[5:]
        self.steps = at.depth - 1
        self.events = [(0, 0)]
        for t in range(self.steps):
            self.events += [(1, t), (2, t)]

    def when(self, event, body):
        kind, t = event
        if kind == 0:
            body()
        elif kind == 1:
            pl.when(self.at.spot - 1 - t >= 0)(body)
        else:
            pl.when(self.at.spot + 1 + t < self.at.depth)(body)

    def origin(self, event):
        kind, t = event
        return self.at.shard + (0, -2 * (t + 1), 2 * (t + 1))[kind]

    def slot(self, group, shard):
        index = group * self.at.shards + shard if self.wide else shard
        return self.out.at[:, index]

    def half(self, ref, which):
        rows = ref.shape[1]
        cut = rows // 32 * 16
        return ref.at[:, pl.ds(0, cut)] if which == 0 else ref.at[:, pl.ds(cut, rows - cut)]

    def line(self, step, direction, shard):
        at = self.at
        k = direction * self.steps + step
        ref = self.slot(at.group, shard)
        source = self.block if step == 0 else ref
        to = at.shard + (2, -2)[direction]
        return sent(source, ref, self.z_out.at[k], self.z_in.at[k], at.group, to)

    def side(self, k, which):
        at, event = self.at, self.events[k]
        ref = self.slot(at.group, self.origin(event))
        source = self.block if event[0] == 0 else ref
        group = (at.first, at.second)[which]
        return sent(source, ref, self.p_out.at[which, k], self.p_in.at[which, k], group, at.shard)

    def turn(self, k, which):
        at = self.at
        shard = self.origin(self.events[k])
        held = self.half(self.slot((at.first, at.second)[which], shard), which)
        group = (at.second, at.first)[which]
        return sent(held, held, self.h_out.at[which, k], self.h_in.at[which, k], group, at.shard)

    def across(self, k, kind):
        at, event = self.at, self.events[k]
        shard = self.origin(event)
        if kind < 3:
            ref = self.slot((at.group, at.first, at.second)[kind], shard)
        else:
            ref = self.half(self.slot(at.corner, shard), kind - 3)
        source = self.block if kind == 0 and event[0] == 0 else ref
        return sent(
            source, ref, self.c_out.at[kind, k], self.c_in.at[kind, k], at.group, at.partner
        )

    def keep(self):
        here = self.slot(self.at.group, self.at.shard)
        return pltpu.make_async_copy(self.block, here, self.own.at[0])

    def onward(self, event, act):
        kind, t = event
        for direction in range(2):
            if kind and direction != kind - 1:
                continue
            step = 0 if kind == 0 else t + 1
            if step >= self.steps:
                continue
            ahead = self.at.spot < self.at.depth - 1 if direction == 0 else self.at.spot > 0
            pl.when(ahead)(
                lambda step=step, direction=direction: act(
                    self.line(step, direction, self.origin(event))
                )
            )

    def lines(self, k):
        event = self.events[k]

        def body():
            kind, t = event
            if kind:
                self.line(t, kind - 1, self.origin(event)).wait_recv()
            self.onward(event, lambda copy: copy.start())
            if self.wide:
                self.side(k, 0).start()
                self.side(k, 1).start()
            self.across(k, 0).start()
            if kind == 0:
                self.keep().start()

        self.when(event, body)

    def sides(self, k):
        def body():
            for which in range(2):
                self.side(k, which).wait_recv()
                self.turn(k, which).start()
                self.across(k, 1 + which).start()

        if self.wide:
            self.when(self.events[k], body)

    def turns(self, k):
        def body():
            for which in range(2):
                self.turn(k, which).wait_recv()
                self.across(k, 3 + which).start()

        if self.wide:
            self.when(self.events[k], body)

    def finish(self, k):
        event = self.events[k]

        def body():
            if event[0] == 0:
                self.keep().wait()
            self.onward(event, lambda copy: copy.wait_send())
            for kind in range(5 if self.wide else 1):
                copy = self.across(k, kind)
                copy.wait_send()
                copy.wait_recv()
            if self.wide:
                for which in range(2):
                    self.side(k, which).wait_send()
                    self.turn(k, which).wait_send()

        self.when(event, body)


class Reduce:
    @staticmethod
    def scratch(parts, wide, shards):
        depth = shards // 2
        block = (parts.shape[0],) + parts.shape[2:]
        kinds = 4 if wide else 1
        dma = pltpu.SemaphoreType.DMA
        out = [
            pltpu.VMEM((kinds, depth) + block, parts.dtype),
            pltpu.VMEM((kinds, depth) + block, parts.dtype),
            pltpu.VMEM((2, depth) + block, parts.dtype),
            dma((kinds, depth)),
            dma((kinds, depth)),
            dma((kinds, depth)),
            dma((2, depth)),
            dma((2, depth)),
        ]
        if wide:
            cut = block[1] // 32 * 16
            out += [
                pltpu.VMEM((depth, block[0], cut, block[2]), parts.dtype),
                pltpu.VMEM((depth, block[0], block[1] - cut, block[2]), parts.dtype),
                pltpu.VMEM((2, depth) + block, parts.dtype),
                dma((2, depth)),
                dma((2, depth)),
                dma((2, depth)),
                dma((2, depth)),
            ]
        return out

    def __init__(self, at, wide, parts, total, *scratch):
        self.at, self.wide, self.parts, self.total = at, wide, parts, total
        self.mine, self.accs, self.z_buf, self.own = scratch[:4]
        self.c_out, self.c_in, self.z_out, self.z_in = scratch[4:8]
        if wide:
            self.h_buf, self.p_buf = scratch[8:10], scratch[10]
            self.h_out, self.h_in, self.p_out, self.p_in = scratch[11:]
        self.order = alternating(at.depth)
        self.kinds = (3, 1, 2, 0) if wide else (0,)
        self.columns = (at.group, at.first, at.second, at.corner)

    def place(self, kind, q, core):
        shard = 2 * q + core
        return self.columns[kind] * self.at.shards + shard if self.wide else shard

    def load(self, kind, q):
        return pltpu.make_async_copy(
            self.parts.at[:, self.place(kind, q, self.at.core)],
            self.mine.at[kind, q],
            self.own.at[kind, q],
        )

    def across(self, kind, q):
        return sent(
            self.parts.at[:, self.place(kind, q, 1 - self.at.core)],
            self.accs.at[kind, q],
            self.c_out.at[kind, q],
            self.c_in.at[kind, q],
            self.at.group,
            self.at.partner,
        )

    def span(self, which):
        rows = self.accs.shape[3]
        cut = rows // 32 * 16
        return pl.ds(0, cut) if which == 0 else pl.ds(cut, rows - cut)

    def turn(self, q, which):
        return sent(
            self.accs.at[3, q, :, self.span(which)],
            self.h_buf[which].at[q],
            self.h_out.at[which, q],
            self.h_in.at[which, q],
            (self.at.first, self.at.second)[which],
            self.at.shard,
        )

    def side(self, q, which):
        return sent(
            self.accs.at[1 + which, q],
            self.p_buf.at[which, q],
            self.p_out.at[which, q],
            self.p_in.at[which, q],
            (self.at.first, self.at.second)[which],
            self.at.shard,
        )

    def line(self, q, direction):
        return sent(
            self.accs.at[0, q],
            self.z_buf.at[direction, q],
            self.z_out.at[direction, q],
            self.z_in.at[direction, q],
            self.at.group,
            self.at.shard + (2, -2)[direction],
        )

    def add(self, kind, q, *others):
        value = self.accs[kind, q].astype(jnp.float32)
        for other in others:
            value = value + other.astype(jnp.float32)
        self.accs[kind, q] = value.astype(self.accs.dtype)

    def pair(self, kind, q):
        self.load(kind, q).wait()
        self.across(kind, q).wait_recv()
        self.add(kind, q, self.mine[kind, q])

    def begin(self):
        for kind in self.kinds:
            for q in self.order:
                self.load(kind, q).start()
                self.across(kind, q).start()

    def corners(self):
        for q in self.order:
            self.pair(3, q)
            self.turn(q, 0).start()
            self.turn(q, 1).start()

    def sides(self):
        for q in self.order:
            for which in range(2):
                kind = 2 - which
                self.pair(kind, q)
                self.turn(q, which).wait_recv()
                span = self.span(which)
                value = self.accs[kind, q, :, span].astype(jnp.float32)
                value = value + self.h_buf[which][q].astype(jnp.float32)
                self.accs[kind, q, :, span] = value.astype(self.accs.dtype)
                self.side(q, kind - 1).start()

    def lines(self):
        at = self.at
        for q in self.order:
            self.pair(0, q)
            if self.wide:
                self.side(q, 0).wait_recv()
                self.side(q, 1).wait_recv()
                self.add(0, q, self.p_buf[0, q], self.p_buf[1, q])
            for direction in range(2):

                @pl.when(q > at.spot if direction == 0 else q < at.spot)
                def _(q=q, direction=direction):
                    @pl.when(at.spot > 0 if direction == 0 else at.spot < at.depth - 1)
                    def _():
                        self.line(q, direction).wait_recv()
                        self.add(0, q, self.z_buf[direction, q])

                    self.line(q, direction).start()

    def finish(self):
        at, total = self.at, self.total
        for q in range(at.depth):

            @pl.when(q == at.spot)
            def _(q=q):
                total[...] = self.accs[0, q].astype(jnp.float32)
                for direction in range(2):
                    if q > 0 if direction == 0 else q < at.depth - 1:
                        self.line(q, direction).wait_recv()
                        total[...] = total[...] + self.z_buf[direction, q].astype(jnp.float32)

            for kind in self.kinds:
                self.across(kind, q).wait_send()
            if self.wide:
                for which in range(2):
                    self.turn(q, which).wait_send()
                    self.side(q, which).wait_send()
            for direction in range(2):

                @pl.when(q > at.spot if direction == 0 else q < at.spot)
                def _(q=q, direction=direction):
                    self.line(q, direction).wait_send()


def cut_refs(refs, sizes):
    out, start = [], 0
    for size in sizes:
        out.append(refs[start : start + size])
        start += size
    return out


def gather_body(shards, groups, wides, swaps, sizes, *refs):
    count = len(wides) + swaps
    ins, outs = refs[:count], refs[count : 2 * count]
    scratch = cut_refs(refs[2 * count :], sizes)
    at = Place(shards, groups)
    at.greet(any(wides), swaps > 0)
    gathers = [Gather(at, wide, ins[i], outs[i], *scratch[i]) for i, wide in enumerate(wides)]
    moves = [Exchange(at, ins[i], outs[i], *scratch[i]) for i in range(len(wides), count)]
    marks = range(len(gathers[0].events))
    for k in marks:
        for g in gathers:
            g.lines(k)
    for m in moves:
        m.start()
    for step in (Gather.sides, Gather.turns, Gather.finish):
        for k in marks:
            for g in gathers:
                step(g, k)
    for m in moves:
        m.finish()


def gathered(arrays, wides, shards, groups, identity, swapped=()):
    shapes = [
        jax.ShapeDtypeStruct(
            (a.shape[0], shards * (groups if wide else 1)) + a.shape[1:], a.dtype
        )
        for a, wide in zip(arrays, wides)
    ] + [jax.ShapeDtypeStruct(a.shape, a.dtype) for a in swapped]
    moved = sum(s.size * s.dtype.itemsize for s in shapes)
    scratch = [Gather.scratch(a, wide, shards) for a, wide in zip(arrays, wides)]
    scratch += [Exchange.scratch(a) for a in swapped]
    return pl.pallas_call(
        functools.partial(
            gather_body,
            shards,
            groups,
            tuple(wides),
            len(swapped),
            tuple(len(s) for s in scratch),
        ),
        out_shape=shapes,
        in_specs=[pl.BlockSpec(memory_space=pltpu.VMEM)] * len(arrays)
        + [pl.BlockSpec(memory_space=pl.ANY)] * len(swapped),
        out_specs=[pl.BlockSpec(memory_space=pl.ANY)] * len(shapes),
        scratch_shapes=[s for some in scratch for s in some],
        compiler_params=pltpu.CompilerParams(collective_id=identity, has_side_effects=True),
        cost_estimate=pl.CostEstimate(flops=0, bytes_accessed=20 * moved, transcendentals=0),
    )(*arrays, *swapped)


def reduce_body(shards, groups, wides, swaps, sizes, *refs):
    count = len(wides) + swaps
    ins, outs = refs[:count], refs[count : 2 * count]
    scratch = cut_refs(refs[2 * count :], sizes)
    at = Place(shards, groups)
    at.greet(any(wides), swaps > 0)
    sums = [Reduce(at, wide, ins[i], outs[i], *scratch[i]) for i, wide in enumerate(wides)]
    moves = [Exchange(at, ins[i], outs[i], *scratch[i]) for i in range(len(wides), count)]
    for r in sums:
        r.begin()
    for m in moves:
        m.start()
    for r in sums:
        if r.wide:
            r.corners()
    for r in sums:
        if not r.wide:
            r.lines()
    for r in sums:
        if r.wide:
            r.sides()
            r.lines()
    for r in sums:
        r.finish()
    for m in moves:
        m.finish()


def reduced(arrays, wides, shards, groups, identity, swapped=()):
    shapes = [
        jax.ShapeDtypeStruct((a.shape[0],) + a.shape[2:], jnp.float32) for a in arrays
    ] + [jax.ShapeDtypeStruct(a.shape, a.dtype) for a in swapped]
    moved = sum(a.size * a.dtype.itemsize for a in (*arrays, *swapped))
    scratch = [Reduce.scratch(a, wide, shards) for a, wide in zip(arrays, wides)]
    scratch += [Exchange.scratch(a) for a in swapped]
    return pl.pallas_call(
        functools.partial(
            reduce_body,
            shards,
            groups,
            tuple(wides),
            len(swapped),
            tuple(len(s) for s in scratch),
        ),
        out_shape=shapes,
        in_specs=[pl.BlockSpec(memory_space=pl.ANY)] * (len(arrays) + len(swapped)),
        out_specs=[pl.BlockSpec(memory_space=pltpu.VMEM)] * len(arrays)
        + [pl.BlockSpec(memory_space=pl.ANY)] * len(swapped),
        scratch_shapes=[s for some in scratch for s in some],
        compiler_params=pltpu.CompilerParams(
            collective_id=identity, has_side_effects=True, vmem_limit_bytes=60 * 1024 * 1024
        ),
        cost_estimate=pl.CostEstimate(flops=0, bytes_accessed=20 * moved, transcendentals=0),
    )(*arrays, *swapped)


def local(
    inputs,
    cotangent,
    routes,
    attn_gain,
    w_query,
    key_matrix,
    value_matrix,
    w_output,
    moe_gain,
    w_router,
    w_experts,
):
    f32, bf16 = jnp.float32, jnp.bfloat16
    both = ("expert", "shard")
    shards, groups = lax.axis_size("shard"), lax.axis_size("expert")
    shard, group = lax.axis_index("shard"), lax.axis_index("expert")
    tokens = inputs.shape[0]
    own_rows = attn_gain.shape[0]
    sequences = tokens // DEVICE_TOKENS
    length = shards * DEVICE_TOKENS
    experts_here = E // groups
    heads = KEY_VALUE_HEADS // shards
    ratio = QUERY_HEADS // KEY_VALUE_HEADS
    query_width, key_width = heads * ratio * HEAD_SIZE, heads * HEAD_SIZE
    scale = 1.0 / HEAD_SIZE

    small = jnp.concatenate([w_router, attn_gain[:, None], moe_gain[:, None]], axis=1)
    small = jnp.pad(small, ((0, 0), (0, LANES - E - 2)))
    qkv_cut = jnp.transpose(
        jnp.concatenate(
            [
                w_query.reshape(own_rows, shards, query_width),
                key_matrix.reshape(own_rows, shards, key_width),
                value_matrix.reshape(own_rows, shards, key_width),
            ],
            axis=2,
        ),
        (1, 0, 2),
    )
    group_inputs, small_all, routes_all, c_all, qkv_own = gathered(
        [
            inputs.reshape(sequences, DEVICE_TOKENS, MODEL_WIDTH),
            small[None],
            jnp.transpose(routes)[None],
            cotangent[None],
        ],
        (False, False, True, True),
        shards,
        groups,
        0,
        [qkv_cut],
    )
    qkv_own = qkv_own.reshape(MODEL_WIDTH, query_width + 2 * key_width)
    r_all = jnp.transpose(routes_all[0], (0, 2, 1))
    c_all = c_all[0]
    small = small_all.reshape(MODEL_WIDTH, LANES)
    router, gain_one, gain_two = small[:, :E], small[:, E].astype(f32), small[:, E + 1].astype(f32)

    group_wide = group_inputs.reshape(sequences * length, MODEL_WIDTH).astype(f32)
    r_group = lax.rsqrt(jnp.mean(group_wide * group_wide, axis=-1, keepdims=True) + EPSILON)
    z_group = group_wide * r_group
    normed = (z_group * gain_one).astype(bf16)
    qkv = jnp.dot(normed, qkv_own, preferred_element_type=f32)
    cosine, sine = angle_tables(jnp.arange(length, dtype=f32))
    q_shape = (sequences, length, heads, ratio, HEAD_SIZE)
    k_shape = (sequences, length, heads, HEAD_SIZE)
    query = rotated(
        qkv[:, :query_width].reshape(q_shape),
        cosine[:, None, None, :],
        sine[:, None, None, :],
    ).astype(bf16)
    keys = rotated(
        qkv[:, query_width : query_width + key_width].reshape(k_shape),
        cosine[:, None, :],
        sine[:, None, :],
    ).astype(bf16)
    values = qkv[:, query_width + key_width :].reshape(k_shape).astype(bf16)
    places = jnp.arange(length, dtype=jnp.int32)
    allowed = places[None, :] <= places[:, None]
    scores = jnp.einsum("nqjgd,nkjd->njgqk", query, keys, preferred_element_type=f32) * scale
    scores = jnp.where(allowed, scores, MASKED)
    top = jnp.max(scores, axis=-1, keepdims=True)
    log_total = top + jnp.log(jnp.sum(jnp.exp(scores - top), axis=-1, keepdims=True))
    probs = jnp.exp(scores - log_total)
    mixed = jnp.einsum(
        "njgqk,nkjd->nqjgd", probs.astype(bf16), values, preferred_element_type=f32
    ).astype(bf16)
    mixed_rows = mixed.reshape(sequences * length, query_width)
    projected = jnp.dot(mixed_rows, w_output, preferred_element_type=f32).astype(bf16)
    line_shape = (sequences, shards, DEVICE_TOKENS, MODEL_WIDTH)
    attended = reduced([projected.reshape(line_shape)], (False,), shards, groups, 1)[0]
    attended = attended.reshape(tokens, MODEL_WIDTH)
    inputs_wide = inputs.astype(f32)
    h_one = inputs_wide + attended
    r_two = lax.rsqrt(jnp.mean(h_one * h_one, axis=-1, keepdims=True) + EPSILON)
    z_two = h_one * r_two
    n_two = (z_two * gain_two).astype(bf16)

    blocks = groups * shards
    n_all, experts_own = gathered(
        [n_two[None]], (True,), shards, groups, 2, [packed_experts(w_experts, shards)]
    )
    n_all = n_all[0]
    experts_own = experts_own.reshape(MODEL_WIDTH, -1)

    def weights_of(rows, picks_of):
        logits = jnp.einsum("...d,de->...e", rows, router, preferred_element_type=f32)
        picks = (picks_of[..., None] == jnp.arange(E, dtype=jnp.int32)).astype(f32)
        chosen = jnp.sum(picks * logits[..., None, :], axis=-1)
        return jax.nn.softmax(chosen, axis=-1), picks

    w_all, _ = weights_of(n_all, r_all)
    whole, extra = divmod(experts_here, shards)
    owned = [(group * experts_here + shard * whole + i, i * 3 * FF, FF) for i in range(whole)]
    if extra:
        cuts = shards // extra
        owned.append(
            (group * experts_here + whole * shards + shard // cuts, whole * 3 * FF, FF // cuts)
        )
    slots = -(-CAP // 8) * 8
    lower = (jnp.arange(tokens)[:, None] <= jnp.arange(tokens)[None, :]).astype(bf16)
    picked, slot_weights = [], []
    for expert, _, _ in owned:
        hit = jnp.any(r_all == expert, axis=-1)
        rank = jnp.einsum("bt,tu->bu", hit.astype(bf16), lower, preferred_element_type=f32)
        place = jnp.where(hit, rank.astype(jnp.int32) - 1, -1)
        pick = place[:, None, :] == jnp.arange(slots, dtype=jnp.int32)[None, :, None]
        weight = jnp.sum(jnp.where(r_all == expert, w_all, 0.0), axis=-1)
        picked.append(pick)
        slot_weights.append(jnp.sum(jnp.where(pick, weight[:, None, :], 0.0), axis=-1))
    selection = jnp.concatenate(picked, axis=1).astype(bf16)
    n_sent = jnp.einsum("bct,btd->bcd", selection, n_all, preferred_element_type=f32).astype(bf16)
    c_sent = jnp.einsum("bct,btd->bcd", selection, c_all, preferred_element_type=f32).astype(bf16)
    produced, d_rows, grads = [], [], []
    d_weights = jnp.zeros((blocks, tokens, TOP), f32)
    for i, (expert, start, width) in enumerate(owned):
        a = n_sent[:, i * slots : (i + 1) * slots].reshape(blocks * slots, MODEL_WIDTH)
        c = c_sent[:, i * slots : (i + 1) * slots].reshape(blocks * slots, MODEL_WIDTH)
        gate_up = experts_own[:, start : start + 2 * width]
        down = experts_own[:, start + 2 * width : start + 3 * width]
        both_parts = jnp.dot(a, gate_up, preferred_element_type=f32)
        d_plain = jnp.dot(c, down, preferred_element_type=f32)
        gate, up = both_parts[:, :width], both_parts[:, width:]
        sig = jax.nn.sigmoid(gate)
        act = gate * sig * up
        w = slot_weights[i].reshape(-1, 1)
        d_slot = jnp.sum(act * d_plain, axis=-1).reshape(blocks, slots)
        d_token = jnp.sum(jnp.where(picked[i], d_slot[:, :, None], 0.0), axis=1)
        d_weights = d_weights + jnp.where(r_all == expert, d_token[:, :, None], 0.0)
        act_w = (act * w).astype(bf16)
        da = d_plain * w
        d_gu = jnp.concatenate(
            [da * up * sig * (1.0 + gate * (1.0 - sig)), da * gate * sig], axis=1
        ).astype(bf16)
        produced.append(
            jnp.einsum("rf,df->rd", act_w, down, preferred_element_type=f32)
            .astype(bf16)
            .reshape(blocks, slots, MODEL_WIDTH)
        )
        d_rows.append(
            jnp.einsum("rf,df->rd", d_gu, gate_up, preferred_element_type=f32)
            .astype(bf16)
            .reshape(blocks, slots, MODEL_WIDTH)
        )
        grads.append(jnp.einsum("rd,rf->df", a, d_gu, preferred_element_type=f32))
        grads.append(jnp.einsum("rd,rf->df", c, act_w, preferred_element_type=f32))
    d_sums = jnp.einsum(
        "bct,bcd->btd", selection, jnp.concatenate(d_rows, axis=1), preferred_element_type=f32
    ).astype(bf16)
    high = d_weights.astype(bf16)
    low = (d_weights - high.astype(f32)).astype(bf16)
    pad_rows = 16
    carried = jnp.stack([high, low], axis=1).reshape(blocks, 2, tokens * TOP)
    carried = jnp.pad(carried, ((0, 0), (0, pad_rows - 2), (0, MODEL_WIDTH - tokens * TOP)))
    grads = jnp.concatenate(grads, axis=1).astype(bf16).reshape(shards, own_rows, -1)
    back, grads = reduced(
        [jnp.concatenate([d_sums, carried], axis=1)[None]], (True,), shards, groups, 3, [grads]
    )
    back = back[0]
    grad_experts = unpacked_experts(grads, experts_here).astype(f32)
    o_sums = jnp.einsum(
        "bct,bcd->btd", selection, jnp.concatenate(produced, axis=1), preferred_element_type=f32
    ).astype(bf16)

    weights, picks = weights_of(n_two, routes)
    carried_back = back[tokens : tokens + 2, : tokens * TOP]
    d_weights = (carried_back[0] + carried_back[1]).reshape(tokens, TOP)
    d_chosen = weights * (d_weights - jnp.sum(weights * d_weights, axis=-1, keepdims=True))
    d_logits = jnp.sum(picks * d_chosen[:, :, None], axis=1).astype(bf16)
    grad_router = jnp.einsum("td,te->de", n_two, d_logits, preferred_element_type=f32)
    d_n_two = jnp.einsum("te,de->td", d_logits, router, preferred_element_type=f32) + back[
        :tokens
    ]
    grad_gain_two = jnp.sum(d_n_two * z_two, axis=0)
    dz_two = d_n_two * gain_two
    dh_one = cotangent.astype(f32) + r_two * (
        dz_two - z_two * jnp.mean(dz_two * z_two, axis=-1, keepdims=True)
    )

    dh_group = gathered(
        [dh_one.astype(bf16).reshape(sequences, DEVICE_TOKENS, MODEL_WIDTH)],
        (False,),
        shards,
        groups,
        4,
    )[0].reshape(sequences * length, MODEL_WIDTH)
    grad_output = jnp.einsum("tk,td->kd", mixed_rows, dh_group, preferred_element_type=f32)
    d_mixed = (
        jnp.einsum("td,kd->tk", dh_group, w_output, preferred_element_type=f32)
        .astype(bf16)
        .reshape(q_shape)
    )
    delta = jnp.sum(d_mixed.astype(f32) * mixed.astype(f32), axis=-1)
    delta = jnp.transpose(delta, (0, 2, 3, 1))[..., None]
    d_probs = jnp.einsum("nqjgd,nkjd->njgqk", d_mixed, values, preferred_element_type=f32)
    d_scores = (probs * (d_probs - delta)).astype(bf16)
    d_query = jnp.einsum("njgqk,nkjd->nqjgd", d_scores, keys, preferred_element_type=f32) * scale
    d_keys = jnp.einsum("njgqk,nqjgd->nkjd", d_scores, query, preferred_element_type=f32) * scale
    d_values = jnp.einsum(
        "njgqk,nqjgd->nkjd", probs.astype(bf16), d_mixed, preferred_element_type=f32
    )
    d_qkv = jnp.concatenate(
        [
            rotated(d_query, cosine[:, None, None, :], -sine[:, None, None, :])
            .astype(bf16)
            .reshape(sequences * length, query_width),
            rotated(d_keys, cosine[:, None, :], -sine[:, None, :])
            .astype(bf16)
            .reshape(sequences * length, key_width),
            d_values.astype(bf16).reshape(sequences * length, key_width),
        ],
        axis=1,
    )
    d_normed = jnp.einsum("tk,dk->td", d_qkv, qkv_own, preferred_element_type=f32)
    grad_gain_one = jnp.sum(d_normed * z_group, axis=0)
    grad_qkv = jnp.einsum("td,tk->dk", normed, d_qkv, preferred_element_type=f32)
    grad_small = jnp.concatenate(
        [grad_router, grad_gain_one[:, None], grad_gain_two[:, None]], axis=1
    ).astype(bf16)
    grad_small = jnp.pad(grad_small, ((0, 0), (0, LANES - E - 2)))
    d_n_one, grad_small, moe_sum, grad_qkv = reduced(
        [
            d_normed.astype(bf16).reshape(line_shape),
            grad_small.reshape(1, shards, own_rows, LANES),
            o_sums[None],
        ],
        (False, False, True),
        shards,
        groups,
        5,
        [grad_qkv.astype(bf16).reshape(shards, own_rows, -1)],
    )
    d_n_one = d_n_one.reshape(tokens, MODEL_WIDTH)
    outputs = (h_one + moe_sum[0]).astype(bf16)
    grad_qkv, grad_output, grad_small = lax.psum(
        (grad_qkv, grad_output.astype(bf16), grad_small[0].astype(bf16)), "expert"
    )
    grad_small = grad_small.astype(f32)

    def columns(start, width):
        part = jnp.transpose(grad_qkv[:, :, start : start + width], (1, 0, 2))
        return part.reshape(own_rows, shards * width).astype(f32)

    r_one = lax.rsqrt(jnp.mean(inputs_wide * inputs_wide, axis=-1, keepdims=True) + EPSILON)
    z_one = inputs_wide * r_one
    dz_one = d_n_one * gain_one
    grad_inputs = dh_one + r_one * (
        dz_one - z_one * jnp.mean(dz_one * z_one, axis=-1, keepdims=True)
    )
    return (
        outputs,
        grad_inputs,
        grad_small[:, E],
        columns(0, query_width),
        columns(query_width, key_width),
        columns(query_width + key_width, key_width),
        grad_output.astype(f32),
        grad_small[:, E + 1],
        grad_small[:, :E],
        grad_experts,
    )


def solution(mesh):
    fits = divides(mesh.shape["shard"], mesh.shape["expert"])
    return jax.shard_map(
        local if fits else general,
        mesh=mesh,
        in_specs=(
            P(("expert", "shard"), None),
            P(("expert", "shard"), None),
            P(("expert", "shard"), None),
            P("shard"),
            P("shard", None),
            P("shard", None),
            P("shard", None),
            P("shard", None),
            P("shard"),
            P("shard", None),
            P("shard", "expert", None),
        ),
        out_specs=(
            P(("expert", "shard"), None),
            P(("expert", "shard"), None),
            P("shard"),
            P("shard", None),
            P("shard", None),
            P("shard", None),
            P("shard", None),
            P("shard"),
            P("shard", None),
            P("shard", "expert", None),
        ),
        check_vma=False,
    )
```

```python
import functools

import jax
import jax.numpy as jnp
from jax import lax
from jax.experimental import pallas as pl
from jax.experimental.pallas import tpu as pltpu
from jax.sharding import PartitionSpec as P

MODEL_WIDTH = 1536
QUERY_HEADS = 24
KEY_VALUE_HEADS = 8
HEAD_SIZE = 64
FF = 512
E = 40
TOP = 8
DEVICE_TOKENS = 64
CAP = 38


EPSILON = 1e-06
ROPE_BASE = 10000.0
MASKED = -1e30
LANES = 128


def angle_tables(positions):
    half_width = HEAD_SIZE // 2
    frequency = jnp.power(
        ROPE_BASE, -(jnp.arange(half_width, dtype=jnp.float32) * (2.0 / HEAD_SIZE))
    )
    angles = positions[:, None] * frequency[None, :]
    return (jnp.cos(angles), jnp.sin(angles))


def apply_rotation(values, cosine_table, sines_table):
    half_width = values.shape[-1] // 2
    first_half, second_half = (values[..., :half_width], values[..., half_width:])
    cosine_table, sines_table = (cosine_table[:, None, :], sines_table[:, None, :])
    return jnp.concatenate(
        [
            first_half * cosine_table - second_half * sines_table,
            second_half * cosine_table + first_half * sines_table,
        ],
        axis=-1,
    )


def reverse_rotation(values, cosine_table, sines_table):
    half_width = values.shape[-1] // 2
    first_half, second_half = (values[..., :half_width], values[..., half_width:])
    cosine_table, sines_table = (cosine_table[:, None, :], sines_table[:, None, :])
    return jnp.concatenate(
        [
            first_half * cosine_table + second_half * sines_table,
            second_half * cosine_table - first_half * sines_table,
        ],
        axis=-1,
    )


def general(
    inputs,
    cotangent,
    routes,
    attn_gain,
    w_query,
    key_matrix,
    value_matrix,
    w_output,
    moe_gain,
    w_router,
    w_experts,
):
    rows_local = inputs.shape[0]
    group_count = lax.axis_size("expert")
    experts_here = E // group_count
    group_width = QUERY_HEADS // KEY_VALUE_HEADS
    key_value_width = KEY_VALUE_HEADS * HEAD_SIZE
    scale_factor = 1.0 / HEAD_SIZE
    sequence_count = rows_local // DEVICE_TOKENS
    gain_one, query_full, key_complete, value_full, output_full, router_full, gain_two = (
        lax.all_gather(attn_gain, "shard", axis=0, tiled=True),
        lax.all_gather(w_query, "shard", axis=0, tiled=True),
        lax.all_gather(key_matrix, "shard", axis=0, tiled=True),
        lax.all_gather(value_matrix, "shard", axis=0, tiled=True),
        lax.all_gather(w_output, "shard", axis=0, tiled=True),
        lax.all_gather(w_router, "shard", axis=0, tiled=True),
        lax.all_gather(moe_gain, "shard", axis=0, tiled=True),
    )
    inputs_wide = inputs.astype(jnp.float32)
    r_one = lax.rsqrt(jnp.mean(inputs_wide * inputs_wide, axis=-1, keepdims=True) + EPSILON)
    z_one = inputs_wide * r_one
    normed_first = (z_one * gain_one.astype(jnp.float32)).astype(jnp.bfloat16)
    offset = lax.axis_index("shard") * DEVICE_TOKENS
    positions = offset + jnp.arange(DEVICE_TOKENS, dtype=jnp.int32)
    row_positions = jnp.tile(positions, sequence_count)
    cosine_table, sines_table = angle_tables(row_positions.astype(jnp.float32))
    query_rotated = apply_rotation(
        jnp.dot(normed_first, query_full, preferred_element_type=jnp.float32).reshape(
            rows_local, QUERY_HEADS, HEAD_SIZE
        ),
        cosine_table,
        sines_table,
    ).astype(jnp.bfloat16)
    keys_rot = apply_rotation(
        jnp.dot(normed_first, key_complete, preferred_element_type=jnp.float32).reshape(
            rows_local, KEY_VALUE_HEADS, HEAD_SIZE
        ),
        cosine_table,
        sines_table,
    ).astype(jnp.bfloat16)
    values_narrow = jnp.dot(normed_first, value_full, preferred_element_type=jnp.float32).astype(
        jnp.bfloat16
    )
    kv_local = jnp.concatenate(
        [keys_rot.reshape(rows_local, key_value_width), values_narrow], axis=1
    ).reshape(sequence_count, DEVICE_TOKENS, 2 * key_value_width)
    kv_all = lax.all_gather(kv_local, "shard", axis=1, tiled=True)
    seq_length = kv_all.shape[1]
    block_of_keys = min(512, seq_length)
    total_of_block = (offset + DEVICE_TOKENS + block_of_keys - 1) // block_of_keys
    query_four_dims = query_rotated.reshape(
        sequence_count, DEVICE_TOKENS, KEY_VALUE_HEADS, group_width, HEAD_SIZE
    )

    def scores_for(block_index):
        start_row = block_index * block_of_keys
        key_value_slice = lax.dynamic_slice_in_dim(kv_all, start_row, block_of_keys, 1)
        keys_block = key_value_slice[..., :key_value_width].reshape(
            sequence_count, block_of_keys, KEY_VALUE_HEADS, HEAD_SIZE
        )
        values_block = key_value_slice[..., key_value_width:].reshape(
            sequence_count, block_of_keys, KEY_VALUE_HEADS, HEAD_SIZE
        )
        scores = (
            jnp.einsum(
                "nqjgd,nkjd->njgqk", query_four_dims, keys_block, preferred_element_type=jnp.float32
            )
            * scale_factor
        )
        key_pos = start_row + jnp.arange(block_of_keys, dtype=jnp.int32)
        allowed = key_pos[None, :] <= positions[:, None]
        return (jnp.where(allowed, scores, MASKED), keys_block, values_block)

    def stats_step(block_index, loop_state):
        running_max, running_sum = loop_state
        scores = scores_for(block_index)[0]
        new_max = jnp.maximum(running_max, jnp.max(scores, axis=-1))
        running_sum = running_sum * jnp.exp(running_max - new_max) + jnp.sum(
            jnp.exp(scores - new_max[..., None]), axis=-1
        )
        return (new_max, running_sum)

    statistics_shape = (sequence_count, KEY_VALUE_HEADS, group_width, DEVICE_TOKENS)
    start_stats = (
        jnp.full(statistics_shape, MASKED, jnp.float32),
        jnp.zeros(statistics_shape, jnp.float32),
    )
    run_max, run_sum = lax.fori_loop(0, total_of_block, stats_step, start_stats)
    log_total = run_max + jnp.log(run_sum)

    def mixing_step(block_index, mixed_sum):
        scores, keys_block, values_block = scores_for(block_index)
        attn_probs = jnp.exp(scores - log_total[..., None]).astype(jnp.bfloat16)
        return mixed_sum + jnp.einsum(
            "njgqk,nkjd->nqjgd", attn_probs, values_block, preferred_element_type=jnp.float32
        )

    attention_mixed = lax.fori_loop(
        0,
        total_of_block,
        mixing_step,
        jnp.zeros(
            (sequence_count, DEVICE_TOKENS, KEY_VALUE_HEADS, group_width, HEAD_SIZE), jnp.float32
        ),
    )
    attention_mixed = attention_mixed.reshape(rows_local, QUERY_HEADS * HEAD_SIZE).astype(
        jnp.bfloat16
    )
    h_one = inputs_wide + jnp.dot(attention_mixed, output_full, preferred_element_type=jnp.float32)
    r_two = lax.rsqrt(jnp.mean(h_one * h_one, axis=-1, keepdims=True) + EPSILON)
    z_two = h_one * r_two
    n_two = (z_two * gain_two.astype(jnp.float32)).astype(jnp.bfloat16)
    logits = jnp.dot(n_two, router_full, preferred_element_type=jnp.float32)
    expert_ids = jnp.arange(E, dtype=jnp.int32)
    route_picks = (routes[:, :, None] == expert_ids[None, None, :]).astype(jnp.float32)
    chosen = jnp.sum(route_picks * logits[:, None, :], axis=-1)
    weights = jax.nn.softmax(chosen, axis=-1)
    flat_routes = routes.reshape(-1)
    route_hits = (flat_routes[:, None] == expert_ids[None, :]).astype(jnp.int32)
    route_ranks = jnp.sum(jnp.cumsum(route_hits, axis=0) * route_hits, axis=1) - 1
    targets = flat_routes * CAP + route_ranks
    token_of = jnp.arange(rows_local * TOP, dtype=jnp.int32) // TOP
    outgoing = jnp.zeros((E * CAP, MODEL_WIDTH), jnp.bfloat16).at[targets].set(n_two[token_of])
    arrived = lax.all_to_all(
        outgoing.reshape(group_count, experts_here, CAP, MODEL_WIDTH),
        "expert",
        split_axis=0,
        concat_axis=0,
        tiled=True,
    )
    expert_full = lax.all_gather(w_experts, "shard", axis=0, tiled=True)
    gate_and_up = expert_full[:, :, : 2 * FF]
    down_part = expert_full[:, :, 2 * FF :]
    both_parts = jnp.einsum(
        "sjcd,djf->sjcf", arrived, gate_and_up, preferred_element_type=jnp.float32
    )
    gate_part = both_parts[..., :FF]
    upper_part = both_parts[..., FF:]
    sigmoid_gate = jax.nn.sigmoid(gate_part)
    activated = (gate_part * sigmoid_gate * upper_part).astype(jnp.bfloat16)
    produced = jnp.einsum(
        "sjcf,djf->sjcd", activated, down_part, preferred_element_type=jnp.float32
    ).astype(jnp.bfloat16)
    returned = lax.all_to_all(produced, "expert", split_axis=0, concat_axis=0, tiled=True).reshape(
        E * CAP, MODEL_WIDTH
    )
    route_out = returned[targets].reshape(rows_local, TOP, MODEL_WIDTH).astype(jnp.float32)
    moe_sum = jnp.sum(weights[:, :, None] * route_out, axis=1)
    outputs = (h_one + moe_sum).astype(jnp.bfloat16)
    dy_wide = cotangent.astype(jnp.float32)
    d_routes = (
        (weights[:, :, None] * dy_wide[:, None, :])
        .astype(jnp.bfloat16)
        .reshape(rows_local * TOP, MODEL_WIDTH)
    )
    d_outgoing = jnp.zeros((E * CAP, MODEL_WIDTH), jnp.bfloat16).at[targets].set(d_routes)
    d_arrived = lax.all_to_all(
        d_outgoing.reshape(group_count, experts_here, CAP, MODEL_WIDTH),
        "expert",
        split_axis=0,
        concat_axis=0,
        tiled=True,
    )
    d_weights = jnp.sum(dy_wide[:, None, :] * route_out, axis=-1)
    d_chosen = weights * (d_weights - jnp.sum(weights * d_weights, axis=-1, keepdims=True))
    d_logits = jnp.sum(route_picks * d_chosen[:, :, None], axis=1).astype(jnp.bfloat16)
    grad_router = jnp.einsum("td,te->de", n_two, d_logits, preferred_element_type=jnp.float32)
    d_act = jnp.einsum("sjcd,djf->sjcf", d_arrived, down_part, preferred_element_type=jnp.float32)
    d_gate_up = jnp.concatenate(
        [
            d_act * upper_part * sigmoid_gate * (1.0 + gate_part * (1.0 - sigmoid_gate)),
            d_act * gate_part * sigmoid_gate,
        ],
        axis=-1,
    ).astype(jnp.bfloat16)
    d_rows = jnp.einsum(
        "sjcf,djf->sjcd", d_gate_up, gate_and_up, preferred_element_type=jnp.float32
    ).astype(jnp.bfloat16)
    d_returned = lax.all_to_all(d_rows, "expert", split_axis=0, concat_axis=0, tiled=True).reshape(
        E * CAP, MODEL_WIDTH
    )
    d_n_two = jnp.einsum(
        "te,de->td", d_logits, router_full, preferred_element_type=jnp.float32
    ) + jnp.sum(
        d_returned[targets].reshape(rows_local, TOP, MODEL_WIDTH).astype(jnp.float32), axis=1
    )
    first_part = jnp.einsum(
        "sjcd,sjcf->djf", arrived, d_gate_up, preferred_element_type=jnp.float32
    )
    second = jnp.einsum("sjcd,sjcf->djf", d_arrived, activated, preferred_element_type=jnp.float32)
    grad_experts = lax.psum_scatter(
        jnp.concatenate([first_part, second], axis=2).astype(jnp.bfloat16),
        "shard",
        scatter_dimension=0,
        tiled=True,
    ).astype(jnp.float32)
    grad_gain_two = jnp.sum(d_n_two * z_two, axis=0)
    dz_two = d_n_two * gain_two.astype(jnp.float32)
    dh_one = dy_wide + r_two * (dz_two - z_two * jnp.mean(dz_two * z_two, axis=-1, keepdims=True))
    dh_narrow = dh_one.astype(jnp.bfloat16)
    grad_output = jnp.einsum(
        "tk,td->kd", attention_mixed, dh_narrow, preferred_element_type=jnp.float32
    )
    mixed_gradient = jnp.einsum(
        "td,kd->tk", dh_narrow, output_full, preferred_element_type=jnp.float32
    ).astype(jnp.bfloat16)
    grad_four_dims = mixed_gradient.reshape(
        sequence_count, DEVICE_TOKENS, KEY_VALUE_HEADS, group_width, HEAD_SIZE
    )
    row_difference = jnp.sum(
        grad_four_dims.astype(jnp.float32)
        * attention_mixed.reshape(
            sequence_count, DEVICE_TOKENS, KEY_VALUE_HEADS, group_width, HEAD_SIZE
        ).astype(jnp.float32),
        axis=-1,
    )
    row_difference = jnp.transpose(row_difference, (0, 2, 3, 1))

    def grad_step(block_index, loop_state):
        d_query_sum, d_key_rows = loop_state
        scores, keys_block, values_block = scores_for(block_index)
        attn_probs = jnp.exp(scores - log_total[..., None])
        d_probs = jnp.einsum(
            "nqjgd,nkjd->njgqk", grad_four_dims, values_block, preferred_element_type=jnp.float32
        )
        d_scores = (attn_probs * (d_probs - row_difference[..., None])).astype(jnp.bfloat16)
        d_query_sum = (
            d_query_sum
            + jnp.einsum(
                "njgqk,nkjd->nqjgd", d_scores, keys_block, preferred_element_type=jnp.float32
            )
            * scale_factor
        )
        key_grad = (
            jnp.einsum(
                "njgqk,nqjgd->nkjd", d_scores, query_four_dims, preferred_element_type=jnp.float32
            )
            * scale_factor
        )
        value_grad = jnp.einsum(
            "njgqk,nqjgd->nkjd",
            attn_probs.astype(jnp.bfloat16),
            grad_four_dims,
            preferred_element_type=jnp.float32,
        )
        update = jnp.concatenate(
            [
                key_grad.reshape(sequence_count, block_of_keys, key_value_width),
                value_grad.reshape(sequence_count, block_of_keys, key_value_width),
            ],
            axis=2,
        )
        d_key_rows = lax.dynamic_update_slice_in_dim(
            d_key_rows, update, block_index * block_of_keys, 1
        )
        return (d_query_sum, d_key_rows)

    start_grads = (
        jnp.zeros(
            (sequence_count, DEVICE_TOKENS, KEY_VALUE_HEADS, group_width, HEAD_SIZE), jnp.float32
        ),
        jnp.zeros((sequence_count, seq_length, 2 * key_value_width), jnp.float32),
    )
    d_query_sum, d_key_rows = lax.fori_loop(0, total_of_block, grad_step, start_grads)
    owned_keys = (
        lax.psum_scatter(d_key_rows.astype(jnp.bfloat16), "shard", scatter_dimension=1, tiled=True)
        .astype(jnp.float32)
        .reshape(rows_local, 2 * key_value_width)
    )
    d_query = (
        reverse_rotation(
            d_query_sum.reshape(rows_local, QUERY_HEADS, HEAD_SIZE), cosine_table, sines_table
        )
        .reshape(rows_local, QUERY_HEADS * HEAD_SIZE)
        .astype(jnp.bfloat16)
    )
    key_gradient = (
        reverse_rotation(
            owned_keys[:, :key_value_width].reshape(rows_local, KEY_VALUE_HEADS, HEAD_SIZE),
            cosine_table,
            sines_table,
        )
        .reshape(rows_local, key_value_width)
        .astype(jnp.bfloat16)
    )
    value_gradient = owned_keys[:, key_value_width:].astype(jnp.bfloat16)
    grad_query = jnp.einsum("td,tk->dk", normed_first, d_query, preferred_element_type=jnp.float32)
    grad_key = jnp.einsum(
        "td,tk->dk", normed_first, key_gradient, preferred_element_type=jnp.float32
    )
    grad_value = jnp.einsum(
        "td,tk->dk", normed_first, value_gradient, preferred_element_type=jnp.float32
    )
    d_n_one = (
        jnp.einsum("tk,dk->td", d_query, query_full, preferred_element_type=jnp.float32)
        + jnp.einsum("tk,dk->td", key_gradient, key_complete, preferred_element_type=jnp.float32)
        + jnp.einsum("tk,dk->td", value_gradient, value_full, preferred_element_type=jnp.float32)
    )
    grad_gain_one = jnp.sum(d_n_one * z_one, axis=0)
    dz_one = d_n_one * gain_one.astype(jnp.float32)
    grad_inputs = dh_one + r_one * (
        dz_one - z_one * jnp.mean(dz_one * z_one, axis=-1, keepdims=True)
    )
    totals = (
        lax.psum_scatter(
            grad_gain_one.astype(jnp.bfloat16), "shard", scatter_dimension=0, tiled=True
        ).astype(jnp.float32),
        lax.psum_scatter(
            grad_query.astype(jnp.bfloat16), "shard", scatter_dimension=0, tiled=True
        ).astype(jnp.float32),
        lax.psum_scatter(
            grad_key.astype(jnp.bfloat16), "shard", scatter_dimension=0, tiled=True
        ).astype(jnp.float32),
        lax.psum_scatter(
            grad_value.astype(jnp.bfloat16), "shard", scatter_dimension=0, tiled=True
        ).astype(jnp.float32),
        lax.psum_scatter(
            grad_output.astype(jnp.bfloat16), "shard", scatter_dimension=0, tiled=True
        ).astype(jnp.float32),
        lax.psum_scatter(
            grad_router.astype(jnp.bfloat16), "shard", scatter_dimension=0, tiled=True
        ).astype(jnp.float32),
        lax.psum_scatter(
            grad_gain_two.astype(jnp.bfloat16), "shard", scatter_dimension=0, tiled=True
        ).astype(jnp.float32),
    )
    totals = (
        lax.psum(totals[0].astype(jnp.bfloat16), "expert").astype(jnp.float32),
        lax.psum(totals[1].astype(jnp.bfloat16), "expert").astype(jnp.float32),
        lax.psum(totals[2].astype(jnp.bfloat16), "expert").astype(jnp.float32),
        lax.psum(totals[3].astype(jnp.bfloat16), "expert").astype(jnp.float32),
        lax.psum(totals[4].astype(jnp.bfloat16), "expert").astype(jnp.float32),
        lax.psum(totals[5].astype(jnp.bfloat16), "expert").astype(jnp.float32),
        lax.psum(totals[6].astype(jnp.bfloat16), "expert").astype(jnp.float32),
    )
    return (
        outputs,
        grad_inputs,
        totals[0],
        totals[1],
        totals[2],
        totals[3],
        totals[4],
        totals[6],
        totals[5],
        grad_experts,
    )


def divides(shards, groups):
    experts_here = E // groups
    if groups != 4 or shards % 2 or shards < 4:
        return False
    if KEY_VALUE_HEADS % shards or shards > experts_here:
        return False
    extra = experts_here % shards
    return extra == 0 or (shards % extra == 0 and FF % (shards // extra) == 0)


def rotated(values, cosine, sine):
    half = HEAD_SIZE // 2
    first, second = values[..., :half], values[..., half:]
    return jnp.concatenate([first * cosine - second * sine, second * cosine + first * sine], axis=-1)


def alternating(depth):
    order = []
    low, high = 0, depth - 1
    while low <= high:
        order.append(high)
        if low != high:
            order.append(low)
        low, high = low + 1, high - 1
    return order


def sent(source, target, send, receive, group, shard):
    return pltpu.make_async_remote_copy(
        src_ref=source,
        dst_ref=target,
        send_sem=send,
        recv_sem=receive,
        device_id=(group, shard),
        device_id_type=pl.DeviceIdType.MESH,
    )


class Place:
    def __init__(self, shards, groups):
        self.group, self.shard = lax.axis_index("expert"), lax.axis_index("shard")
        self.shards, self.groups = shards, groups
        self.depth = shards // 2
        self.spot, self.core = self.shard // 2, self.shard % 2
        self.first = self.group + 1 - 2 * (self.group % 2)
        self.second = (self.group + 2) % 4
        self.corner = (self.first + 2) % 4
        self.partner = self.shard + 1 - 2 * self.core

    def greet(self, wide, whole_line, corner=False):
        barrier = pltpu.get_barrier_semaphore()

        def signal(group, shard):
            pl.semaphore_signal(
                barrier, inc=1, device_id=(group, shard), device_id_type=pl.DeviceIdType.MESH
            )

        more = (2 if wide else 0) + (1 if corner else 0)
        if wide:
            signal(self.first, self.shard)
            signal(self.second, self.shard)
        if corner:
            signal(self.corner, self.shard)
        if whole_line:
            for i in range(1, self.shards):
                signal(self.group, (self.shard + i) % self.shards)
            pl.semaphore_wait(barrier, more + self.shards - 1)
            return
        signal(self.group, self.partner)
        inside = (self.spot > 0) & (self.spot < self.depth - 1)

        @pl.when(self.spot > 0)
        def _():
            signal(self.group, self.shard - 2)

        @pl.when(self.spot < self.depth - 1)
        def _():
            signal(self.group, self.shard + 2)

        @pl.when(inside)
        def _():
            pl.semaphore_wait(barrier, more + 3)

        @pl.when(jnp.logical_not(inside))
        def _():
            pl.semaphore_wait(barrier, more + 2)


class Exchange:
    @staticmethod
    def scratch(block, dtype, pieces, n):
        dma = pltpu.SemaphoreType.DMA
        return [pltpu.VMEM(block, dtype), dma((2, pieces)), dma((n, pieces)), dma((n, pieces))]

    def __init__(self, at, plan, source, target, stage, own, out, come):
        self.at, self.source, self.target = at, source, target
        self.stage, self.own, self.out, self.come = stage, own, out, come
        self.take, self.give, self.parts = plan.take, plan.give, plan.parts

    def copies(self, i):
        at = self.at
        to = (at.shard + i) % at.shards
        for k, (taken, given) in enumerate(zip(self.take(to), self.give(at.shard))):
            yield sent(
                self.source.at[taken],
                self.target.at[given],
                self.out.at[i, k],
                self.come.at[i, k],
                at.group,
                to,
            )

    def keep(self, way):
        here = self.at.shard
        for k, (taken, given) in enumerate(zip(self.take(here), self.give(here))):
            held = self.stage.at[self.parts[k]]
            if way == 0:
                yield pltpu.make_async_copy(self.source.at[taken], held, self.own.at[0, k])
            else:
                yield pltpu.make_async_copy(held, self.target.at[given], self.own.at[1, k])

    def start(self):
        for copy in self.keep(0):
            copy.start()
        for i in range(self.at.shards - 1, 0, -1):
            for copy in self.copies(i):
                copy.start()
        for copy in self.keep(0):
            copy.wait()
        for copy in self.keep(1):
            copy.start()

    def wait(self):
        for copy in self.keep(1):
            copy.wait()
        for i in range(1, self.at.shards):
            for copy in self.copies(i):
                copy.wait()


class Rows:
    def __init__(self, array):
        self.shape, self.block, self.count = array.shape, array.shape[1:], 1
        self.parts = [...]

    def take(self, i):
        return [i]

    def give(self, me):
        return [me]


class Experts:
    def __init__(self, array, shards, experts_here, back, thirds=(0, 3)):
        self.shards, self.back, self.first = shards, back, thirds[0]
        self.thirds = thirds[1] - thirds[0]
        self.whole, self.extra = divmod(experts_here, shards)
        self.cuts = shards // self.extra if self.extra else 1
        self.width = FF // self.cuts
        rows = array.shape[1]
        held = 3 * (FF * self.whole + (self.width if self.extra else 0))
        moved = held * self.thirds // 3
        self.shape = (experts_here, rows, self.thirds * FF) if back else (shards, rows, held)
        self.block = (rows, moved)
        self.parts = [(slice(None), cut) for cut in self.inside(0, self.thirds)]
        self.count = len(self.parts)

    def inside(self, first, thirds):
        cuts = [
            pl.ds((i * thirds + first) * FF, self.thirds * FF) for i in range(self.whole)
        ]
        if self.extra:
            start = self.whole * thirds * FF
            cuts += [
                pl.ds(start + (first + k) * self.width, self.width) for k in range(self.thirds)
            ]
        return cuts

    def owner(self, i):
        return [(i, slice(None), cut) for cut in self.inside(self.first, 3)]

    def outside(self, i):
        first = 0 if self.back else self.first
        cuts = [
            (i * self.whole + k, slice(None), pl.ds(first * FF, self.thirds * FF))
            for k in range(self.whole)
        ]
        if self.extra:
            expert = self.whole * self.shards + i // self.cuts
            for k in range(self.thirds):
                start = pl.multiple_of((first + k) * FF + i % self.cuts * self.width, 128)
                cuts.append((expert, slice(None), pl.ds(start, self.width)))
        return cuts

    def take(self, i):
        return self.owner(i) if self.back else self.outside(i)

    def give(self, me):
        return self.outside(me) if self.back else self.owner(me)


class Across:
    @staticmethod
    def scratch(shape, dtype):
        block = (shape[0] // 4,) + shape[1:]
        dma = pltpu.SemaphoreType.DMA
        return [pltpu.VMEM((4,) + block, dtype), pltpu.VMEM(block, dtype)] + [
            dma((4,)) for _ in range(4)
        ]

    def __init__(self, at, source, target, held, mine, r_out, r_in, g_out, g_in):
        self.at, self.source, self.target, self.held, self.mine = at, source, target, held, mine
        self.r_out, self.r_in, self.g_out, self.g_in = r_out, r_in, g_out, g_in
        self.size = mine.shape[0]

    def part(self, ref, group):
        return ref.at[pl.ds(group * self.size, self.size)]

    def peer(self, i):
        return (self.at.first, self.at.second, self.at.corner)[i - 1]

    def out(self, i):
        return sent(
            self.part(self.source, self.peer(i)),
            self.held.at[i],
            self.r_out.at[i],
            self.r_in.at[i],
            self.peer(i),
            self.at.shard,
        )

    def back(self, i):
        return sent(
            self.mine,
            self.part(self.target, self.at.group),
            self.g_out.at[i],
            self.g_in.at[i],
            self.peer(i),
            self.at.shard,
        )

    def own(self, way):
        if way == 0:
            here = self.part(self.source, self.at.group)
            return pltpu.make_async_copy(here, self.held.at[0], self.r_in.at[0])
        here = self.part(self.target, self.at.group)
        return pltpu.make_async_copy(self.mine, here, self.g_in.at[0])

    def start(self):
        self.own(0).start()
        for i in (3, 1, 2):
            self.out(i).start()

    def turn(self):
        self.own(0).wait()
        for i in range(1, 4):
            self.out(i).wait_recv()
        total = self.held[0].astype(jnp.float32)
        for i in range(1, 4):
            total = total + self.held[i].astype(jnp.float32)
        self.mine[...] = total.astype(self.mine.dtype)
        self.own(1).start()
        for i in (3, 1, 2):
            self.back(i).start()

    def wait(self):
        self.own(1).wait()
        for i in range(1, 4):
            self.out(i).wait_send()
            self.back(i).wait()


class Gather:
    @staticmethod
    def scratch(array, wide, shards):
        steps = shards // 2 - 1
        marks = 1 + 2 * steps
        dma = pltpu.SemaphoreType.DMA
        turns = 2 if wide else 1
        return [
            dma((1,)),
            dma((2 * steps,)),
            dma((2 * steps,)),
            dma((turns, marks)),
            dma((turns, marks)),
            dma((turns, marks)),
            dma((turns, marks)),
            dma((5 if wide else 1, marks)),
            dma((5 if wide else 1, marks)),
        ]

    def __init__(self, at, wide, block, out, *sems):
        self.at, self.wide, self.block, self.out = at, wide, block, out
        self.own, self.z_out, self.z_in, self.p_out, self.p_in = sems[:5]
        self.h_out, self.h_in, self.c_out, self.c_in = sems[5:]
        self.steps = at.depth - 1
        self.events = [(0, 0)]
        for t in range(self.steps):
            self.events += [(1, t), (2, t)]

    def when(self, event, body):
        kind, t = event
        if kind == 0:
            body()
        elif kind == 1:
            pl.when(self.at.spot - 1 - t >= 0)(body)
        else:
            pl.when(self.at.spot + 1 + t < self.at.depth)(body)

    def origin(self, event):
        kind, t = event
        return self.at.shard + (0, -2 * (t + 1), 2 * (t + 1))[kind]

    def slot(self, group, shard):
        index = group * self.at.shards + shard if self.wide else shard
        return self.out.at[:, index]

    def half(self, ref, which):
        rows = ref.shape[1]
        cut = rows // 32 * 16
        return ref.at[:, pl.ds(0, cut)] if which == 0 else ref.at[:, pl.ds(cut, rows - cut)]

    def line(self, step, direction, shard):
        at = self.at
        k = direction * self.steps + step
        ref = self.slot(at.group, shard)
        source = self.block if step == 0 else ref
        to = at.shard + (2, -2)[direction]
        return sent(source, ref, self.z_out.at[k], self.z_in.at[k], at.group, to)

    def side(self, k, which):
        at, event = self.at, self.events[k]
        ref = self.slot(at.group, self.origin(event))
        source = self.block if event[0] == 0 else ref
        group = (at.first, at.second)[which]
        return sent(source, ref, self.p_out.at[which, k], self.p_in.at[which, k], group, at.shard)

    def turn(self, k, which):
        at = self.at
        shard = self.origin(self.events[k])
        held = self.half(self.slot((at.first, at.second)[which], shard), which)
        group = (at.second, at.first)[which]
        return sent(held, held, self.h_out.at[which, k], self.h_in.at[which, k], group, at.shard)

    def across(self, k, kind):
        at, event = self.at, self.events[k]
        shard = self.origin(event)
        if kind < 3:
            ref = self.slot((at.group, at.first, at.second)[kind], shard)
        else:
            ref = self.half(self.slot(at.corner, shard), kind - 3)
        source = self.block if kind == 0 and event[0] == 0 else ref
        return sent(
            source, ref, self.c_out.at[kind, k], self.c_in.at[kind, k], at.group, at.partner
        )

    def keep(self):
        here = self.slot(self.at.group, self.at.shard)
        return pltpu.make_async_copy(self.block, here, self.own.at[0])

    def onward(self, event, act):
        kind, t = event
        for direction in range(2):
            if kind and direction != kind - 1:
                continue
            step = 0 if kind == 0 else t + 1
            if step >= self.steps:
                continue
            ahead = self.at.spot < self.at.depth - 1 if direction == 0 else self.at.spot > 0
            pl.when(ahead)(
                lambda step=step, direction=direction: act(
                    self.line(step, direction, self.origin(event))
                )
            )

    def lines(self, k):
        event = self.events[k]

        def body():
            kind, t = event
            if kind:
                self.line(t, kind - 1, self.origin(event)).wait_recv()
            self.onward(event, lambda copy: copy.start())
            if self.wide:
                self.side(k, 0).start()
                self.side(k, 1).start()
            self.across(k, 0).start()
            if kind == 0:
                self.keep().start()

        self.when(event, body)

    def sides(self, k):
        def body():
            for which in range(2):
                self.side(k, which).wait_recv()
                self.turn(k, which).start()
                self.across(k, 1 + which).start()

        if self.wide:
            self.when(self.events[k], body)

    def turns(self, k):
        def body():
            for which in range(2):
                self.turn(k, which).wait_recv()
                self.across(k, 3 + which).start()

        if self.wide:
            self.when(self.events[k], body)

    def finish(self, k):
        event = self.events[k]

        def body():
            if event[0] == 0:
                self.keep().wait()
            self.onward(event, lambda copy: copy.wait_send())
            for kind in range(5 if self.wide else 1):
                copy = self.across(k, kind)
                copy.wait_send()
                copy.wait_recv()
            if self.wide:
                for which in range(2):
                    self.side(k, which).wait_send()
                    self.turn(k, which).wait_send()

        self.when(event, body)


class Reduce:
    @staticmethod
    def scratch(parts, wide, shards):
        depth = shards // 2
        block = (parts.shape[0],) + parts.shape[2:]
        kinds = 4 if wide else 1
        dma = pltpu.SemaphoreType.DMA
        out = [
            pltpu.VMEM((kinds, depth) + block, parts.dtype),
            pltpu.VMEM((kinds, depth) + block, parts.dtype),
            pltpu.VMEM((2, depth) + block, parts.dtype),
            dma((kinds, depth)),
            dma((kinds, depth)),
            dma((kinds, depth)),
            dma((2, depth)),
            dma((2, depth)),
        ]
        if wide:
            cut = block[1] // 32 * 16
            out += [
                pltpu.VMEM((depth, block[0], cut, block[2]), parts.dtype),
                pltpu.VMEM((depth, block[0], block[1] - cut, block[2]), parts.dtype),
                pltpu.VMEM((2, depth) + block, parts.dtype),
                dma((2, depth)),
                dma((2, depth)),
                dma((2, depth)),
                dma((2, depth)),
            ]
        return out

    def __init__(self, at, wide, parts, total, *scratch):
        self.at, self.wide, self.parts, self.total = at, wide, parts, total
        self.mine, self.accs, self.z_buf, self.own = scratch[:4]
        self.c_out, self.c_in, self.z_out, self.z_in = scratch[4:8]
        if wide:
            self.h_buf, self.p_buf = scratch[8:10], scratch[10]
            self.h_out, self.h_in, self.p_out, self.p_in = scratch[11:]
        self.order = alternating(at.depth)
        self.kinds = (3, 1, 2, 0) if wide else (0,)
        self.columns = (at.group, at.first, at.second, at.corner)

    def place(self, kind, q, core):
        shard = 2 * q + core
        return self.columns[kind] * self.at.shards + shard if self.wide else shard

    def load(self, kind, q):
        return pltpu.make_async_copy(
            self.parts.at[:, self.place(kind, q, self.at.core)],
            self.mine.at[kind, q],
            self.own.at[kind, q],
        )

    def across(self, kind, q):
        return sent(
            self.parts.at[:, self.place(kind, q, 1 - self.at.core)],
            self.accs.at[kind, q],
            self.c_out.at[kind, q],
            self.c_in.at[kind, q],
            self.at.group,
            self.at.partner,
        )

    def span(self, which):
        rows = self.accs.shape[3]
        cut = rows // 32 * 16
        return pl.ds(0, cut) if which == 0 else pl.ds(cut, rows - cut)

    def turn(self, q, which):
        return sent(
            self.accs.at[3, q, :, self.span(which)],
            self.h_buf[which].at[q],
            self.h_out.at[which, q],
            self.h_in.at[which, q],
            (self.at.first, self.at.second)[which],
            self.at.shard,
        )

    def side(self, q, which):
        return sent(
            self.accs.at[1 + which, q],
            self.p_buf.at[which, q],
            self.p_out.at[which, q],
            self.p_in.at[which, q],
            (self.at.first, self.at.second)[which],
            self.at.shard,
        )

    def line(self, q, direction):
        return sent(
            self.accs.at[0, q],
            self.z_buf.at[direction, q],
            self.z_out.at[direction, q],
            self.z_in.at[direction, q],
            self.at.group,
            self.at.shard + (2, -2)[direction],
        )

    def add(self, kind, q, *others):
        value = self.accs[kind, q].astype(jnp.float32)
        for other in others:
            value = value + other.astype(jnp.float32)
        self.accs[kind, q] = value.astype(self.accs.dtype)

    def pair(self, kind, q):
        self.load(kind, q).wait()
        self.across(kind, q).wait_recv()
        self.add(kind, q, self.mine[kind, q])

    def begin(self):
        for kind in self.kinds:
            for q in self.order:
                self.load(kind, q).start()
                self.across(kind, q).start()

    def corners(self):
        for q in self.order:
            self.pair(3, q)
            self.turn(q, 0).start()
            self.turn(q, 1).start()

    def sides(self):
        for q in self.order:
            for which in range(2):
                kind = 2 - which
                self.pair(kind, q)
                self.turn(q, which).wait_recv()
                span = self.span(which)
                value = self.accs[kind, q, :, span].astype(jnp.float32)
                value = value + self.h_buf[which][q].astype(jnp.float32)
                self.accs[kind, q, :, span] = value.astype(self.accs.dtype)
                self.side(q, kind - 1).start()

    def lines(self, q):
        at = self.at
        self.pair(0, q)
        if self.wide:
            self.side(q, 0).wait_recv()
            self.side(q, 1).wait_recv()
            self.add(0, q, self.p_buf[0, q], self.p_buf[1, q])
        for direction in range(2):

            @pl.when(q > at.spot if direction == 0 else q < at.spot)
            def _(direction=direction):
                @pl.when(at.spot > 0 if direction == 0 else at.spot < at.depth - 1)
                def _():
                    self.line(q, direction).wait_recv()
                    self.add(0, q, self.z_buf[direction, q])

                self.line(q, direction).start()

    def finish(self):
        at, total = self.at, self.total
        for q in range(at.depth):

            @pl.when(q == at.spot)
            def _(q=q):
                total[...] = self.accs[0, q].astype(jnp.float32)
                for direction in range(2):
                    if q > 0 if direction == 0 else q < at.depth - 1:
                        self.line(q, direction).wait_recv()
                        total[...] = total[...] + self.z_buf[direction, q].astype(jnp.float32)

            for kind in self.kinds:
                self.across(kind, q).wait_send()
            if self.wide:
                for which in range(2):
                    self.turn(q, which).wait_send()
                    self.side(q, which).wait_send()
            for direction in range(2):

                @pl.when(q > at.spot if direction == 0 else q < at.spot)
                def _(q=q, direction=direction):
                    self.line(q, direction).wait_send()


def cut_refs(refs, sizes):
    out, start = [], 0
    for size in sizes:
        out.append(refs[start : start + size])
        start += size
    return out


def gather_body(shards, groups, wides, plans, sizes, *refs):
    count = len(wides) + len(plans)
    ins, outs = refs[:count], refs[count : 2 * count]
    scratch = cut_refs(refs[2 * count :], sizes)
    at = Place(shards, groups)
    at.greet(any(wides), len(plans) > 0)
    gathers = [Gather(at, wide, ins[i], outs[i], *scratch[i]) for i, wide in enumerate(wides)]
    moves = [
        Exchange(at, plan, ins[i], outs[i], *scratch[i])
        for i, plan in enumerate(plans, len(wides))
    ]
    marks = range(len(gathers[0].events))
    for k in marks:
        for g in gathers:
            g.lines(k)
    for m in moves:
        m.start()
    for step in (Gather.sides, Gather.turns, Gather.finish):
        for k in marks:
            for g in gathers:
                step(g, k)
    for m in moves:
        m.wait()


def gathered(arrays, wides, shards, groups, identity, swapped=(), plans=()):
    shapes = [
        jax.ShapeDtypeStruct(
            (a.shape[0], shards * (groups if wide else 1)) + a.shape[1:], a.dtype
        )
        for a, wide in zip(arrays, wides)
    ] + [jax.ShapeDtypeStruct(p.shape, a.dtype) for a, p in zip(swapped, plans)]
    moved = sum(s.size * s.dtype.itemsize for s in shapes)
    scratch = [Gather.scratch(a, wide, shards) for a, wide in zip(arrays, wides)]
    scratch += [Exchange.scratch(p.block, a.dtype, p.count, shards) for a, p in zip(swapped, plans)]
    return pl.pallas_call(
        functools.partial(
            gather_body, shards, groups, tuple(wides), tuple(plans), tuple(len(s) for s in scratch)
        ),
        out_shape=shapes,
        in_specs=[pl.BlockSpec(memory_space=pltpu.VMEM)] * len(arrays)
        + [pl.BlockSpec(memory_space=pl.ANY)] * len(swapped),
        out_specs=[pl.BlockSpec(memory_space=pl.ANY)] * len(shapes),
        scratch_shapes=[s for some in scratch for s in some],
        compiler_params=pltpu.CompilerParams(collective_id=identity, has_side_effects=True),
        cost_estimate=pl.CostEstimate(flops=0, bytes_accessed=20 * moved, transcendentals=0),
    )(*arrays, *swapped)


def halved(array, wide):
    block = array.size // array.shape[1] * array.dtype.itemsize
    return not wide and array.shape[0] == 2 and block > 200_000


def reduce_body(shards, groups, wides, halves, plans, sums, sizes, *refs):
    given = len(wides) + len(plans)
    count = given + sum(1 for kind, _ in sums if kind == "in")
    results = given + len(sums)
    ins, outs = refs[:count], refs[count : count + results]
    scratch = cut_refs(refs[count + results :], sizes)
    at = Place(shards, groups)
    at.greet(any(wides) or len(sums) > 0, len(plans) > 0, len(sums) > 0)
    reductions = []
    for i, wide in enumerate(wides):
        if halves[i]:
            for j in range(2):
                half = pl.ds(j, 1)
                reductions.append(
                    Reduce(at, wide, ins[i].at[half], outs[i].at[half], *scratch.pop(0))
                )
        else:
            reductions.append(Reduce(at, wide, ins[i], outs[i], *scratch.pop(0)))
    moves = [
        Exchange(at, plan, ins[i], outs[i], *scratch.pop(0))
        for i, plan in enumerate(plans, len(wides))
    ]
    totals = []
    for i, (kind, which) in enumerate(sums, given):
        source = {"in": ins, "sum": outs, "swap": outs}[kind]
        source = source[which + (0 if kind == "sum" else given if kind == "in" else len(wides))]
        totals.append(Across(at, source, outs[i], *scratch.pop(0)))
    flat = [r for r in reductions if not r.wide]
    wide_ones = [r for r in reductions if r.wide]
    order = reductions[0].order
    late = [i for i in range(len(moves)) if flat and ("swap", i) not in sums]

    def swapped_sums():
        for (kind, which), s in zip(sums, totals):
            if kind == "swap":
                moves[which].wait()
                s.start()

    for r in reductions:
        r.begin()
    for i, m in enumerate(moves):
        if i not in late:
            m.start()
    for (kind, _), s in zip(sums, totals):
        if kind == "in":
            s.start()
    for r in wide_ones:
        r.corners()
    for step, q in enumerate(order):
        for r in flat:
            r.lines(q)
        if step == min(1, len(order) - 1):
            for i in late:
                moves[i].start()
        if step == min(2, len(order) - 1):
            swapped_sums()
    for r in flat:
        r.finish()
    for (kind, _), s in zip(sums, totals):
        if kind == "sum":
            s.start()
    for r in wide_ones:
        r.sides()
    for s in totals:
        s.turn()
    for r in wide_ones:
        for q in order:
            r.lines(q)
    for r in wide_ones:
        r.finish()
    for s in totals:
        s.wait()
    for i, m in enumerate(moves):
        if ("swap", i) not in sums:
            m.wait()


def reduced(arrays, wides, shards, groups, identity, swapped=(), plans=(), sums=(), terms=()):
    shapes = [
        jax.ShapeDtypeStruct((a.shape[0],) + a.shape[2:], jnp.float32) for a in arrays
    ] + [jax.ShapeDtypeStruct(p.shape, a.dtype) for a, p in zip(swapped, plans)]
    for kind, which in sums:
        if kind == "in":
            source = terms[which]
        else:
            source = shapes[which + (0 if kind == "sum" else len(arrays))]
        shapes.append(jax.ShapeDtypeStruct(source.shape, source.dtype))
    operands = (*arrays, *swapped, *terms)
    moved = sum(a.size * a.dtype.itemsize for a in operands)
    halves = tuple(halved(a, wide) for a, wide in zip(arrays, wides))
    scratch = []
    for a, wide, half in zip(arrays, wides, halves):
        block = jax.ShapeDtypeStruct((1,) + a.shape[1:] if half else a.shape, a.dtype)
        scratch += [Reduce.scratch(block, wide, shards)] * (2 if half else 1)
    scratch += [Exchange.scratch(p.block, a.dtype, p.count, shards) for a, p in zip(swapped, plans)]
    scratch += [Across.scratch(a.shape, a.dtype) for a in shapes[len(arrays) + len(swapped) :]]
    return pl.pallas_call(
        functools.partial(
            reduce_body,
            shards,
            groups,
            tuple(wides),
            halves,
            tuple(plans),
            tuple(sums),
            tuple(len(s) for s in scratch),
        ),
        out_shape=shapes,
        in_specs=[pl.BlockSpec(memory_space=pl.ANY)] * len(operands),
        out_specs=[pl.BlockSpec(memory_space=pltpu.VMEM)] * len(arrays)
        + [pl.BlockSpec(memory_space=pl.ANY)] * (len(shapes) - len(arrays)),
        scratch_shapes=[s for some in scratch for s in some],
        compiler_params=pltpu.CompilerParams(
            collective_id=identity, has_side_effects=True, vmem_limit_bytes=64 * 1024 * 1024 - 65536
        ),
        cost_estimate=pl.CostEstimate(flops=0, bytes_accessed=20 * moved, transcendentals=0),
    )(*operands)


PAIR = 256
TILE = 320


def experts_body(
    shape,
    ids,
    routes,
    router,
    n_from,
    c_from,
    w_from,
    y_to,
    d_to,
    g_to,
    rows_n,
    rows_c,
    weights,
    picks,
    slot_w,
    slot_d,
    act_rows,
    gu_rows,
    y_rows,
    d_rows,
    n_buf,
    c_buf,
    y_buf,
    d_buf,
    g_buf,
    n_sem,
    c_sem,
    w_sem,
    y_sem,
    d_sem,
    g_sem,
):
    units, pairs, slots, tokens, extra = shape
    f32, bf16 = jnp.float32, jnp.bfloat16
    whole = 2 * slots
    chunk = weights.shape[0] // w_from.shape[0]

    def bring(p, slot):
        return (
            pltpu.make_async_copy(n_from.at[pl.ds(2 * p, 2)], n_buf.at[slot], n_sem.at[slot]),
            pltpu.make_async_copy(c_from.at[pl.ds(2 * p, 2)], c_buf.at[slot], c_sem.at[slot]),
        )

    def weight_copy(i):
        return pltpu.make_async_copy(
            w_from.at[i], weights.at[pl.ds(i * chunk, chunk)], w_sem.at[i]
        )

    for copy in bring(0, 0):
        copy.start()
    for i in range(w_from.shape[0]):
        weight_copy(i).start()
    row = lax.broadcasted_iota(jnp.int32, (PAIR, PAIR), 0)
    column = lax.broadcasted_iota(jnp.int32, (PAIR, PAIR), 1)
    upto = ((row <= column) & (row // tokens == column // tokens)).astype(bf16)
    names = lax.broadcasted_iota(jnp.int32, (router.shape[0], PAIR), 0)
    lanes = lax.broadcasted_iota(jnp.int32, (1, PAIR), 1)
    places = lax.broadcasted_iota(jnp.int32, (whole, PAIR), 0)
    sixteen = lax.broadcasted_iota(jnp.int32, (16, PAIR), 0)

    def dispatch(p, _):
        slot = p % 2
        for copy in bring(p, slot):
            copy.wait()

        @pl.when(p + 1 < pairs)
        def _():
            for copy in bring(p + 1, 1 - slot):
                copy.start()

        n = n_buf[slot].reshape(PAIR, n_buf.shape[3])
        c = c_buf[slot].reshape(PAIR, c_buf.shape[3])
        named = routes[p]
        logits = lax.dot_general(
            router[...], n, (((1,), (1,)), ((), ())), preferred_element_type=f32
        )
        hit = names == named[0:1]
        for j in range(1, TOP):
            hit = hit | (names == named[j : j + 1])
        masked = jnp.where(hit, logits, MASKED)
        top = jnp.max(masked, axis=0, keepdims=True)
        raised = jnp.where(hit, jnp.exp(masked - top), 0.0)
        share = raised / jnp.sum(raised, axis=0, keepdims=True)
        hits = []
        for u in range(len(units)):
            mine = hit & (names == ids[u])
            hits.append(jnp.sum(jnp.where(mine, 1.0, 0.0), axis=0, keepdims=True))
        both = jnp.zeros((16, PAIR), f32)
        for u in range(len(units)):
            both = jnp.where(sixteen == u, hits[u], both)
        ranks = jnp.dot(both.astype(bf16), upto, preferred_element_type=f32)
        for u in range(len(units)):
            weight = jnp.sum(
                jnp.where(hit & (names == ids[u]), share, 0.0), axis=0, keepdims=True
            )
            place = jnp.where(
                hits[u] > 0.5,
                ranks[u : u + 1].astype(jnp.int32) - 1 + lanes // tokens * slots,
                -1,
            )
            pick = (places == place).astype(f32)
            at = pl.ds(pl.multiple_of(p * whole, 16), whole)
            slot_w[u, at] = jnp.sum(pick * weight, axis=1, keepdims=True)
            pick = pick.astype(bf16)
            picks[u, p] = pick
            rows_n[u, at] = jnp.dot(pick, n, preferred_element_type=f32).astype(bf16)
            rows_c[u, at] = jnp.dot(pick, c, preferred_element_type=f32).astype(bf16)
        return 0

    lax.fori_loop(0, pairs, dispatch, 0)
    for i in range(w_from.shape[0]):
        weight_copy(i).wait()
    turned = (((1,), (1,)), ((), ()))
    summed = (((0,), (0,)), ((), ()))
    for u, (start, width) in enumerate(units):
        gu = pl.ds(start, 2 * width)
        down = pl.ds(start + 2 * width, width)

        def tile(i, _, u=u, start=start, width=width, gu=gu, down=down):
            at = pl.ds(pl.multiple_of(i * TILE, 16), TILE)
            parts = jnp.dot(rows_n[u, at], weights[:, gu], preferred_element_type=f32)
            plain = jnp.dot(rows_c[u, at], weights[:, down], preferred_element_type=f32)
            gate, up = parts[:, :width], parts[:, width:]
            sig = jax.nn.sigmoid(gate)
            act = gate * sig * up
            w = slot_w[u, at]
            slot_d[u, at] = jnp.sum(act * plain, axis=1, keepdims=True)
            act_w = (act * w).astype(bf16)
            da = plain * w
            d_gate = (da * up * sig * (1.0 + gate * (1.0 - sig))).astype(bf16)
            d_up = (da * gate * sig).astype(bf16)
            act_rows[u, at, :width] = act_w
            gu_rows[u, at, :width] = d_gate
            gu_rows[u, at, width : 2 * width] = d_up
            y_rows[u, at] = lax.dot_general(
                act_w, weights[:, down], turned, preferred_element_type=f32
            ).astype(bf16)
            d_rows[u, at] = lax.dot_general(
                gu_rows[u, at, : 2 * width], weights[:, gu], turned, preferred_element_type=f32
            ).astype(bf16)
            return 0

        lax.fori_loop(0, pairs * whole // TILE, tile, 0)

    deep = 256

    def grad_copy(i):
        return pltpu.make_async_copy(
            g_buf.at[pl.ds(i * chunk, chunk)], g_to.at[i], g_sem.at[i]
        )

    def grads(i, _):
        at = pl.ds(pl.multiple_of(i * deep, deep), deep)
        for u, (start, width) in enumerate(units):
            g_buf[at, start : start + 2 * width] = lax.dot_general(
                rows_n[u, :, at], gu_rows[u, :, : 2 * width], summed, preferred_element_type=f32
            ).astype(bf16)
            g_buf[at, start + 2 * width : start + 3 * width] = lax.dot_general(
                rows_c[u, :, at], act_rows[u, :, :width], summed, preferred_element_type=f32
            ).astype(bf16)
        return 0

    lax.fori_loop(0, weights.shape[0] // deep, grads, 0)
    for i in range(g_to.shape[0]):
        grad_copy(i).start()

    def put(p, slot):
        return (
            pltpu.make_async_copy(y_buf.at[slot], y_to.at[pl.ds(2 * p, 2)], y_sem.at[slot]),
            pltpu.make_async_copy(d_buf.at[slot], d_to.at[pl.ds(2 * p, 2)], d_sem.at[slot]),
        )

    d_buf[:, :, tokens:] = jnp.zeros((2, 2, extra, d_buf.shape[3]), bf16)

    def combine(p, _):
        slot = p % 2

        @pl.when(p >= 2)
        def _():
            for copy in put(p - 2, slot):
                copy.wait()

        at = pl.ds(pl.multiple_of(p * whole, 16), whole)
        y = jnp.zeros((PAIR, y_rows.shape[2]), f32)
        d = jnp.zeros((PAIR, y_rows.shape[2]), f32)
        d_w = jnp.zeros((TOP, PAIR), f32)
        for u in range(len(units)):
            pick = picks[u, p]
            y = y + lax.dot_general(pick, y_rows[u, at], summed, preferred_element_type=f32)
            d = d + lax.dot_general(pick, d_rows[u, at], summed, preferred_element_type=f32)
            back = jnp.sum(pick.astype(f32) * slot_d[u, at], axis=0, keepdims=True)
            d_w = d_w + jnp.where(routes[p] == ids[u], back, 0.0)
        high = d_w.astype(bf16)
        low = (d_w - high.astype(f32)).astype(bf16)
        y_buf[slot] = y.astype(bf16).reshape(y_buf.shape[1:])
        d_buf[slot, :, :tokens] = d.astype(bf16).reshape(2, tokens, d.shape[1])
        both = jnp.concatenate([high.astype(f32), low.astype(f32)], axis=0).astype(bf16)
        for i in range(2):
            d_buf[slot, i, tokens:, :tokens] = both[:, i * tokens : (i + 1) * tokens]
        for copy in put(p, slot):
            copy.start()
        return 0

    lax.fori_loop(0, pairs, combine, 0)
    for p in range(pairs - 2, pairs):
        for copy in put(p, p % 2):
            copy.wait()
    for i in range(g_to.shape[0]):
        grad_copy(i).wait()


def experts(ids, routes, router, n_all, c_all, owned, units, slots, extra):
    blocks, tokens, width = n_all.shape
    pairs = blocks // 2
    rows = pairs * 2 * slots
    count = len(units)
    hidden = max(w for _, w in units)
    bf16, f32 = jnp.bfloat16, jnp.float32
    shards, own_rows, columns = owned.shape
    dma = pltpu.SemaphoreType.DMA
    any_space, vmem = pl.BlockSpec(memory_space=pl.ANY), pl.BlockSpec(memory_space=pltpu.VMEM)
    flops = 2 * rows * width * sum(w for _, w in units) * 9
    return pl.pallas_call(
        functools.partial(experts_body, (tuple(units), pairs, slots, tokens, extra)),
        out_shape=[
            jax.ShapeDtypeStruct((blocks, tokens, width), bf16),
            jax.ShapeDtypeStruct((blocks, tokens + extra, width), bf16),
            jax.ShapeDtypeStruct(owned.shape, bf16),
        ],
        in_specs=[pl.BlockSpec(memory_space=pltpu.SMEM), vmem, vmem] + [any_space] * 3,
        out_specs=[any_space] * 3,
        scratch_shapes=[
            pltpu.VMEM((count, rows, width), bf16),
            pltpu.VMEM((count, rows, width), bf16),
            pltpu.VMEM((shards * own_rows, columns), bf16),
            pltpu.VMEM((count, pairs, 2 * slots, PAIR), bf16),
            pltpu.VMEM((count, rows, 1), f32),
            pltpu.VMEM((count, rows, 1), f32),
            pltpu.VMEM((count, rows, hidden), bf16),
            pltpu.VMEM((count, rows, 2 * hidden), bf16),
            pltpu.VMEM((count, rows, width), bf16),
            pltpu.VMEM((count, rows, width), bf16),
            pltpu.VMEM((2, 2, tokens, width), bf16),
            pltpu.VMEM((2, 2, tokens, width), bf16),
            pltpu.VMEM((2, 2, tokens, width), bf16),
            pltpu.VMEM((2, 2, tokens + extra, width), bf16),
            pltpu.VMEM((shards * own_rows, columns), bf16),
            dma((2,)),
            dma((2,)),
            dma((shards,)),
            dma((2,)),
            dma((2,)),
            dma((shards,)),
        ],
        compiler_params=pltpu.CompilerParams(vmem_limit_bytes=67_000_000),
        cost_estimate=pl.CostEstimate(
            flops=flops, bytes_accessed=60 * 1024 * 1024, transcendentals=rows * hidden
        ),
    )(ids, routes, router, n_all, c_all, owned)


def local(
    inputs,
    cotangent,
    routes,
    attn_gain,
    w_query,
    key_matrix,
    value_matrix,
    w_output,
    moe_gain,
    w_router,
    w_experts,
):
    f32, bf16 = jnp.float32, jnp.bfloat16
    both = ("expert", "shard")
    shards, groups = lax.axis_size("shard"), lax.axis_size("expert")
    shard, group = lax.axis_index("shard"), lax.axis_index("expert")
    tokens = inputs.shape[0]
    own_rows = attn_gain.shape[0]
    sequences = tokens // DEVICE_TOKENS
    length = shards * DEVICE_TOKENS
    experts_here = E // groups
    heads = KEY_VALUE_HEADS // shards
    ratio = QUERY_HEADS // KEY_VALUE_HEADS
    query_width, key_width = heads * ratio * HEAD_SIZE, heads * HEAD_SIZE
    scale = 1.0 / HEAD_SIZE

    small = jnp.concatenate([w_router, attn_gain[:, None], moe_gain[:, None]], axis=1)
    small = jnp.pad(small, ((0, 0), (0, LANES - E - 2)))
    qkv_cut = jnp.transpose(
        jnp.concatenate(
            [
                w_query.reshape(own_rows, shards, query_width),
                key_matrix.reshape(own_rows, shards, key_width),
                value_matrix.reshape(own_rows, shards, key_width),
            ],
            axis=2,
        ),
        (1, 0, 2),
    )
    group_inputs, small_all, routes_all, qkv_own = gathered(
        [
            inputs.reshape(sequences, DEVICE_TOKENS, MODEL_WIDTH),
            small[None],
            jnp.transpose(routes)[None],
        ],
        (False, False, True),
        shards,
        groups,
        0,
        [qkv_cut],
        [Rows(qkv_cut)],
    )
    qkv_own = qkv_own.reshape(MODEL_WIDTH, query_width + 2 * key_width)
    small = small_all.reshape(MODEL_WIDTH, LANES)
    router_pad = jnp.where(jnp.arange(LANES) < E, small, 0)
    router, gain_one, gain_two = small[:, :E], small[:, E].astype(f32), small[:, E + 1].astype(f32)

    group_wide = group_inputs.reshape(sequences * length, MODEL_WIDTH).astype(f32)
    r_group = lax.rsqrt(jnp.mean(group_wide * group_wide, axis=-1, keepdims=True) + EPSILON)
    z_group = group_wide * r_group
    normed = (z_group * gain_one).astype(bf16)
    qkv = jnp.dot(normed, qkv_own, preferred_element_type=f32)
    cosine, sine = angle_tables(jnp.arange(length, dtype=f32))
    q_shape = (sequences, length, heads, ratio, HEAD_SIZE)
    k_shape = (sequences, length, heads, HEAD_SIZE)
    query = rotated(
        qkv[:, :query_width].reshape(q_shape),
        cosine[:, None, None, :],
        sine[:, None, None, :],
    ).astype(bf16)
    keys = rotated(
        qkv[:, query_width : query_width + key_width].reshape(k_shape),
        cosine[:, None, :],
        sine[:, None, :],
    ).astype(bf16)
    values = qkv[:, query_width + key_width :].reshape(k_shape).astype(bf16)
    places = jnp.arange(length, dtype=jnp.int32)
    allowed = places[None, :] <= places[:, None]
    scores = jnp.einsum("nqjgd,nkjd->njgqk", query, keys, preferred_element_type=f32) * scale
    scores = jnp.where(allowed, scores, MASKED)
    top = jnp.max(scores, axis=-1, keepdims=True)
    log_total = top + jnp.log(jnp.sum(jnp.exp(scores - top), axis=-1, keepdims=True))
    probs = jnp.exp(scores - log_total)
    mixed = jnp.einsum(
        "njgqk,nkjd->nqjgd", probs.astype(bf16), values, preferred_element_type=f32
    ).astype(bf16)
    mixed_rows = mixed.reshape(sequences * length, query_width)
    projected = jnp.dot(mixed_rows, w_output, preferred_element_type=f32).astype(bf16)
    line_shape = (sequences, shards, DEVICE_TOKENS, MODEL_WIDTH)
    attended = reduced([projected.reshape(line_shape)], (False,), shards, groups, 1)[0]
    attended = attended.reshape(tokens, MODEL_WIDTH)
    inputs_wide = inputs.astype(f32)
    h_one = inputs_wide + attended
    r_two = lax.rsqrt(jnp.mean(h_one * h_one, axis=-1, keepdims=True) + EPSILON)
    z_two = h_one * r_two
    n_two = (z_two * gain_two).astype(bf16)

    blocks = groups * shards
    experts_cut = jnp.transpose(w_experts, (1, 0, 2))
    n_all, c_all, experts_own = gathered(
        [n_two[None], cotangent[None]],
        (True, True),
        shards,
        groups,
        2,
        [experts_cut],
        [Experts(experts_cut, shards, experts_here, False)],
    )
    c_all = c_all[0]
    n_all = n_all[0]

    whole, extra = divmod(experts_here, shards)
    owned = [(group * experts_here + shard * whole + i, i * 3 * FF, FF) for i in range(whole)]
    if extra:
        cuts = shards // extra
        owned.append(
            (group * experts_here + whole * shards + shard // cuts, whole * 3 * FF, FF // cuts)
        )
    slots = -(-CAP // 8) * 8
    routes_pairs = jnp.transpose(
        routes_all.reshape(blocks // 2, 2, TOP, tokens), (0, 2, 1, 3)
    ).reshape(blocks // 2, TOP, 2 * tokens)
    o_sums, d_sums, grads = experts(
        jnp.stack([expert for expert, _, _ in owned]).astype(jnp.int32),
        routes_pairs,
        jnp.transpose(router_pad)[: -(-E // 16) * 16],
        n_all,
        c_all,
        experts_own,
        [(start, width) for _, start, width in owned],
        slots,
        2 * TOP,
    )
    back, moe_sum, gate_up = reduced(
        [d_sums[None], o_sums[None]],
        (True, True),
        shards,
        groups,
        3,
        [grads],
        [Experts(grads, shards, experts_here, True, (0, 2))],
    )
    back = back[0]
    outputs = (h_one + moe_sum[0]).astype(bf16)

    logits = jnp.dot(n_two, router, preferred_element_type=f32)
    picks = (routes[:, :, None] == jnp.arange(E, dtype=jnp.int32)).astype(f32)
    weights = jax.nn.softmax(jnp.sum(picks * logits[:, None, :], axis=-1), axis=-1)
    carried = back[tokens:, :tokens]
    d_weights = jnp.transpose(carried[:TOP] + carried[TOP:])
    d_chosen = weights * (d_weights - jnp.sum(weights * d_weights, axis=-1, keepdims=True))
    d_logits = jnp.sum(picks * d_chosen[:, :, None], axis=1).astype(bf16)
    grad_router = jnp.einsum("td,te->de", n_two, d_logits, preferred_element_type=f32)
    d_n_two = jnp.einsum("te,de->td", d_logits, router, preferred_element_type=f32) + back[
        :tokens
    ]
    grad_gain_two = jnp.sum(d_n_two * z_two, axis=0)
    dz_two = d_n_two * gain_two
    dh_one = cotangent.astype(f32) + r_two * (
        dz_two - z_two * jnp.mean(dz_two * z_two, axis=-1, keepdims=True)
    )

    dh_group = gathered(
        [dh_one.astype(bf16).reshape(sequences, DEVICE_TOKENS, MODEL_WIDTH)],
        (False,),
        shards,
        groups,
        4,
    )[0].reshape(sequences * length, MODEL_WIDTH)
    grad_output = jnp.einsum("tk,td->kd", mixed_rows, dh_group, preferred_element_type=f32)
    d_mixed = (
        jnp.einsum("td,kd->tk", dh_group, w_output, preferred_element_type=f32)
        .astype(bf16)
        .reshape(q_shape)
    )
    delta = jnp.sum(d_mixed.astype(f32) * mixed.astype(f32), axis=-1)
    delta = jnp.transpose(delta, (0, 2, 3, 1))[..., None]
    d_probs = jnp.einsum("nqjgd,nkjd->njgqk", d_mixed, values, preferred_element_type=f32)
    d_scores = (probs * (d_probs - delta)).astype(bf16)
    d_query = jnp.einsum("njgqk,nkjd->nqjgd", d_scores, keys, preferred_element_type=f32) * scale
    d_keys = jnp.einsum("njgqk,nqjgd->nkjd", d_scores, query, preferred_element_type=f32) * scale
    d_values = jnp.einsum(
        "njgqk,nqjgd->nkjd", probs.astype(bf16), d_mixed, preferred_element_type=f32
    )
    d_qkv = jnp.concatenate(
        [
            rotated(d_query, cosine[:, None, None, :], -sine[:, None, None, :])
            .astype(bf16)
            .reshape(sequences * length, query_width),
            rotated(d_keys, cosine[:, None, :], -sine[:, None, :])
            .astype(bf16)
            .reshape(sequences * length, key_width),
            d_values.astype(bf16).reshape(sequences * length, key_width),
        ],
        axis=1,
    )
    d_normed = jnp.einsum("tk,dk->td", d_qkv, qkv_own, preferred_element_type=f32)
    grad_gain_one = jnp.sum(d_normed * z_group, axis=0)
    grad_qkv = jnp.einsum("td,tk->dk", normed, d_qkv, preferred_element_type=f32)
    grad_small = jnp.concatenate(
        [grad_router, grad_gain_one[:, None], grad_gain_two[:, None]], axis=1
    ).astype(bf16)
    grad_small = jnp.pad(grad_small, ((0, 0), (0, LANES - E - 2)))
    grad_qkv = grad_qkv.astype(bf16).reshape(shards, own_rows, -1)
    d_n_one, _, _, down, grad_qkv, grad_small, grad_output = reduced(
        [
            d_normed.astype(bf16).reshape(line_shape),
            jnp.transpose(
                grad_small.reshape(shards, groups, own_rows // groups, LANES), (1, 0, 2, 3)
            ),
        ],
        (False, False),
        shards,
        groups,
        5,
        [grad_qkv, grads],
        [Rows(grad_qkv), Experts(grads, shards, experts_here, True, (2, 3))],
        [("swap", 0), ("sum", 1), ("in", 0)],
        [grad_output.astype(bf16).reshape(groups, own_rows // groups, MODEL_WIDTH)],
    )
    grad_experts = jnp.transpose(jnp.concatenate([gate_up, down], axis=2), (1, 0, 2)).astype(f32)
    grad_output = grad_output.reshape(own_rows, MODEL_WIDTH)
    grad_small = grad_small.reshape(own_rows, LANES)
    d_n_one = d_n_one.reshape(tokens, MODEL_WIDTH)
    grad_small = grad_small.astype(f32)

    def columns(start, width):
        part = jnp.transpose(grad_qkv[:, :, start : start + width], (1, 0, 2))
        return part.reshape(own_rows, shards * width).astype(f32)

    r_one = lax.rsqrt(jnp.mean(inputs_wide * inputs_wide, axis=-1, keepdims=True) + EPSILON)
    z_one = inputs_wide * r_one
    dz_one = d_n_one * gain_one
    grad_inputs = dh_one + r_one * (
        dz_one - z_one * jnp.mean(dz_one * z_one, axis=-1, keepdims=True)
    )
    return (
        outputs,
        grad_inputs,
        grad_small[:, E],
        columns(0, query_width),
        columns(query_width, key_width),
        columns(query_width + key_width, key_width),
        grad_output.astype(f32),
        grad_small[:, E + 1],
        grad_small[:, :E],
        grad_experts,
    )


def solution(mesh):
    fits = divides(mesh.shape["shard"], mesh.shape["expert"])
    return jax.shard_map(
        local if fits else general,
        mesh=mesh,
        in_specs=(
            P(("expert", "shard"), None),
            P(("expert", "shard"), None),
            P(("expert", "shard"), None),
            P("shard"),
            P("shard", None),
            P("shard", None),
            P("shard", None),
            P("shard", None),
            P("shard"),
            P("shard", None),
            P("shard", "expert", None),
        ),
        out_specs=(
            P(("expert", "shard"), None),
            P(("expert", "shard"), None),
            P("shard"),
            P("shard", None),
            P("shard", None),
            P("shard", None),
            P("shard", None),
            P("shard"),
            P("shard", None),
            P("shard", "expert", None),
        ),
        check_vma=False,
    )
```

```python
import functools

import jax
import jax.numpy as jnp
from jax import lax
from jax.experimental import pallas as pl
from jax.experimental.pallas import tpu as pltpu
from jax.sharding import PartitionSpec as P

MODEL_WIDTH = 1536
QUERY_HEADS = 24
KEY_VALUE_HEADS = 8
HEAD_SIZE = 64
FF = 512
E = 40
TOP = 8
DEVICE_TOKENS = 64
CAP = 38


EPSILON = 1e-06
ROPE_BASE = 10000.0
MASKED = -1e30
LANES = 128


def angle_tables(positions):
    half_width = HEAD_SIZE // 2
    frequency = jnp.power(
        ROPE_BASE, -(jnp.arange(half_width, dtype=jnp.float32) * (2.0 / HEAD_SIZE))
    )
    angles = positions[:, None] * frequency[None, :]
    return (jnp.cos(angles), jnp.sin(angles))


def apply_rotation(values, cosine_table, sines_table):
    half_width = values.shape[-1] // 2
    first_half, second_half = (values[..., :half_width], values[..., half_width:])
    cosine_table, sines_table = (cosine_table[:, None, :], sines_table[:, None, :])
    return jnp.concatenate(
        [
            first_half * cosine_table - second_half * sines_table,
            second_half * cosine_table + first_half * sines_table,
        ],
        axis=-1,
    )


def reverse_rotation(values, cosine_table, sines_table):
    half_width = values.shape[-1] // 2
    first_half, second_half = (values[..., :half_width], values[..., half_width:])
    cosine_table, sines_table = (cosine_table[:, None, :], sines_table[:, None, :])
    return jnp.concatenate(
        [
            first_half * cosine_table + second_half * sines_table,
            second_half * cosine_table - first_half * sines_table,
        ],
        axis=-1,
    )


def general(
    inputs,
    cotangent,
    routes,
    attn_gain,
    w_query,
    key_matrix,
    value_matrix,
    w_output,
    moe_gain,
    w_router,
    w_experts,
):
    rows_local = inputs.shape[0]
    group_count = lax.axis_size("expert")
    experts_here = E // group_count
    group_width = QUERY_HEADS // KEY_VALUE_HEADS
    key_value_width = KEY_VALUE_HEADS * HEAD_SIZE
    scale_factor = 1.0 / HEAD_SIZE
    sequence_count = rows_local // DEVICE_TOKENS
    gain_one, query_full, key_complete, value_full, output_full, router_full, gain_two = (
        lax.all_gather(attn_gain, "shard", axis=0, tiled=True),
        lax.all_gather(w_query, "shard", axis=0, tiled=True),
        lax.all_gather(key_matrix, "shard", axis=0, tiled=True),
        lax.all_gather(value_matrix, "shard", axis=0, tiled=True),
        lax.all_gather(w_output, "shard", axis=0, tiled=True),
        lax.all_gather(w_router, "shard", axis=0, tiled=True),
        lax.all_gather(moe_gain, "shard", axis=0, tiled=True),
    )
    inputs_wide = inputs.astype(jnp.float32)
    r_one = lax.rsqrt(jnp.mean(inputs_wide * inputs_wide, axis=-1, keepdims=True) + EPSILON)
    z_one = inputs_wide * r_one
    normed_first = (z_one * gain_one.astype(jnp.float32)).astype(jnp.bfloat16)
    offset = lax.axis_index("shard") * DEVICE_TOKENS
    positions = offset + jnp.arange(DEVICE_TOKENS, dtype=jnp.int32)
    row_positions = jnp.tile(positions, sequence_count)
    cosine_table, sines_table = angle_tables(row_positions.astype(jnp.float32))
    query_rotated = apply_rotation(
        jnp.dot(normed_first, query_full, preferred_element_type=jnp.float32).reshape(
            rows_local, QUERY_HEADS, HEAD_SIZE
        ),
        cosine_table,
        sines_table,
    ).astype(jnp.bfloat16)
    keys_rot = apply_rotation(
        jnp.dot(normed_first, key_complete, preferred_element_type=jnp.float32).reshape(
            rows_local, KEY_VALUE_HEADS, HEAD_SIZE
        ),
        cosine_table,
        sines_table,
    ).astype(jnp.bfloat16)
    values_narrow = jnp.dot(normed_first, value_full, preferred_element_type=jnp.float32).astype(
        jnp.bfloat16
    )
    kv_local = jnp.concatenate(
        [keys_rot.reshape(rows_local, key_value_width), values_narrow], axis=1
    ).reshape(sequence_count, DEVICE_TOKENS, 2 * key_value_width)
    kv_all = lax.all_gather(kv_local, "shard", axis=1, tiled=True)
    seq_length = kv_all.shape[1]
    block_of_keys = min(512, seq_length)
    total_of_block = (offset + DEVICE_TOKENS + block_of_keys - 1) // block_of_keys
    query_four_dims = query_rotated.reshape(
        sequence_count, DEVICE_TOKENS, KEY_VALUE_HEADS, group_width, HEAD_SIZE
    )

    def scores_for(block_index):
        start_row = block_index * block_of_keys
        key_value_slice = lax.dynamic_slice_in_dim(kv_all, start_row, block_of_keys, 1)
        keys_block = key_value_slice[..., :key_value_width].reshape(
            sequence_count, block_of_keys, KEY_VALUE_HEADS, HEAD_SIZE
        )
        values_block = key_value_slice[..., key_value_width:].reshape(
            sequence_count, block_of_keys, KEY_VALUE_HEADS, HEAD_SIZE
        )
        scores = (
            jnp.einsum(
                "nqjgd,nkjd->njgqk", query_four_dims, keys_block, preferred_element_type=jnp.float32
            )
            * scale_factor
        )
        key_pos = start_row + jnp.arange(block_of_keys, dtype=jnp.int32)
        allowed = key_pos[None, :] <= positions[:, None]
        return (jnp.where(allowed, scores, MASKED), keys_block, values_block)

    def stats_step(block_index, loop_state):
        running_max, running_sum = loop_state
        scores = scores_for(block_index)[0]
        new_max = jnp.maximum(running_max, jnp.max(scores, axis=-1))
        running_sum = running_sum * jnp.exp(running_max - new_max) + jnp.sum(
            jnp.exp(scores - new_max[..., None]), axis=-1
        )
        return (new_max, running_sum)

    statistics_shape = (sequence_count, KEY_VALUE_HEADS, group_width, DEVICE_TOKENS)
    start_stats = (
        jnp.full(statistics_shape, MASKED, jnp.float32),
        jnp.zeros(statistics_shape, jnp.float32),
    )
    run_max, run_sum = lax.fori_loop(0, total_of_block, stats_step, start_stats)
    log_total = run_max + jnp.log(run_sum)

    def mixing_step(block_index, mixed_sum):
        scores, keys_block, values_block = scores_for(block_index)
        attn_probs = jnp.exp(scores - log_total[..., None]).astype(jnp.bfloat16)
        return mixed_sum + jnp.einsum(
            "njgqk,nkjd->nqjgd", attn_probs, values_block, preferred_element_type=jnp.float32
        )

    attention_mixed = lax.fori_loop(
        0,
        total_of_block,
        mixing_step,
        jnp.zeros(
            (sequence_count, DEVICE_TOKENS, KEY_VALUE_HEADS, group_width, HEAD_SIZE), jnp.float32
        ),
    )
    attention_mixed = attention_mixed.reshape(rows_local, QUERY_HEADS * HEAD_SIZE).astype(
        jnp.bfloat16
    )
    h_one = inputs_wide + jnp.dot(attention_mixed, output_full, preferred_element_type=jnp.float32)
    r_two = lax.rsqrt(jnp.mean(h_one * h_one, axis=-1, keepdims=True) + EPSILON)
    z_two = h_one * r_two
    n_two = (z_two * gain_two.astype(jnp.float32)).astype(jnp.bfloat16)
    logits = jnp.dot(n_two, router_full, preferred_element_type=jnp.float32)
    expert_ids = jnp.arange(E, dtype=jnp.int32)
    route_picks = (routes[:, :, None] == expert_ids[None, None, :]).astype(jnp.float32)
    chosen = jnp.sum(route_picks * logits[:, None, :], axis=-1)
    weights = jax.nn.softmax(chosen, axis=-1)
    flat_routes = routes.reshape(-1)
    route_hits = (flat_routes[:, None] == expert_ids[None, :]).astype(jnp.int32)
    route_ranks = jnp.sum(jnp.cumsum(route_hits, axis=0) * route_hits, axis=1) - 1
    targets = flat_routes * CAP + route_ranks
    token_of = jnp.arange(rows_local * TOP, dtype=jnp.int32) // TOP
    outgoing = jnp.zeros((E * CAP, MODEL_WIDTH), jnp.bfloat16).at[targets].set(n_two[token_of])
    arrived = lax.all_to_all(
        outgoing.reshape(group_count, experts_here, CAP, MODEL_WIDTH),
        "expert",
        split_axis=0,
        concat_axis=0,
        tiled=True,
    )
    expert_full = lax.all_gather(w_experts, "shard", axis=0, tiled=True)
    gate_and_up = expert_full[:, :, : 2 * FF]
    down_part = expert_full[:, :, 2 * FF :]
    both_parts = jnp.einsum(
        "sjcd,djf->sjcf", arrived, gate_and_up, preferred_element_type=jnp.float32
    )
    gate_part = both_parts[..., :FF]
    upper_part = both_parts[..., FF:]
    sigmoid_gate = jax.nn.sigmoid(gate_part)
    activated = (gate_part * sigmoid_gate * upper_part).astype(jnp.bfloat16)
    produced = jnp.einsum(
        "sjcf,djf->sjcd", activated, down_part, preferred_element_type=jnp.float32
    ).astype(jnp.bfloat16)
    returned = lax.all_to_all(produced, "expert", split_axis=0, concat_axis=0, tiled=True).reshape(
        E * CAP, MODEL_WIDTH
    )
    route_out = returned[targets].reshape(rows_local, TOP, MODEL_WIDTH).astype(jnp.float32)
    moe_sum = jnp.sum(weights[:, :, None] * route_out, axis=1)
    outputs = (h_one + moe_sum).astype(jnp.bfloat16)
    dy_wide = cotangent.astype(jnp.float32)
    d_routes = (
        (weights[:, :, None] * dy_wide[:, None, :])
        .astype(jnp.bfloat16)
        .reshape(rows_local * TOP, MODEL_WIDTH)
    )
    d_outgoing = jnp.zeros((E * CAP, MODEL_WIDTH), jnp.bfloat16).at[targets].set(d_routes)
    d_arrived = lax.all_to_all(
        d_outgoing.reshape(group_count, experts_here, CAP, MODEL_WIDTH),
        "expert",
        split_axis=0,
        concat_axis=0,
        tiled=True,
    )
    d_weights = jnp.sum(dy_wide[:, None, :] * route_out, axis=-1)
    d_chosen = weights * (d_weights - jnp.sum(weights * d_weights, axis=-1, keepdims=True))
    d_logits = jnp.sum(route_picks * d_chosen[:, :, None], axis=1).astype(jnp.bfloat16)
    grad_router = jnp.einsum("td,te->de", n_two, d_logits, preferred_element_type=jnp.float32)
    d_act = jnp.einsum("sjcd,djf->sjcf", d_arrived, down_part, preferred_element_type=jnp.float32)
    d_gate_up = jnp.concatenate(
        [
            d_act * upper_part * sigmoid_gate * (1.0 + gate_part * (1.0 - sigmoid_gate)),
            d_act * gate_part * sigmoid_gate,
        ],
        axis=-1,
    ).astype(jnp.bfloat16)
    d_rows = jnp.einsum(
        "sjcf,djf->sjcd", d_gate_up, gate_and_up, preferred_element_type=jnp.float32
    ).astype(jnp.bfloat16)
    d_returned = lax.all_to_all(d_rows, "expert", split_axis=0, concat_axis=0, tiled=True).reshape(
        E * CAP, MODEL_WIDTH
    )
    d_n_two = jnp.einsum(
        "te,de->td", d_logits, router_full, preferred_element_type=jnp.float32
    ) + jnp.sum(
        d_returned[targets].reshape(rows_local, TOP, MODEL_WIDTH).astype(jnp.float32), axis=1
    )
    first_part = jnp.einsum(
        "sjcd,sjcf->djf", arrived, d_gate_up, preferred_element_type=jnp.float32
    )
    second = jnp.einsum("sjcd,sjcf->djf", d_arrived, activated, preferred_element_type=jnp.float32)
    grad_experts = lax.psum_scatter(
        jnp.concatenate([first_part, second], axis=2).astype(jnp.bfloat16),
        "shard",
        scatter_dimension=0,
        tiled=True,
    ).astype(jnp.float32)
    grad_gain_two = jnp.sum(d_n_two * z_two, axis=0)
    dz_two = d_n_two * gain_two.astype(jnp.float32)
    dh_one = dy_wide + r_two * (dz_two - z_two * jnp.mean(dz_two * z_two, axis=-1, keepdims=True))
    dh_narrow = dh_one.astype(jnp.bfloat16)
    grad_output = jnp.einsum(
        "tk,td->kd", attention_mixed, dh_narrow, preferred_element_type=jnp.float32
    )
    mixed_gradient = jnp.einsum(
        "td,kd->tk", dh_narrow, output_full, preferred_element_type=jnp.float32
    ).astype(jnp.bfloat16)
    grad_four_dims = mixed_gradient.reshape(
        sequence_count, DEVICE_TOKENS, KEY_VALUE_HEADS, group_width, HEAD_SIZE
    )
    row_difference = jnp.sum(
        grad_four_dims.astype(jnp.float32)
        * attention_mixed.reshape(
            sequence_count, DEVICE_TOKENS, KEY_VALUE_HEADS, group_width, HEAD_SIZE
        ).astype(jnp.float32),
        axis=-1,
    )
    row_difference = jnp.transpose(row_difference, (0, 2, 3, 1))

    def grad_step(block_index, loop_state):
        d_query_sum, d_key_rows = loop_state
        scores, keys_block, values_block = scores_for(block_index)
        attn_probs = jnp.exp(scores - log_total[..., None])
        d_probs = jnp.einsum(
            "nqjgd,nkjd->njgqk", grad_four_dims, values_block, preferred_element_type=jnp.float32
        )
        d_scores = (attn_probs * (d_probs - row_difference[..., None])).astype(jnp.bfloat16)
        d_query_sum = (
            d_query_sum
            + jnp.einsum(
                "njgqk,nkjd->nqjgd", d_scores, keys_block, preferred_element_type=jnp.float32
            )
            * scale_factor
        )
        key_grad = (
            jnp.einsum(
                "njgqk,nqjgd->nkjd", d_scores, query_four_dims, preferred_element_type=jnp.float32
            )
            * scale_factor
        )
        value_grad = jnp.einsum(
            "njgqk,nqjgd->nkjd",
            attn_probs.astype(jnp.bfloat16),
            grad_four_dims,
            preferred_element_type=jnp.float32,
        )
        update = jnp.concatenate(
            [
                key_grad.reshape(sequence_count, block_of_keys, key_value_width),
                value_grad.reshape(sequence_count, block_of_keys, key_value_width),
            ],
            axis=2,
        )
        d_key_rows = lax.dynamic_update_slice_in_dim(
            d_key_rows, update, block_index * block_of_keys, 1
        )
        return (d_query_sum, d_key_rows)

    start_grads = (
        jnp.zeros(
            (sequence_count, DEVICE_TOKENS, KEY_VALUE_HEADS, group_width, HEAD_SIZE), jnp.float32
        ),
        jnp.zeros((sequence_count, seq_length, 2 * key_value_width), jnp.float32),
    )
    d_query_sum, d_key_rows = lax.fori_loop(0, total_of_block, grad_step, start_grads)
    owned_keys = (
        lax.psum_scatter(d_key_rows.astype(jnp.bfloat16), "shard", scatter_dimension=1, tiled=True)
        .astype(jnp.float32)
        .reshape(rows_local, 2 * key_value_width)
    )
    d_query = (
        reverse_rotation(
            d_query_sum.reshape(rows_local, QUERY_HEADS, HEAD_SIZE), cosine_table, sines_table
        )
        .reshape(rows_local, QUERY_HEADS * HEAD_SIZE)
        .astype(jnp.bfloat16)
    )
    key_gradient = (
        reverse_rotation(
            owned_keys[:, :key_value_width].reshape(rows_local, KEY_VALUE_HEADS, HEAD_SIZE),
            cosine_table,
            sines_table,
        )
        .reshape(rows_local, key_value_width)
        .astype(jnp.bfloat16)
    )
    value_gradient = owned_keys[:, key_value_width:].astype(jnp.bfloat16)
    grad_query = jnp.einsum("td,tk->dk", normed_first, d_query, preferred_element_type=jnp.float32)
    grad_key = jnp.einsum(
        "td,tk->dk", normed_first, key_gradient, preferred_element_type=jnp.float32
    )
    grad_value = jnp.einsum(
        "td,tk->dk", normed_first, value_gradient, preferred_element_type=jnp.float32
    )
    d_n_one = (
        jnp.einsum("tk,dk->td", d_query, query_full, preferred_element_type=jnp.float32)
        + jnp.einsum("tk,dk->td", key_gradient, key_complete, preferred_element_type=jnp.float32)
        + jnp.einsum("tk,dk->td", value_gradient, value_full, preferred_element_type=jnp.float32)
    )
    grad_gain_one = jnp.sum(d_n_one * z_one, axis=0)
    dz_one = d_n_one * gain_one.astype(jnp.float32)
    grad_inputs = dh_one + r_one * (
        dz_one - z_one * jnp.mean(dz_one * z_one, axis=-1, keepdims=True)
    )
    totals = (
        lax.psum_scatter(
            grad_gain_one.astype(jnp.bfloat16), "shard", scatter_dimension=0, tiled=True
        ).astype(jnp.float32),
        lax.psum_scatter(
            grad_query.astype(jnp.bfloat16), "shard", scatter_dimension=0, tiled=True
        ).astype(jnp.float32),
        lax.psum_scatter(
            grad_key.astype(jnp.bfloat16), "shard", scatter_dimension=0, tiled=True
        ).astype(jnp.float32),
        lax.psum_scatter(
            grad_value.astype(jnp.bfloat16), "shard", scatter_dimension=0, tiled=True
        ).astype(jnp.float32),
        lax.psum_scatter(
            grad_output.astype(jnp.bfloat16), "shard", scatter_dimension=0, tiled=True
        ).astype(jnp.float32),
        lax.psum_scatter(
            grad_router.astype(jnp.bfloat16), "shard", scatter_dimension=0, tiled=True
        ).astype(jnp.float32),
        lax.psum_scatter(
            grad_gain_two.astype(jnp.bfloat16), "shard", scatter_dimension=0, tiled=True
        ).astype(jnp.float32),
    )
    totals = (
        lax.psum(totals[0].astype(jnp.bfloat16), "expert").astype(jnp.float32),
        lax.psum(totals[1].astype(jnp.bfloat16), "expert").astype(jnp.float32),
        lax.psum(totals[2].astype(jnp.bfloat16), "expert").astype(jnp.float32),
        lax.psum(totals[3].astype(jnp.bfloat16), "expert").astype(jnp.float32),
        lax.psum(totals[4].astype(jnp.bfloat16), "expert").astype(jnp.float32),
        lax.psum(totals[5].astype(jnp.bfloat16), "expert").astype(jnp.float32),
        lax.psum(totals[6].astype(jnp.bfloat16), "expert").astype(jnp.float32),
    )
    return (
        outputs,
        grad_inputs,
        totals[0],
        totals[1],
        totals[2],
        totals[3],
        totals[4],
        totals[6],
        totals[5],
        grad_experts,
    )


def fits(shards, groups):
    if groups != 4 or shards != KEY_VALUE_HEADS or shards % 2 or E % groups:
        return False
    extra = E // groups % shards
    return E // groups > shards and extra > 0 and FF % (shards // extra * LANES) == 0


def alternating(depth):
    order = []
    low, high = 0, depth - 1
    while low <= high:
        order.append(high)
        if low != high:
            order.append(low)
        low, high = low + 1, high - 1
    return order


def sent(source, target, send, receive, group, shard):
    return pltpu.make_async_remote_copy(
        src_ref=source,
        dst_ref=target,
        send_sem=send,
        recv_sem=receive,
        device_id=(group, shard),
        device_id_type=pl.DeviceIdType.MESH,
    )


class Place:
    def __init__(self, shards, groups):
        self.group, self.shard = lax.axis_index("expert"), lax.axis_index("shard")
        self.shards, self.groups = shards, groups
        self.depth = shards // 2
        self.spot, self.core = self.shard // 2, self.shard % 2
        self.first = self.group + 1 - 2 * (self.group % 2)
        self.second = (self.group + 2) % 4
        self.corner = (self.first + 2) % 4
        self.partner = self.shard + 1 - 2 * self.core

    def greet(self, wide, whole_line, corner=False):
        barrier = pltpu.get_barrier_semaphore()

        def signal(group, shard):
            pl.semaphore_signal(
                barrier, inc=1, device_id=(group, shard), device_id_type=pl.DeviceIdType.MESH
            )

        more = (2 if wide else 0) + (1 if corner else 0)
        if wide:
            signal(self.first, self.shard)
            signal(self.second, self.shard)
        if corner:
            signal(self.corner, self.shard)
        if whole_line:
            for i in range(1, self.shards):
                signal(self.group, (self.shard + i) % self.shards)
            pl.semaphore_wait(barrier, more + self.shards - 1)
            return
        signal(self.group, self.partner)
        inside = (self.spot > 0) & (self.spot < self.depth - 1)

        @pl.when(self.spot > 0)
        def _():
            signal(self.group, self.shard - 2)

        @pl.when(self.spot < self.depth - 1)
        def _():
            signal(self.group, self.shard + 2)

        @pl.when(inside)
        def _():
            pl.semaphore_wait(barrier, more + 3)

        @pl.when(jnp.logical_not(inside))
        def _():
            pl.semaphore_wait(barrier, more + 2)


class Exchange:
    @staticmethod
    def scratch(block, dtype, pieces, n):
        dma = pltpu.SemaphoreType.DMA
        return [pltpu.VMEM(block, dtype), dma((2, pieces)), dma((n, pieces)), dma((n, pieces))]

    def __init__(self, at, plan, source, target, stage, own, out, come):
        self.at, self.source, self.target = at, source, target
        self.stage, self.own, self.out, self.come = stage, own, out, come
        self.take, self.give, self.parts = plan.take, plan.give, plan.parts

    def copies(self, i):
        at = self.at
        to = (at.shard + i) % at.shards
        for k, (taken, given) in enumerate(zip(self.take(to), self.give(at.shard))):
            yield sent(
                self.source.at[taken],
                self.target.at[given],
                self.out.at[i, k],
                self.come.at[i, k],
                at.group,
                to,
            )

    def keep(self, way):
        here = self.at.shard
        for k, (taken, given) in enumerate(zip(self.take(here), self.give(here))):
            held = self.stage.at[self.parts[k]]
            if way == 0:
                yield pltpu.make_async_copy(self.source.at[taken], held, self.own.at[0, k])
            else:
                yield pltpu.make_async_copy(held, self.target.at[given], self.own.at[1, k])

    def start(self):
        for copy in self.keep(0):
            copy.start()
        for i in range(self.at.shards - 1, 0, -1):
            for copy in self.copies(i):
                copy.start()
        for copy in self.keep(0):
            copy.wait()
        for copy in self.keep(1):
            copy.start()

    def wait(self):
        for copy in self.keep(1):
            copy.wait()
        for i in range(1, self.at.shards):
            for copy in self.copies(i):
                copy.wait()


class Rows:
    def __init__(self, array):
        self.shape, self.block, self.count = array.shape, array.shape[1:], 1
        self.parts = [...]

    def take(self, i):
        return [i]

    def give(self, me):
        return [me]


class Experts:
    def __init__(self, array, shards, experts_here, back, thirds=(0, 3), cut_thirds=(0, 3)):
        self.back, self.thirds, self.cut_thirds = back, thirds, cut_thirds
        self.whole, self.extra = divmod(experts_here, shards)
        self.shards = shards
        self.cuts = shards // self.extra if self.extra else 1
        self.width = FF // self.cuts
        if not self.extra:
            self.cut_thirds = (0, 0)
        rows = array.shape[1]
        held = 3 * (FF * self.whole + (self.width if self.extra else 0))
        self.shape = (experts_here, rows, 3 * FF) if back else (shards, rows, held)
        self.block = (rows, held)
        self.parts = [cut for _, cut in self.owner_cuts()]
        self.count = len(self.parts)

    def owner_cuts(self):
        cuts = []
        first, last = self.thirds
        for i in range(self.whole if last > first else 0):
            cuts.append((i, pl.ds((3 * i + first) * FF, (last - first) * FF)))
        start = self.whole * 3 * FF
        for k in range(*self.cut_thirds):
            cuts.append((k, pl.ds(start + k * self.width, self.width)))
        return [(k, (slice(None), cut)) for k, cut in cuts]

    def owner(self, i):
        return [(i, *cut) for _, cut in self.owner_cuts()]

    def outside(self, i):
        cuts = []
        first, last = self.thirds
        for k in range(self.whole if last > first else 0):
            cuts.append(
                (i * self.whole + k, slice(None), pl.ds(first * FF, (last - first) * FF))
            )
        for k in range(*self.cut_thirds):
            expert = self.whole * self.shards + i // self.cuts
            start = pl.multiple_of(k * FF + i % self.cuts * self.width, 128)
            cuts.append((expert, slice(None), pl.ds(start, self.width)))
        return cuts

    def take(self, i):
        return self.owner(i) if self.back else self.outside(i)

    def give(self, me):
        return self.outside(me) if self.back else self.owner(me)


class Across:
    @staticmethod
    def scratch(shape, dtype):
        block = (shape[0] // 4,) + shape[1:]
        dma = pltpu.SemaphoreType.DMA
        return [pltpu.VMEM((4,) + block, dtype), pltpu.VMEM(block, dtype)] + [
            dma((4,)) for _ in range(4)
        ]

    def __init__(self, at, source, target, held, mine, r_out, r_in, g_out, g_in):
        self.at, self.source, self.target, self.held, self.mine = at, source, target, held, mine
        self.r_out, self.r_in, self.g_out, self.g_in = r_out, r_in, g_out, g_in
        self.size = mine.shape[0]

    def part(self, ref, group):
        return ref.at[pl.ds(group * self.size, self.size)]

    def peer(self, i):
        return (self.at.first, self.at.second, self.at.corner)[i - 1]

    def out(self, i):
        return sent(
            self.part(self.source, self.peer(i)),
            self.held.at[i],
            self.r_out.at[i],
            self.r_in.at[i],
            self.peer(i),
            self.at.shard,
        )

    def back(self, i):
        return sent(
            self.mine,
            self.part(self.target, self.at.group),
            self.g_out.at[i],
            self.g_in.at[i],
            self.peer(i),
            self.at.shard,
        )

    def own(self, way):
        if way == 0:
            here = self.part(self.source, self.at.group)
            return pltpu.make_async_copy(here, self.held.at[0], self.r_in.at[0])
        here = self.part(self.target, self.at.group)
        return pltpu.make_async_copy(self.mine, here, self.g_in.at[0])

    def start(self):
        self.own(0).start()
        for i in (3, 1, 2):
            self.out(i).start()

    def turn(self):
        self.own(0).wait()
        for i in range(1, 4):
            self.out(i).wait_recv()
        total = self.held[0].astype(jnp.float32)
        for i in range(1, 4):
            total = total + self.held[i].astype(jnp.float32)
        self.mine[...] = total.astype(self.mine.dtype)
        self.own(1).start()
        for i in (3, 1, 2):
            self.back(i).start()

    def wait(self):
        self.own(1).wait()
        for i in range(1, 4):
            self.out(i).wait_send()
            self.back(i).wait()


class Gather:
    @staticmethod
    def scratch(array, wide, shards):
        steps = shards // 2 - 1
        marks = 1 + 2 * steps
        dma = pltpu.SemaphoreType.DMA
        turns = 2 if wide else 1
        return [
            dma((1,)),
            dma((2 * steps,)),
            dma((2 * steps,)),
            dma((turns, marks)),
            dma((turns, marks)),
            dma((turns, marks)),
            dma((turns, marks)),
            dma((5 if wide else 1, marks)),
            dma((5 if wide else 1, marks)),
        ]

    def __init__(self, at, wide, block, out, *sems):
        self.at, self.wide, self.block, self.out = at, wide, block, out
        self.own, self.z_out, self.z_in, self.p_out, self.p_in = sems[:5]
        self.h_out, self.h_in, self.c_out, self.c_in = sems[5:]
        self.steps = at.depth - 1
        self.events = [(0, 0)]
        for t in range(self.steps):
            self.events += [(1, t), (2, t)]

    def when(self, event, body):
        kind, t = event
        if kind == 0:
            body()
        elif kind == 1:
            pl.when(self.at.spot - 1 - t >= 0)(body)
        else:
            pl.when(self.at.spot + 1 + t < self.at.depth)(body)

    def origin(self, event):
        kind, t = event
        return self.at.shard + (0, -2 * (t + 1), 2 * (t + 1))[kind]

    def slot(self, group, shard):
        index = group * self.at.shards + shard if self.wide else shard
        return self.out.at[:, index]

    def half(self, ref, which):
        rows = ref.shape[1]
        cut = rows // 32 * 16
        return ref.at[:, pl.ds(0, cut)] if which == 0 else ref.at[:, pl.ds(cut, rows - cut)]

    def line(self, step, direction, shard):
        at = self.at
        k = direction * self.steps + step
        ref = self.slot(at.group, shard)
        source = self.block if step == 0 else ref
        to = at.shard + (2, -2)[direction]
        return sent(source, ref, self.z_out.at[k], self.z_in.at[k], at.group, to)

    def side(self, k, which):
        at, event = self.at, self.events[k]
        ref = self.slot(at.group, self.origin(event))
        source = self.block if event[0] == 0 else ref
        group = (at.first, at.second)[which]
        return sent(source, ref, self.p_out.at[which, k], self.p_in.at[which, k], group, at.shard)

    def turn(self, k, which):
        at = self.at
        shard = self.origin(self.events[k])
        held = self.half(self.slot((at.first, at.second)[which], shard), which)
        group = (at.second, at.first)[which]
        return sent(held, held, self.h_out.at[which, k], self.h_in.at[which, k], group, at.shard)

    def across(self, k, kind):
        at, event = self.at, self.events[k]
        shard = self.origin(event)
        if kind < 3:
            ref = self.slot((at.group, at.first, at.second)[kind], shard)
        else:
            ref = self.half(self.slot(at.corner, shard), kind - 3)
        source = self.block if kind == 0 and event[0] == 0 else ref
        return sent(
            source, ref, self.c_out.at[kind, k], self.c_in.at[kind, k], at.group, at.partner
        )

    def keep(self):
        here = self.slot(self.at.group, self.at.shard)
        return pltpu.make_async_copy(self.block, here, self.own.at[0])

    def onward(self, event, act):
        kind, t = event
        for direction in range(2):
            if kind and direction != kind - 1:
                continue
            step = 0 if kind == 0 else t + 1
            if step >= self.steps:
                continue
            ahead = self.at.spot < self.at.depth - 1 if direction == 0 else self.at.spot > 0
            pl.when(ahead)(
                lambda step=step, direction=direction: act(
                    self.line(step, direction, self.origin(event))
                )
            )

    def lines(self, k):
        event = self.events[k]

        def body():
            kind, t = event
            if kind:
                self.line(t, kind - 1, self.origin(event)).wait_recv()
            self.onward(event, lambda copy: copy.start())
            if self.wide:
                self.side(k, 0).start()
                self.side(k, 1).start()
            self.across(k, 0).start()
            if kind == 0:
                self.keep().start()

        self.when(event, body)

    def sides(self, k):
        def body():
            for which in range(2):
                self.side(k, which).wait_recv()
                self.turn(k, which).start()
                self.across(k, 1 + which).start()

        if self.wide:
            self.when(self.events[k], body)

    def turns(self, k):
        def body():
            for which in range(2):
                self.turn(k, which).wait_recv()
                self.across(k, 3 + which).start()

        if self.wide:
            self.when(self.events[k], body)

    def finish(self, k):
        event = self.events[k]

        def body():
            if event[0] == 0:
                self.keep().wait()
            self.onward(event, lambda copy: copy.wait_send())
            for kind in range(5 if self.wide else 1):
                copy = self.across(k, kind)
                copy.wait_send()
                copy.wait_recv()
            if self.wide:
                for which in range(2):
                    self.side(k, which).wait_send()
                    self.turn(k, which).wait_send()

        self.when(event, body)


class Reduce:
    @staticmethod
    def scratch(parts, wide, shards):
        depth = shards // 2
        block = (parts.shape[0],) + parts.shape[2:]
        kinds = 4 if wide else 1
        dma = pltpu.SemaphoreType.DMA
        out = [
            pltpu.VMEM((kinds, depth) + block, parts.dtype),
            pltpu.VMEM((kinds, depth) + block, parts.dtype),
            pltpu.VMEM((2, depth) + block, parts.dtype),
            dma((kinds, depth)),
            dma((kinds, depth)),
            dma((kinds, depth)),
            dma((2, depth)),
            dma((2, depth)),
        ]
        if wide:
            cut = block[1] // 32 * 16
            out += [
                pltpu.VMEM((depth, block[0], cut, block[2]), parts.dtype),
                pltpu.VMEM((depth, block[0], block[1] - cut, block[2]), parts.dtype),
                pltpu.VMEM((2, depth) + block, parts.dtype),
                dma((2, depth)),
                dma((2, depth)),
                dma((2, depth)),
                dma((2, depth)),
            ]
        return out

    def __init__(self, at, wide, parts, total, *scratch):
        self.at, self.wide, self.parts, self.total = at, wide, parts, total
        self.mine, self.accs, self.z_buf, self.own = scratch[:4]
        self.c_out, self.c_in, self.z_out, self.z_in = scratch[4:8]
        if wide:
            self.h_buf, self.p_buf = scratch[8:10], scratch[10]
            self.h_out, self.h_in, self.p_out, self.p_in = scratch[11:]
        self.order = alternating(at.depth)
        self.kinds = (3, 1, 2, 0) if wide else (0,)
        self.columns = (at.group, at.first, at.second, at.corner)

    def place(self, kind, q, core):
        shard = 2 * q + core
        return self.columns[kind] * self.at.shards + shard if self.wide else shard

    def load(self, kind, q):
        return pltpu.make_async_copy(
            self.parts.at[:, self.place(kind, q, self.at.core)],
            self.mine.at[kind, q],
            self.own.at[kind, q],
        )

    def across(self, kind, q):
        return sent(
            self.parts.at[:, self.place(kind, q, 1 - self.at.core)],
            self.accs.at[kind, q],
            self.c_out.at[kind, q],
            self.c_in.at[kind, q],
            self.at.group,
            self.at.partner,
        )

    def span(self, which):
        rows = self.accs.shape[3]
        cut = rows // 32 * 16
        return pl.ds(0, cut) if which == 0 else pl.ds(cut, rows - cut)

    def turn(self, q, which):
        return sent(
            self.accs.at[3, q, :, self.span(which)],
            self.h_buf[which].at[q],
            self.h_out.at[which, q],
            self.h_in.at[which, q],
            (self.at.first, self.at.second)[which],
            self.at.shard,
        )

    def side(self, q, which):
        return sent(
            self.accs.at[1 + which, q],
            self.p_buf.at[which, q],
            self.p_out.at[which, q],
            self.p_in.at[which, q],
            (self.at.first, self.at.second)[which],
            self.at.shard,
        )

    def line(self, q, direction):
        return sent(
            self.accs.at[0, q],
            self.z_buf.at[direction, q],
            self.z_out.at[direction, q],
            self.z_in.at[direction, q],
            self.at.group,
            self.at.shard + (2, -2)[direction],
        )

    def add(self, kind, q, *others):
        value = self.accs[kind, q].astype(jnp.float32)
        for other in others:
            value = value + other.astype(jnp.float32)
        self.accs[kind, q] = value.astype(self.accs.dtype)

    def pair(self, kind, q):
        self.load(kind, q).wait()
        self.across(kind, q).wait_recv()
        self.add(kind, q, self.mine[kind, q])

    def begin(self):
        for kind in self.kinds:
            for q in self.order:
                self.load(kind, q).start()
                self.across(kind, q).start()

    def corners(self):
        for q in self.order:
            self.pair(3, q)
            self.turn(q, 0).start()
            self.turn(q, 1).start()

    def sides(self):
        for q in self.order:
            for which in range(2):
                kind = 2 - which
                self.pair(kind, q)
                self.turn(q, which).wait_recv()
                span = self.span(which)
                value = self.accs[kind, q, :, span].astype(jnp.float32)
                value = value + self.h_buf[which][q].astype(jnp.float32)
                self.accs[kind, q, :, span] = value.astype(self.accs.dtype)
                self.side(q, kind - 1).start()

    def lines(self, q):
        at = self.at
        self.pair(0, q)
        if self.wide:
            self.side(q, 0).wait_recv()
            self.side(q, 1).wait_recv()
            self.add(0, q, self.p_buf[0, q], self.p_buf[1, q])
        for direction in range(2):

            @pl.when(q > at.spot if direction == 0 else q < at.spot)
            def _(direction=direction):
                @pl.when(at.spot > 0 if direction == 0 else at.spot < at.depth - 1)
                def _():
                    self.line(q, direction).wait_recv()
                    self.add(0, q, self.z_buf[direction, q])

                self.line(q, direction).start()

    def finish(self):
        at, total = self.at, self.total
        for q in range(at.depth):

            @pl.when(q == at.spot)
            def _(q=q):
                total[...] = self.accs[0, q].astype(jnp.float32)
                for direction in range(2):
                    if q > 0 if direction == 0 else q < at.depth - 1:
                        self.line(q, direction).wait_recv()
                        total[...] = total[...] + self.z_buf[direction, q].astype(jnp.float32)

            for kind in self.kinds:
                self.across(kind, q).wait_send()
            if self.wide:
                for which in range(2):
                    self.turn(q, which).wait_send()
                    self.side(q, which).wait_send()
            for direction in range(2):

                @pl.when(q > at.spot if direction == 0 else q < at.spot)
                def _(q=q, direction=direction):
                    self.line(q, direction).wait_send()


def cut_refs(refs, sizes):
    out, start = [], 0
    for size in sizes:
        out.append(refs[start : start + size])
        start += size
    return out


def gather_body(shards, groups, wides, plans, sizes, *refs):
    count = len(wides) + len(plans)
    ins, outs = refs[:count], refs[count : 2 * count]
    scratch = cut_refs(refs[2 * count :], sizes)
    at = Place(shards, groups)
    at.greet(any(wides), len(plans) > 0)
    gathers = [Gather(at, wide, ins[i], outs[i], *scratch[i]) for i, wide in enumerate(wides)]
    moves = [
        Exchange(at, plan, ins[i], outs[i], *scratch[i])
        for i, plan in enumerate(plans, len(wides))
    ]
    marks = range(len(gathers[0].events))
    for k in marks:
        for g in gathers:
            g.lines(k)
    for m in moves:
        m.start()
    for step in (Gather.sides, Gather.turns, Gather.finish):
        for k in marks:
            for g in gathers:
                step(g, k)
    for m in moves:
        m.wait()


def gathered(arrays, wides, shards, groups, identity, swapped=(), plans=()):
    shapes = [
        jax.ShapeDtypeStruct(
            (a.shape[0], shards * (groups if wide else 1)) + a.shape[1:], a.dtype
        )
        for a, wide in zip(arrays, wides)
    ] + [jax.ShapeDtypeStruct(p.shape, a.dtype) for a, p in zip(swapped, plans)]
    moved = sum(s.size * s.dtype.itemsize for s in shapes)
    scratch = [Gather.scratch(a, wide, shards) for a, wide in zip(arrays, wides)]
    scratch += [Exchange.scratch(p.block, a.dtype, p.count, shards) for a, p in zip(swapped, plans)]
    return pl.pallas_call(
        functools.partial(
            gather_body, shards, groups, tuple(wides), tuple(plans), tuple(len(s) for s in scratch)
        ),
        out_shape=shapes,
        in_specs=[pl.BlockSpec(memory_space=pltpu.VMEM)] * len(arrays)
        + [pl.BlockSpec(memory_space=pl.ANY)] * len(swapped),
        out_specs=[pl.BlockSpec(memory_space=pl.ANY)] * len(shapes),
        scratch_shapes=[s for some in scratch for s in some],
        compiler_params=pltpu.CompilerParams(collective_id=identity, has_side_effects=True),
        cost_estimate=pl.CostEstimate(flops=0, bytes_accessed=20 * moved, transcendentals=0),
    )(*arrays, *swapped)


def halved(array, wide):
    block = array.size // array.shape[1] * array.dtype.itemsize
    return not wide and array.shape[0] == 2 and block > 200_000


def reduce_body(shards, groups, wides, halves, plans, sums, sizes, *refs):
    given = len(wides) + len(plans)
    count = given + sum(1 for kind, _ in sums if kind == "in")
    results = given + len(sums)
    ins, outs = refs[:count], refs[count : count + results]
    scratch = cut_refs(refs[count + results :], sizes)
    at = Place(shards, groups)
    at.greet(any(wides) or len(sums) > 0, len(plans) > 0, len(sums) > 0)
    reductions = []
    for i, wide in enumerate(wides):
        if halves[i]:
            for j in range(2):
                half = pl.ds(j, 1)
                reductions.append(
                    Reduce(at, wide, ins[i].at[half], outs[i].at[half], *scratch.pop(0))
                )
        else:
            reductions.append(Reduce(at, wide, ins[i], outs[i], *scratch.pop(0)))
    moves = [
        Exchange(at, plan, ins[i], outs[i], *scratch.pop(0))
        for i, plan in enumerate(plans, len(wides))
    ]
    totals = []
    for i, (kind, which) in enumerate(sums, given):
        source = {"in": ins, "sum": outs, "swap": outs}[kind]
        source = source[which + (0 if kind == "sum" else given if kind == "in" else len(wides))]
        totals.append(Across(at, source, outs[i], *scratch.pop(0)))
    flat = [r for r in reductions if not r.wide]
    wide_ones = [r for r in reductions if r.wide]
    order = reductions[0].order
    late = [i for i in range(len(moves)) if flat and ("swap", i) not in sums]

    def swapped_sums():
        for (kind, which), s in zip(sums, totals):
            if kind == "swap":
                moves[which].wait()
                s.start()

    for r in reductions:
        r.begin()
    for i, m in enumerate(moves):
        if i not in late:
            m.start()
    for (kind, _), s in zip(sums, totals):
        if kind == "in":
            s.start()
    for r in wide_ones:
        r.corners()
    for step, q in enumerate(order):
        for r in flat:
            r.lines(q)
        if step == min(1, len(order) - 1):
            for i in late:
                moves[i].start()
        if step == min(2, len(order) - 1):
            swapped_sums()
    for r in flat:
        r.finish()
    for (kind, _), s in zip(sums, totals):
        if kind == "sum":
            s.start()
    for r in wide_ones:
        r.sides()
    for s in totals:
        s.turn()
    for r in wide_ones:
        for q in order:
            r.lines(q)
    for r in wide_ones:
        r.finish()
    for s in totals:
        s.wait()
    for i, m in enumerate(moves):
        if ("swap", i) not in sums:
            m.wait()


def reduced(arrays, wides, shards, groups, identity, swapped=(), plans=(), sums=(), terms=()):
    shapes = [
        jax.ShapeDtypeStruct((a.shape[0],) + a.shape[2:], jnp.float32) for a in arrays
    ] + [jax.ShapeDtypeStruct(p.shape, a.dtype) for a, p in zip(swapped, plans)]
    for kind, which in sums:
        if kind == "in":
            source = terms[which]
        else:
            source = shapes[which + (0 if kind == "sum" else len(arrays))]
        shapes.append(jax.ShapeDtypeStruct(source.shape, source.dtype))
    operands = (*arrays, *swapped, *terms)
    moved = sum(a.size * a.dtype.itemsize for a in operands)
    halves = tuple(halved(a, wide) for a, wide in zip(arrays, wides))
    scratch = []
    for a, wide, half in zip(arrays, wides, halves):
        block = jax.ShapeDtypeStruct((1,) + a.shape[1:] if half else a.shape, a.dtype)
        scratch += [Reduce.scratch(block, wide, shards)] * (2 if half else 1)
    scratch += [Exchange.scratch(p.block, a.dtype, p.count, shards) for a, p in zip(swapped, plans)]
    scratch += [Across.scratch(a.shape, a.dtype) for a in shapes[len(arrays) + len(swapped) :]]
    return pl.pallas_call(
        functools.partial(
            reduce_body,
            shards,
            groups,
            tuple(wides),
            halves,
            tuple(plans),
            tuple(sums),
            tuple(len(s) for s in scratch),
        ),
        out_shape=shapes,
        in_specs=[pl.BlockSpec(memory_space=pl.ANY)] * len(operands),
        out_specs=[pl.BlockSpec(memory_space=pltpu.VMEM)] * len(arrays)
        + [pl.BlockSpec(memory_space=pl.ANY)] * (len(shapes) - len(arrays)),
        scratch_shapes=[s for some in scratch for s in some],
        compiler_params=pltpu.CompilerParams(
            collective_id=identity, has_side_effects=True, vmem_limit_bytes=64 * 1024 * 1024 - 65536
        ),
        cost_estimate=pl.CostEstimate(flops=0, bytes_accessed=20 * moved, transcendentals=0),
    )(*operands)


PAIR = 256
TILE = 320


def experts_body(
    shape,
    ids,
    routes,
    router,
    n_from,
    c_from,
    w_from,
    w_cut,
    y_to,
    d_to,
    g_to,
    rows_n,
    rows_c,
    weights,
    picks,
    slot_w,
    slot_d,
    act_rows,
    gu_rows,
    y_rows,
    d_rows,
    n_buf,
    c_buf,
    y_buf,
    d_buf,
    g_buf,
    n_sem,
    c_sem,
    w_sem,
    y_sem,
    d_sem,
    g_sem,
):
    units, pairs, slots, tokens, extra = shape
    f32, bf16 = jnp.float32, jnp.bfloat16
    whole = 2 * slots
    chunk = weights.shape[0] // w_from.shape[0]

    def bring(p, slot):
        return (
            pltpu.make_async_copy(n_from.at[pl.ds(2 * p, 2)], n_buf.at[slot], n_sem.at[slot]),
            pltpu.make_async_copy(c_from.at[pl.ds(2 * p, 2)], c_buf.at[slot], c_sem.at[slot]),
        )

    split = units[-1][0]

    def weight_copies(i):
        here = pl.ds(i * chunk, chunk)
        for k, (source, cut) in enumerate(
            ((w_from, pl.ds(0, split)), (w_cut, pl.ds(split, weights.shape[1] - split)))
        ):
            yield pltpu.make_async_copy(
                source.at[i, :, cut], weights.at[here, cut], w_sem.at[i, k]
            )

    for copy in bring(0, 0):
        copy.start()
    for i in range(w_from.shape[0]):
        for copy in weight_copies(i):
            copy.start()
    row = lax.broadcasted_iota(jnp.int32, (PAIR, PAIR), 0)
    column = lax.broadcasted_iota(jnp.int32, (PAIR, PAIR), 1)
    upto = ((row <= column) & (row // tokens == column // tokens)).astype(bf16)
    names = lax.broadcasted_iota(jnp.int32, (router.shape[0], PAIR), 0)
    lanes = lax.broadcasted_iota(jnp.int32, (1, PAIR), 1)
    places = lax.broadcasted_iota(jnp.int32, (whole, PAIR), 0)
    sixteen = lax.broadcasted_iota(jnp.int32, (16, PAIR), 0)

    def dispatch(p, _):
        slot = p % 2
        for copy in bring(p, slot):
            copy.wait()

        @pl.when(p + 1 < pairs)
        def _():
            for copy in bring(p + 1, 1 - slot):
                copy.start()

        n = n_buf[slot].reshape(PAIR, n_buf.shape[3])
        c = c_buf[slot].reshape(PAIR, c_buf.shape[3])
        named = routes[p]
        logits = lax.dot_general(
            router[...], n, (((1,), (1,)), ((), ())), preferred_element_type=f32
        )
        hit = names == named[0:1]
        for j in range(1, TOP):
            hit = hit | (names == named[j : j + 1])
        masked = jnp.where(hit, logits, MASKED)
        top = jnp.max(masked, axis=0, keepdims=True)
        raised = jnp.where(hit, jnp.exp(masked - top), 0.0)
        share = raised / jnp.sum(raised, axis=0, keepdims=True)
        hits = []
        for u in range(len(units)):
            mine = hit & (names == ids[u])
            hits.append(jnp.sum(jnp.where(mine, 1.0, 0.0), axis=0, keepdims=True))
        both = jnp.zeros((16, PAIR), f32)
        for u in range(len(units)):
            both = jnp.where(sixteen == u, hits[u], both)
        ranks = jnp.dot(both.astype(bf16), upto, preferred_element_type=f32)
        for u in range(len(units)):
            weight = jnp.sum(
                jnp.where(hit & (names == ids[u]), share, 0.0), axis=0, keepdims=True
            )
            place = jnp.where(
                hits[u] > 0.5,
                ranks[u : u + 1].astype(jnp.int32) - 1 + lanes // tokens * slots,
                -1,
            )
            pick = (places == place).astype(f32)
            at = pl.ds(pl.multiple_of(p * whole, 16), whole)
            slot_w[u, at] = jnp.sum(pick * weight, axis=1, keepdims=True)
            picks[p, u * whole : (u + 1) * whole] = pick.astype(bf16)
        at = pl.ds(pl.multiple_of(p * whole, 16), whole)
        sent_n = jnp.dot(picks[p], n, preferred_element_type=f32).astype(bf16)
        sent_c = jnp.dot(picks[p], c, preferred_element_type=f32).astype(bf16)
        for u in range(len(units)):
            rows_n[u, at] = sent_n[u * whole : (u + 1) * whole]
            rows_c[u, at] = sent_c[u * whole : (u + 1) * whole]
        return 0

    lax.fori_loop(0, pairs, dispatch, 0)
    for i in range(w_from.shape[0]):
        for copy in weight_copies(i):
            copy.wait()
    turned = (((1,), (1,)), ((), ()))
    summed = (((0,), (0,)), ((), ()))
    for u, (start, width) in enumerate(units):
        gu = pl.ds(start, 2 * width)
        down = pl.ds(start + 2 * width, width)

        def tile(i, _, u=u, start=start, width=width, gu=gu, down=down):
            at = pl.ds(pl.multiple_of(i * TILE, 16), TILE)
            parts = jnp.dot(rows_n[u, at], weights[:, gu], preferred_element_type=f32)
            plain = jnp.dot(rows_c[u, at], weights[:, down], preferred_element_type=f32)
            gate, up = parts[:, :width], parts[:, width:]
            sig = jax.nn.sigmoid(gate)
            act = gate * sig * up
            w = slot_w[u, at]
            slot_d[u, at] = jnp.sum(act * plain, axis=1, keepdims=True)
            act_w = (act * w).astype(bf16)
            da = plain * w
            d_gate = (da * up * sig * (1.0 + gate * (1.0 - sig))).astype(bf16)
            d_up = (da * gate * sig).astype(bf16)
            act_rows[u, at, :width] = act_w
            gu_rows[u, at, :width] = d_gate
            gu_rows[u, at, width : 2 * width] = d_up
            y_rows[u, at] = lax.dot_general(
                act_w, weights[:, down], turned, preferred_element_type=f32
            ).astype(bf16)
            d_rows[u, at] = lax.dot_general(
                gu_rows[u, at, : 2 * width], weights[:, gu], turned, preferred_element_type=f32
            ).astype(bf16)
            return 0

        lax.fori_loop(0, pairs * whole // TILE, tile, 0)

    deep = 256

    def grad_copy(i):
        return pltpu.make_async_copy(
            g_buf.at[pl.ds(i * chunk, chunk)], g_to.at[i], g_sem.at[i]
        )

    def grads(i, _):
        at = pl.ds(pl.multiple_of(i * deep, deep), deep)
        for u, (start, width) in enumerate(units):
            g_buf[at, start : start + 2 * width] = lax.dot_general(
                rows_n[u, :, at], gu_rows[u, :, : 2 * width], summed, preferred_element_type=f32
            ).astype(bf16)
            g_buf[at, start + 2 * width : start + 3 * width] = lax.dot_general(
                rows_c[u, :, at], act_rows[u, :, :width], summed, preferred_element_type=f32
            ).astype(bf16)
        return 0

    lax.fori_loop(0, weights.shape[0] // deep, grads, 0)
    for i in range(g_to.shape[0]):
        grad_copy(i).start()

    def put(p, slot):
        return (
            pltpu.make_async_copy(y_buf.at[slot], y_to.at[pl.ds(2 * p, 2)], y_sem.at[slot]),
            pltpu.make_async_copy(d_buf.at[slot], d_to.at[pl.ds(2 * p, 2)], d_sem.at[slot]),
        )

    d_buf[:, :, tokens:] = jnp.zeros((2, 2, extra, d_buf.shape[3]), bf16)

    def combine(p, _):
        slot = p % 2

        @pl.when(p >= 2)
        def _():
            for copy in put(p - 2, slot):
                copy.wait()

        at = pl.ds(pl.multiple_of(p * whole, 16), whole)
        pick = picks[p]
        both = [y_rows[u, at] for u in range(len(units))]
        y = lax.dot_general(pick, jnp.concatenate(both), summed, preferred_element_type=f32)
        both = [d_rows[u, at] for u in range(len(units))]
        d = lax.dot_general(pick, jnp.concatenate(both), summed, preferred_element_type=f32)
        d_w = jnp.zeros((TOP, PAIR), f32)
        for u in range(len(units)):
            pick = picks[p, u * whole : (u + 1) * whole]
            back = jnp.sum(pick.astype(f32) * slot_d[u, at], axis=0, keepdims=True)
            d_w = d_w + jnp.where(routes[p] == ids[u], back, 0.0)
        high = d_w.astype(bf16)
        low = (d_w - high.astype(f32)).astype(bf16)
        y_buf[slot] = y.astype(bf16).reshape(y_buf.shape[1:])
        d_buf[slot, :, :tokens] = d.astype(bf16).reshape(2, tokens, d.shape[1])
        both = jnp.concatenate([high.astype(f32), low.astype(f32)], axis=0).astype(bf16)
        for i in range(2):
            d_buf[slot, i, tokens:, :tokens] = both[:, i * tokens : (i + 1) * tokens]
        for copy in put(p, slot):
            copy.start()
        return 0

    lax.fori_loop(0, pairs, combine, 0)
    for p in range(pairs - 2, pairs):
        for copy in put(p, p % 2):
            copy.wait()
    for i in range(g_to.shape[0]):
        grad_copy(i).wait()


def experts(ids, routes, router, n_all, c_all, owned, owned_cut, units, slots, extra):
    blocks, tokens, width = n_all.shape
    pairs = blocks // 2
    rows = pairs * 2 * slots
    count = len(units)
    hidden = max(w for _, w in units)
    bf16, f32 = jnp.bfloat16, jnp.float32
    shards, own_rows, columns = owned.shape
    dma = pltpu.SemaphoreType.DMA
    any_space, vmem = pl.BlockSpec(memory_space=pl.ANY), pl.BlockSpec(memory_space=pltpu.VMEM)
    flops = 2 * rows * width * sum(w for _, w in units) * 9
    return pl.pallas_call(
        functools.partial(experts_body, (tuple(units), pairs, slots, tokens, extra)),
        out_shape=[
            jax.ShapeDtypeStruct((blocks, tokens, width), bf16),
            jax.ShapeDtypeStruct((blocks, tokens + extra, width), bf16),
            jax.ShapeDtypeStruct(owned.shape, bf16),
        ],
        in_specs=[pl.BlockSpec(memory_space=pltpu.SMEM), vmem, vmem] + [any_space] * 4,
        out_specs=[any_space] * 3,
        scratch_shapes=[
            pltpu.VMEM((count, rows, width), bf16),
            pltpu.VMEM((count, rows, width), bf16),
            pltpu.VMEM((shards * own_rows, columns), bf16),
            pltpu.VMEM((pairs, count * 2 * slots, PAIR), bf16),
            pltpu.VMEM((count, rows, 1), f32),
            pltpu.VMEM((count, rows, 1), f32),
            pltpu.VMEM((count, rows, hidden), bf16),
            pltpu.VMEM((count, rows, 2 * hidden), bf16),
            pltpu.VMEM((count, rows, width), bf16),
            pltpu.VMEM((count, rows, width), bf16),
            pltpu.VMEM((2, 2, tokens, width), bf16),
            pltpu.VMEM((2, 2, tokens, width), bf16),
            pltpu.VMEM((2, 2, tokens, width), bf16),
            pltpu.VMEM((2, 2, tokens + extra, width), bf16),
            pltpu.VMEM((shards * own_rows, columns), bf16),
            dma((2,)),
            dma((2,)),
            dma((shards, 2)),
            dma((2,)),
            dma((2,)),
            dma((shards,)),
        ],
        compiler_params=pltpu.CompilerParams(vmem_limit_bytes=67_000_000),
        cost_estimate=pl.CostEstimate(
            flops=flops, bytes_accessed=60 * 1024 * 1024, transcendentals=rows * hidden
        ),
    )(ids, routes, router, n_all, c_all, owned, owned_cut)


def turned_lanes(values, cosine, sine):
    lane = lax.broadcasted_iota(jnp.int32, values.shape, 1)
    half = HEAD_SIZE // 2
    other = jnp.where(
        lane % HEAD_SIZE < half,
        pltpu.roll(values, LANES - half, 1),
        pltpu.roll(values, half, 1),
    )
    return values * cosine + other * sine


def causal(rows, columns, first_row):
    row = lax.broadcasted_iota(jnp.int32, (rows, columns), 0) + first_row
    return lax.broadcasted_iota(jnp.int32, (rows, columns), 1) <= row


NT = (((1,), (1,)), ((), ()))
TN = (((0,), (0,)), ((), ()))


def product(a, b, dims):
    return lax.dot_general(a, b, dims, preferred_element_type=jnp.float32)


def front_body(shards, groups, plans, sizes, *refs):
    x, small, routes, w_output, cosine, sine, qkv_cut, experts_cut = refs[:8]
    small_all, routes_all, qkv_own, piece, normed, turned, log_sums, mixed, attended = refs[8:17]
    x_all, parts = refs[17:19]
    scratch = cut_refs(refs[19:], sizes)
    f32, bf16 = jnp.float32, jnp.bfloat16
    at = Place(shards, groups)
    at.greet(True, True)
    gathers = [
        Gather(at, False, x, x_all, *scratch[0]),
        Gather(at, False, small, small_all, *scratch[1]),
        Gather(at, True, routes, routes_all, *scratch[2]),
    ]
    qkv_move = Exchange(at, plans[0], qkv_cut, qkv_own, *scratch[3])
    piece_move = Exchange(at, plans[1], experts_cut, piece, *scratch[4])
    sums = [
        Reduce(at, False, parts.at[pl.ds(j, 1)], attended.at[pl.ds(j, 1)], *scratch[5 + j])
        for j in range(2)
    ]
    marks = range(len(gathers[0].events))
    for k in marks:
        for g in gathers:
            g.lines(k)
        if k == 0:
            qkv_move.start()
    piece_move.start()
    for step in (Gather.sides, Gather.turns, Gather.finish):
        for k in marks:
            for g in gathers:
                step(g, k)
    qkv_move.wait()

    width = x.shape[2]
    length = shards * DEVICE_TOKENS
    tile = 256
    at_lane = lax.broadcasted_iota(jnp.int32, (16, LANES), 1)
    at_row = lax.broadcasted_iota(jnp.int32, (16, LANES), 0)
    one_hot = ((at_lane == E) & (at_row == 0)).astype(bf16)
    gain = product(one_hot, small_all[0].reshape(width, LANES), NT)[0:1]
    per = length // tile

    def project(t, _):
        j, i = t // per, t % per
        count = tile // DEVICE_TOKENS
        rows = x_all[j, pl.ds(i * count, count)].reshape(tile, width).astype(f32)
        rate = lax.rsqrt(jnp.mean(rows * rows, axis=-1, keepdims=True) + EPSILON)
        n = (rows * rate * gain).astype(bf16)
        here = pl.ds(pl.multiple_of(i * tile, tile), tile)
        normed[j, here] = n
        qkv = jnp.dot(n, qkv_own[...].reshape(width, -1), preferred_element_type=f32)
        for lanes in (0, LANES):
            turned[j, here, lanes : lanes + LANES] = turned_lanes(
                qkv[:, lanes : lanes + LANES], cosine[here], sine[here]
            ).astype(bf16)
        turned[j, here, 2 * LANES :] = qkv[:, 2 * LANES :].astype(bf16)
        return 0

    lax.fori_loop(0, 2 * per, project, 0)
    ratio = QUERY_HEADS // KEY_VALUE_HEADS
    scale = 1.0 / HEAD_SIZE
    for j in range(2):
        key = turned[j, :, ratio * HEAD_SIZE : (ratio + 1) * HEAD_SIZE]
        value = turned[j, :, (ratio + 1) * HEAD_SIZE :]
        for i in range(per):
            here = slice(i * tile, (i + 1) * tile)
            seen = (i + 1) * tile
            outs, logs = [], []
            for h in range(ratio):
                query = turned[j, here, h * HEAD_SIZE : (h + 1) * HEAD_SIZE]
                scores = product(query, key[:seen], NT) * scale
                scores = jnp.where(causal(tile, seen, i * tile), scores, MASKED)
                top = jnp.max(scores, axis=-1, keepdims=True)
                raised = jnp.exp(scores - top)
                total = jnp.sum(raised, axis=-1, keepdims=True)
                logs.append(top + jnp.log(total))
                probs = (raised * (1.0 / total)).astype(bf16)
                outs.append(jnp.dot(probs, value[:seen], preferred_element_type=f32))
            mixed[j, here] = jnp.concatenate(outs, axis=1).astype(bf16)
            for h in range(ratio):
                log_sums[j, here, h : h + 1] = logs[h]
            out = jnp.dot(mixed[j, here], w_output[...], preferred_element_type=f32).astype(bf16)
            count = tile // DEVICE_TOKENS
            parts[j, i * count : (i + 1) * count] = out.reshape(count, DEVICE_TOKENS, width)
        sums[j].begin()
    for q in sums[0].order:
        for s in sums:
            s.lines(q)
    for s in sums:
        s.finish()
    piece_move.wait()


def front(x, small, routes, w_output, cosine, sine, qkv_cut, experts_cut, shards, groups, plans):
    f32, bf16 = jnp.float32, jnp.bfloat16
    sequences, rows, width = x.shape
    length = shards * rows
    block = jax.ShapeDtypeStruct((1, shards, rows, width), bf16)
    scratch = [
        Gather.scratch(x, False, shards),
        Gather.scratch(small, False, shards),
        Gather.scratch(routes, True, shards),
        Exchange.scratch(plans[0].block, bf16, plans[0].count, shards),
        Exchange.scratch(plans[1].block, bf16, plans[1].count, shards),
        Reduce.scratch(block, False, shards),
        Reduce.scratch(block, False, shards),
    ]
    any_space, vmem = pl.BlockSpec(memory_space=pl.ANY), pl.BlockSpec(memory_space=pltpu.VMEM)
    columns = qkv_cut.shape[2]
    queries = w_output.shape[0]
    return pl.pallas_call(
        functools.partial(
            front_body, shards, groups, tuple(plans), tuple(len(s) for s in scratch)
        ),
        out_shape=[
            jax.ShapeDtypeStruct((1, shards) + small.shape[1:], bf16),
            jax.ShapeDtypeStruct((1, shards * groups) + routes.shape[1:], routes.dtype),
            jax.ShapeDtypeStruct(plans[0].shape, bf16),
            jax.ShapeDtypeStruct(plans[1].shape, bf16),
            jax.ShapeDtypeStruct((sequences, length, width), bf16),
            jax.ShapeDtypeStruct((sequences, length, columns), bf16),
            jax.ShapeDtypeStruct((sequences, length, LANES), f32),
            jax.ShapeDtypeStruct((sequences, length, queries), bf16),
            jax.ShapeDtypeStruct((sequences, rows, width), f32),
        ],
        in_specs=[vmem] * 6 + [any_space] * 2,
        out_specs=[vmem, any_space, vmem, any_space, vmem, vmem, vmem, vmem, vmem],
        scratch_shapes=[
            pltpu.VMEM((sequences, shards, rows, width), bf16),
            pltpu.VMEM((sequences, shards, rows, width), bf16),
        ]
        + [s for some in scratch for s in some],
        compiler_params=pltpu.CompilerParams(
            collective_id=0, has_side_effects=True, vmem_limit_bytes=60 * 1024 * 1024
        ),
        cost_estimate=pl.CostEstimate(
            flops=4 * 10**9, bytes_accessed=100 * 10**6, transcendentals=3 * 10**6
        ),
    )(x, small, routes, w_output, cosine, sine, qkv_cut, experts_cut)


def rear_body(shards, groups, plans, sizes, *refs):
    dh, w_output, normed, qkv_own, turned, log_sums, mixed, cosine, sine = refs[:9]
    grad_small, grads, _ = refs[9:12]
    d_normed, small_line, qkv_sum, small_sum, output_sum, experts_out = refs[12:18]
    dh_all, parts, d_qkv, d_keys, d_values, grad_qkv, swapped, grad_output = refs[18:26]
    scratch = cut_refs(refs[26:], sizes)
    f32, bf16 = jnp.float32, jnp.bfloat16
    at = Place(shards, groups)
    at.greet(True, True, True)
    gather = Gather(at, False, dh, dh_all, *scratch[0])
    experts_move = Exchange(at, plans[0], grads, experts_out, *scratch[1])
    qkv_move = Exchange(at, plans[1], grad_qkv, swapped, *scratch[2])
    sums = [
        Reduce(at, False, parts.at[pl.ds(j, 1)], d_normed.at[pl.ds(j, 1)], *scratch[3 + j])
        for j in range(2)
    ]
    small = Reduce(at, False, grad_small, small_line, *scratch[5])
    of_qkv = Across(at, swapped, qkv_sum, *scratch[6])
    of_small = Across(at, small_line, small_sum, *scratch[7])
    of_output = Across(at, grad_output, output_sum, *scratch[8])
    small.begin()
    marks = range(len(gather.events))
    for k in marks:
        gather.lines(k)
    for q in small.order:
        small.lines(q)
    experts_move.start()
    small.finish()
    of_small.start()
    for k in marks:
        gather.finish(k)

    width = dh.shape[2]
    length = shards * DEVICE_TOKENS
    tile = 256
    ratio = QUERY_HEADS // KEY_VALUE_HEADS
    scale = 1.0 / HEAD_SIZE
    total = jnp.zeros((ratio * HEAD_SIZE, width), f32)
    for j in range(2):
        total = total + product(mixed[j], dh_all[j].reshape(length, width), TN)
    grad_output[...] = total.astype(bf16).reshape(grad_output.shape)
    of_output.start()
    for j in range(2):
        d_mixed = product(dh_all[j].reshape(length, width), w_output[...], NT).astype(bf16)
        key = turned[j, :, ratio * HEAD_SIZE : (ratio + 1) * HEAD_SIZE]
        value = turned[j, :, (ratio + 1) * HEAD_SIZE :]
        d_keys[...] = jnp.zeros_like(d_keys)
        d_values[...] = jnp.zeros_like(d_values)
        d_queries = []
        for i in range(length // tile):
            here = slice(i * tile, (i + 1) * tile)
            seen = (i + 1) * tile
            row = []
            for h in range(ratio):
                head = slice(h * HEAD_SIZE, (h + 1) * HEAD_SIZE)
                query = turned[j, here, head]
                d_out = d_mixed[here, head]
                scores = product(query, key[:seen], NT) * scale
                scores = jnp.where(causal(tile, seen, i * tile), scores, MASKED)
                probs = jnp.exp(scores - log_sums[j, here, h : h + 1])
                delta = jnp.sum(
                    d_out.astype(f32) * mixed[j, here, head].astype(f32), axis=-1, keepdims=True
                )
                d_scores = probs * (product(d_out, value[:seen], NT) - delta)
                d_scores = d_scores.astype(bf16)
                row.append(jnp.dot(d_scores, key[:seen], preferred_element_type=f32) * scale)
                d_keys[:seen] = d_keys[:seen] + product(d_scores, query, TN) * scale
                d_values[:seen] = d_values[:seen] + product(probs.astype(bf16), d_out, TN)
            d_queries.append(jnp.concatenate(row, axis=1))
        d_query = jnp.concatenate(d_queries, axis=0)
        last = jnp.concatenate([d_query[:, LANES:], d_keys[...]], axis=1)
        d_qkv[j, :, :LANES] = turned_lanes(d_query[:, :LANES], cosine[...], -sine[...]).astype(bf16)
        d_qkv[j, :, LANES : 2 * LANES] = turned_lanes(last, cosine[...], -sine[...]).astype(bf16)
        d_qkv[j, :, 2 * LANES :] = d_values[...].astype(bf16)
        out = product(d_qkv[j], qkv_own[...].reshape(width, -1), NT).astype(bf16)
        parts[j] = out.reshape(shards, DEVICE_TOKENS, width)
        sums[j].begin()
    cut = 2 * grad_qkv.shape[1]
    for i in range(width // cut):
        here = slice(i * cut, (i + 1) * cut)
        value = product(normed[0, :, here], d_qkv[0], TN) + product(
            normed[1, :, here], d_qkv[1], TN
        )
        grad_qkv[2 * i : 2 * i + 2] = value.astype(bf16).reshape(2, cut // 2, -1)
    qkv_move.start()
    order = sums[0].order
    for step, q in enumerate(order):
        for s in sums:
            s.lines(q)
        if step == min(1, len(order) - 1):
            of_small.turn()
            of_output.turn()
        if step == min(2, len(order) - 1):
            qkv_move.wait()
            of_qkv.start()
    for s in sums:
        s.finish()
    of_qkv.turn()
    for s in (of_small, of_output, of_qkv):
        s.wait()
    experts_move.wait()


def rear(
    dh, w_output, normed, qkv_own, turned, log_sums, mixed, cosine, sine, grad_small, grads, held,
    shards, groups, plan,
):
    f32, bf16 = jnp.float32, jnp.bfloat16
    sequences, rows, width = dh.shape
    length = shards * rows
    queries = w_output.shape[0]
    block = jax.ShapeDtypeStruct((1, shards, rows, width), bf16)
    small_shape = grad_small.shape[:1] + grad_small.shape[2:]
    output_shape = (groups, queries // groups, width)
    qkv_plan = Rows(qkv_own)
    scratch = [
        Gather.scratch(dh, False, shards),
        Exchange.scratch(plan.block, bf16, plan.count, shards),
        Exchange.scratch(qkv_plan.block, bf16, qkv_plan.count, shards),
        Reduce.scratch(block, False, shards),
        Reduce.scratch(block, False, shards),
        Reduce.scratch(grad_small, False, shards),
        Across.scratch(qkv_own.shape, bf16),
        Across.scratch(small_shape, f32),
        Across.scratch(output_shape, bf16),
    ]
    any_space, vmem = pl.BlockSpec(memory_space=pl.ANY), pl.BlockSpec(memory_space=pltpu.VMEM)
    return pl.pallas_call(
        functools.partial(
            rear_body, shards, groups, (plan, qkv_plan), tuple(len(s) for s in scratch)
        ),
        out_shape=[
            jax.ShapeDtypeStruct(dh.shape, f32),
            jax.ShapeDtypeStruct(small_shape, f32),
            jax.ShapeDtypeStruct(qkv_own.shape, bf16),
            jax.ShapeDtypeStruct(small_shape, f32),
            jax.ShapeDtypeStruct(output_shape, bf16),
            jax.ShapeDtypeStruct(held.shape, bf16),
        ],
        in_specs=[vmem] * 9 + [any_space] * 3,
        out_specs=[vmem] * 2 + [any_space] * 4,
        scratch_shapes=[
            pltpu.VMEM((sequences, shards, rows, width), bf16),
            pltpu.VMEM((sequences, shards, rows, width), bf16),
            pltpu.VMEM(turned.shape, bf16),
            pltpu.VMEM((length, HEAD_SIZE), f32),
            pltpu.VMEM((length, HEAD_SIZE), f32),
            pltpu.VMEM(qkv_own.shape, bf16),
            pltpu.VMEM(qkv_own.shape, bf16),
            pltpu.VMEM(output_shape, bf16),
        ]
        + [s for some in scratch for s in some],
        input_output_aliases={11: 5},
        compiler_params=pltpu.CompilerParams(
            collective_id=5, has_side_effects=True, vmem_limit_bytes=64 * 1024 * 1024 - 65536
        ),
        cost_estimate=pl.CostEstimate(
            flops=8 * 10**9, bytes_accessed=100 * 10**6, transcendentals=3 * 10**6
        ),
    )(
        dh, w_output, normed, qkv_own, turned, log_sums, mixed, cosine, sine, grad_small, grads,
        held,
    )


def local(
    inputs,
    cotangent,
    routes,
    attn_gain,
    w_query,
    key_matrix,
    value_matrix,
    w_output,
    moe_gain,
    w_router,
    w_experts,
):
    f32, bf16 = jnp.float32, jnp.bfloat16
    shards, groups = lax.axis_size("shard"), lax.axis_size("expert")
    shard, group = lax.axis_index("shard"), lax.axis_index("expert")
    tokens = inputs.shape[0]
    own_rows = attn_gain.shape[0]
    sequences = tokens // DEVICE_TOKENS
    length = shards * DEVICE_TOKENS
    experts_here = E // groups
    blocks = groups * shards
    ratio = QUERY_HEADS // KEY_VALUE_HEADS
    query_width, key_width = ratio * HEAD_SIZE, HEAD_SIZE

    small = jnp.concatenate([w_router, attn_gain[:, None], moe_gain[:, None]], axis=1)
    small = jnp.pad(small, ((0, 0), (0, LANES - E - 2)))
    qkv_cut = jnp.transpose(
        jnp.concatenate(
            [
                w_query.reshape(own_rows, shards, query_width),
                key_matrix.reshape(own_rows, shards, key_width),
                value_matrix.reshape(own_rows, shards, key_width),
            ],
            axis=2,
        ),
        (1, 0, 2),
    )
    experts_cut = jnp.transpose(w_experts, (1, 0, 2))
    cosine, sine = angle_tables(jnp.arange(length, dtype=f32))
    twice = LANES // HEAD_SIZE
    cosine = jnp.tile(cosine, (1, 2 * twice))
    sine = jnp.tile(jnp.concatenate([-sine, sine], axis=1), (1, twice))
    small_all, routes_all, qkv_own, cut_own, normed, turned, log_sums, mixed, attended = front(
        inputs.reshape(sequences, DEVICE_TOKENS, MODEL_WIDTH),
        small[None],
        jnp.transpose(routes)[None],
        w_output,
        cosine,
        sine,
        qkv_cut,
        experts_cut,
        shards,
        groups,
        [Rows(qkv_cut), Experts(experts_cut, shards, experts_here, False, (0, 0), (0, 3))],
    )
    small = small_all.reshape(MODEL_WIDTH, LANES)
    router_pad = jnp.where(jnp.arange(LANES) < E, small, 0)
    router, gain_one, gain_two = small[:, :E], small[:, E].astype(f32), small[:, E + 1].astype(f32)
    inputs_wide = inputs.astype(f32)
    h_one = inputs_wide + attended.reshape(tokens, MODEL_WIDTH)
    r_two = lax.rsqrt(jnp.mean(h_one * h_one, axis=-1, keepdims=True) + EPSILON)
    z_two = h_one * r_two
    n_two = (z_two * gain_two).astype(bf16)

    n_all, c_all, experts_own = gathered(
        [n_two[None], cotangent[None]],
        (True, True),
        shards,
        groups,
        2,
        [experts_cut],
        [Experts(experts_cut, shards, experts_here, False, (0, 3), (0, 0))],
    )
    whole, extra = divmod(experts_here, shards)
    cuts = shards // extra
    owned = [(group * experts_here + shard * whole + i, i * 3 * FF, FF) for i in range(whole)]
    owned.append(
        (group * experts_here + whole * shards + shard // cuts, whole * 3 * FF, FF // cuts)
    )
    slots = -(-CAP // 8) * 8
    routes_pairs = jnp.transpose(
        routes_all.reshape(blocks // 2, 2, TOP, tokens), (0, 2, 1, 3)
    ).reshape(blocks // 2, TOP, 2 * tokens)
    o_sums, d_sums, grads = experts(
        jnp.stack([expert for expert, _, _ in owned]).astype(jnp.int32),
        routes_pairs,
        jnp.transpose(router_pad)[: -(-E // 16) * 16],
        n_all[0],
        c_all[0],
        experts_own,
        cut_own,
        [(start, width) for _, start, width in owned],
        slots,
        2 * TOP,
    )
    back, moe_sum, gate_up = reduced(
        [d_sums[None], o_sums[None]],
        (True, True),
        shards,
        groups,
        3,
        [grads],
        [Experts(grads, shards, experts_here, True, (0, 2), (0, 2))],
    )
    back = back[0]
    outputs = (h_one + moe_sum[0]).astype(bf16)

    logits = jnp.dot(n_two, router, preferred_element_type=f32)
    picks = (routes[:, :, None] == jnp.arange(E, dtype=jnp.int32)).astype(f32)
    weights = jax.nn.softmax(jnp.sum(picks * logits[:, None, :], axis=-1), axis=-1)
    carried = back[tokens:, :tokens]
    d_weights = jnp.transpose(carried[:TOP] + carried[TOP:])
    d_chosen = weights * (d_weights - jnp.sum(weights * d_weights, axis=-1, keepdims=True))
    d_logits = jnp.sum(picks * d_chosen[:, :, None], axis=1).astype(bf16)
    grad_router = jnp.einsum("td,te->de", n_two, d_logits, preferred_element_type=f32)
    d_n_two = jnp.einsum("te,de->td", d_logits, router, preferred_element_type=f32)
    d_n_two = d_n_two + back[:tokens]
    grad_gain_two = jnp.sum(d_n_two * z_two, axis=0)
    dz_two = d_n_two * gain_two
    dh_one = cotangent.astype(f32) + r_two * (
        dz_two - z_two * jnp.mean(dz_two * z_two, axis=-1, keepdims=True)
    )
    grad_small = jnp.concatenate([grad_router, grad_gain_two[:, None]], axis=1).astype(bf16)
    grad_small = jnp.pad(grad_small, ((0, 0), (0, LANES - E - 1)))
    grad_small = jnp.transpose(
        grad_small.reshape(shards, groups, own_rows // groups, LANES), (1, 0, 2, 3)
    )
    dh_rows = dh_one.astype(bf16).reshape(sequences, DEVICE_TOKENS, MODEL_WIDTH)
    d_n_one, _, grad_qkv, grad_small, grad_output, grad_experts = rear(
        dh_rows,
        w_output,
        normed,
        qkv_own,
        turned,
        log_sums,
        mixed,
        cosine,
        sine,
        grad_small,
        grads,
        gate_up,
        shards,
        groups,
        Experts(grads, shards, experts_here, True, (2, 3), (2, 3)),
    )
    grad_output = grad_output.reshape(own_rows, MODEL_WIDTH).astype(f32)
    grad_small = grad_small.reshape(own_rows, LANES)
    grad_experts = jnp.transpose(grad_experts, (1, 0, 2)).astype(f32)

    def columns(start, width):
        part = jnp.transpose(grad_qkv[:, :, start : start + width], (1, 0, 2))
        return part.reshape(own_rows, shards * width).astype(f32)

    grad_query = columns(0, query_width)
    grad_key = columns(query_width, key_width)
    grad_value = columns(query_width + key_width, key_width)
    grad_gain_one = (
        jnp.sum(grad_query * w_query.astype(f32), axis=1)
        + jnp.sum(grad_key * key_matrix.astype(f32), axis=1)
        + jnp.sum(grad_value * value_matrix.astype(f32), axis=1)
    ) / attn_gain.astype(f32)
    r_one = lax.rsqrt(jnp.mean(inputs_wide * inputs_wide, axis=-1, keepdims=True) + EPSILON)
    z_one = inputs_wide * r_one
    dz_one = d_n_one.reshape(tokens, MODEL_WIDTH) * gain_one
    grad_inputs = dh_one + r_one * (
        dz_one - z_one * jnp.mean(dz_one * z_one, axis=-1, keepdims=True)
    )
    return (
        outputs,
        grad_inputs,
        grad_gain_one,
        grad_query,
        grad_key,
        grad_value,
        grad_output,
        grad_small[:, E],
        grad_small[:, :E],
        grad_experts,
    )


def solution(mesh):
    return jax.shard_map(
        local if fits(mesh.shape["shard"], mesh.shape["expert"]) else general,
        mesh=mesh,
        in_specs=(
            P(("expert", "shard"), None),
            P(("expert", "shard"), None),
            P(("expert", "shard"), None),
            P("shard"),
            P("shard", None),
            P("shard", None),
            P("shard", None),
            P("shard", None),
            P("shard"),
            P("shard", None),
            P("shard", "expert", None),
        ),
        out_specs=(
            P(("expert", "shard"), None),
            P(("expert", "shard"), None),
            P("shard"),
            P("shard", None),
            P("shard", None),
            P("shard", None),
            P("shard", None),
            P("shard"),
            P("shard", None),
            P("shard", "expert", None),
        ),
        check_vma=False,
    )
```

```python
import functools

import jax
import jax.numpy as jnp
from jax import lax
from jax.experimental import pallas as pl
from jax.experimental.pallas import tpu as pltpu
from jax.sharding import PartitionSpec as P

MODEL_WIDTH = 1536
QUERY_HEADS = 24
KEY_VALUE_HEADS = 8
HEAD_SIZE = 64
FF = 512
E = 40
TOP = 8
DEVICE_TOKENS = 64
CAP = 38


EPSILON = 1e-06
ROPE_BASE = 10000.0
MASKED = -1e30
LANES = 128


def angle_tables(positions):
    half_width = HEAD_SIZE // 2
    frequency = jnp.power(
        ROPE_BASE, -(jnp.arange(half_width, dtype=jnp.float32) * (2.0 / HEAD_SIZE))
    )
    angles = positions[:, None] * frequency[None, :]
    return (jnp.cos(angles), jnp.sin(angles))


def apply_rotation(values, cosine_table, sines_table):
    half_width = values.shape[-1] // 2
    first_half, second_half = (values[..., :half_width], values[..., half_width:])
    cosine_table, sines_table = (cosine_table[:, None, :], sines_table[:, None, :])
    return jnp.concatenate(
        [
            first_half * cosine_table - second_half * sines_table,
            second_half * cosine_table + first_half * sines_table,
        ],
        axis=-1,
    )


def reverse_rotation(values, cosine_table, sines_table):
    half_width = values.shape[-1] // 2
    first_half, second_half = (values[..., :half_width], values[..., half_width:])
    cosine_table, sines_table = (cosine_table[:, None, :], sines_table[:, None, :])
    return jnp.concatenate(
        [
            first_half * cosine_table + second_half * sines_table,
            second_half * cosine_table - first_half * sines_table,
        ],
        axis=-1,
    )


def general(
    inputs,
    cotangent,
    routes,
    attn_gain,
    w_query,
    key_matrix,
    value_matrix,
    w_output,
    moe_gain,
    w_router,
    w_experts,
):
    rows_local = inputs.shape[0]
    group_count = lax.axis_size("expert")
    experts_here = E // group_count
    group_width = QUERY_HEADS // KEY_VALUE_HEADS
    key_value_width = KEY_VALUE_HEADS * HEAD_SIZE
    scale_factor = 1.0 / HEAD_SIZE
    sequence_count = rows_local // DEVICE_TOKENS
    gain_one, query_full, key_complete, value_full, output_full, router_full, gain_two = (
        lax.all_gather(attn_gain, "shard", axis=0, tiled=True),
        lax.all_gather(w_query, "shard", axis=0, tiled=True),
        lax.all_gather(key_matrix, "shard", axis=0, tiled=True),
        lax.all_gather(value_matrix, "shard", axis=0, tiled=True),
        lax.all_gather(w_output, "shard", axis=0, tiled=True),
        lax.all_gather(w_router, "shard", axis=0, tiled=True),
        lax.all_gather(moe_gain, "shard", axis=0, tiled=True),
    )
    inputs_wide = inputs.astype(jnp.float32)
    r_one = lax.rsqrt(jnp.mean(inputs_wide * inputs_wide, axis=-1, keepdims=True) + EPSILON)
    z_one = inputs_wide * r_one
    normed_first = (z_one * gain_one.astype(jnp.float32)).astype(jnp.bfloat16)
    offset = lax.axis_index("shard") * DEVICE_TOKENS
    positions = offset + jnp.arange(DEVICE_TOKENS, dtype=jnp.int32)
    row_positions = jnp.tile(positions, sequence_count)
    cosine_table, sines_table = angle_tables(row_positions.astype(jnp.float32))
    query_rotated = apply_rotation(
        jnp.dot(normed_first, query_full, preferred_element_type=jnp.float32).reshape(
            rows_local, QUERY_HEADS, HEAD_SIZE
        ),
        cosine_table,
        sines_table,
    ).astype(jnp.bfloat16)
    keys_rot = apply_rotation(
        jnp.dot(normed_first, key_complete, preferred_element_type=jnp.float32).reshape(
            rows_local, KEY_VALUE_HEADS, HEAD_SIZE
        ),
        cosine_table,
        sines_table,
    ).astype(jnp.bfloat16)
    values_narrow = jnp.dot(normed_first, value_full, preferred_element_type=jnp.float32).astype(
        jnp.bfloat16
    )
    kv_local = jnp.concatenate(
        [keys_rot.reshape(rows_local, key_value_width), values_narrow], axis=1
    ).reshape(sequence_count, DEVICE_TOKENS, 2 * key_value_width)
    kv_all = lax.all_gather(kv_local, "shard", axis=1, tiled=True)
    seq_length = kv_all.shape[1]
    block_of_keys = min(512, seq_length)
    total_of_block = (offset + DEVICE_TOKENS + block_of_keys - 1) // block_of_keys
    query_four_dims = query_rotated.reshape(
        sequence_count, DEVICE_TOKENS, KEY_VALUE_HEADS, group_width, HEAD_SIZE
    )

    def scores_for(block_index):
        start_row = block_index * block_of_keys
        key_value_slice = lax.dynamic_slice_in_dim(kv_all, start_row, block_of_keys, 1)
        keys_block = key_value_slice[..., :key_value_width].reshape(
            sequence_count, block_of_keys, KEY_VALUE_HEADS, HEAD_SIZE
        )
        values_block = key_value_slice[..., key_value_width:].reshape(
            sequence_count, block_of_keys, KEY_VALUE_HEADS, HEAD_SIZE
        )
        scores = (
            jnp.einsum(
                "nqjgd,nkjd->njgqk", query_four_dims, keys_block, preferred_element_type=jnp.float32
            )
            * scale_factor
        )
        key_pos = start_row + jnp.arange(block_of_keys, dtype=jnp.int32)
        allowed = key_pos[None, :] <= positions[:, None]
        return (jnp.where(allowed, scores, MASKED), keys_block, values_block)

    def stats_step(block_index, loop_state):
        running_max, running_sum = loop_state
        scores = scores_for(block_index)[0]
        new_max = jnp.maximum(running_max, jnp.max(scores, axis=-1))
        running_sum = running_sum * jnp.exp(running_max - new_max) + jnp.sum(
            jnp.exp(scores - new_max[..., None]), axis=-1
        )
        return (new_max, running_sum)

    statistics_shape = (sequence_count, KEY_VALUE_HEADS, group_width, DEVICE_TOKENS)
    start_stats = (
        jnp.full(statistics_shape, MASKED, jnp.float32),
        jnp.zeros(statistics_shape, jnp.float32),
    )
    run_max, run_sum = lax.fori_loop(0, total_of_block, stats_step, start_stats)
    log_total = run_max + jnp.log(run_sum)

    def mixing_step(block_index, mixed_sum):
        scores, keys_block, values_block = scores_for(block_index)
        attn_probs = jnp.exp(scores - log_total[..., None]).astype(jnp.bfloat16)
        return mixed_sum + jnp.einsum(
            "njgqk,nkjd->nqjgd", attn_probs, values_block, preferred_element_type=jnp.float32
        )

    attention_mixed = lax.fori_loop(
        0,
        total_of_block,
        mixing_step,
        jnp.zeros(
            (sequence_count, DEVICE_TOKENS, KEY_VALUE_HEADS, group_width, HEAD_SIZE), jnp.float32
        ),
    )
    attention_mixed = attention_mixed.reshape(rows_local, QUERY_HEADS * HEAD_SIZE).astype(
        jnp.bfloat16
    )
    h_one = inputs_wide + jnp.dot(attention_mixed, output_full, preferred_element_type=jnp.float32)
    r_two = lax.rsqrt(jnp.mean(h_one * h_one, axis=-1, keepdims=True) + EPSILON)
    z_two = h_one * r_two
    n_two = (z_two * gain_two.astype(jnp.float32)).astype(jnp.bfloat16)
    logits = jnp.dot(n_two, router_full, preferred_element_type=jnp.float32)
    expert_ids = jnp.arange(E, dtype=jnp.int32)
    route_picks = (routes[:, :, None] == expert_ids[None, None, :]).astype(jnp.float32)
    chosen = jnp.sum(route_picks * logits[:, None, :], axis=-1)
    weights = jax.nn.softmax(chosen, axis=-1)
    flat_routes = routes.reshape(-1)
    route_hits = (flat_routes[:, None] == expert_ids[None, :]).astype(jnp.int32)
    route_ranks = jnp.sum(jnp.cumsum(route_hits, axis=0) * route_hits, axis=1) - 1
    targets = flat_routes * CAP + route_ranks
    token_of = jnp.arange(rows_local * TOP, dtype=jnp.int32) // TOP
    outgoing = jnp.zeros((E * CAP, MODEL_WIDTH), jnp.bfloat16).at[targets].set(n_two[token_of])
    arrived = lax.all_to_all(
        outgoing.reshape(group_count, experts_here, CAP, MODEL_WIDTH),
        "expert",
        split_axis=0,
        concat_axis=0,
        tiled=True,
    )
    expert_full = lax.all_gather(w_experts, "shard", axis=0, tiled=True)
    gate_and_up = expert_full[:, :, : 2 * FF]
    down_part = expert_full[:, :, 2 * FF :]
    both_parts = jnp.einsum(
        "sjcd,djf->sjcf", arrived, gate_and_up, preferred_element_type=jnp.float32
    )
    gate_part = both_parts[..., :FF]
    upper_part = both_parts[..., FF:]
    sigmoid_gate = jax.nn.sigmoid(gate_part)
    activated = (gate_part * sigmoid_gate * upper_part).astype(jnp.bfloat16)
    produced = jnp.einsum(
        "sjcf,djf->sjcd", activated, down_part, preferred_element_type=jnp.float32
    ).astype(jnp.bfloat16)
    returned = lax.all_to_all(produced, "expert", split_axis=0, concat_axis=0, tiled=True).reshape(
        E * CAP, MODEL_WIDTH
    )
    route_out = returned[targets].reshape(rows_local, TOP, MODEL_WIDTH).astype(jnp.float32)
    moe_sum = jnp.sum(weights[:, :, None] * route_out, axis=1)
    outputs = (h_one + moe_sum).astype(jnp.bfloat16)
    dy_wide = cotangent.astype(jnp.float32)
    d_routes = (
        (weights[:, :, None] * dy_wide[:, None, :])
        .astype(jnp.bfloat16)
        .reshape(rows_local * TOP, MODEL_WIDTH)
    )
    d_outgoing = jnp.zeros((E * CAP, MODEL_WIDTH), jnp.bfloat16).at[targets].set(d_routes)
    d_arrived = lax.all_to_all(
        d_outgoing.reshape(group_count, experts_here, CAP, MODEL_WIDTH),
        "expert",
        split_axis=0,
        concat_axis=0,
        tiled=True,
    )
    d_weights = jnp.sum(dy_wide[:, None, :] * route_out, axis=-1)
    d_chosen = weights * (d_weights - jnp.sum(weights * d_weights, axis=-1, keepdims=True))
    d_logits = jnp.sum(route_picks * d_chosen[:, :, None], axis=1).astype(jnp.bfloat16)
    grad_router = jnp.einsum("td,te->de", n_two, d_logits, preferred_element_type=jnp.float32)
    d_act = jnp.einsum("sjcd,djf->sjcf", d_arrived, down_part, preferred_element_type=jnp.float32)
    d_gate_up = jnp.concatenate(
        [
            d_act * upper_part * sigmoid_gate * (1.0 + gate_part * (1.0 - sigmoid_gate)),
            d_act * gate_part * sigmoid_gate,
        ],
        axis=-1,
    ).astype(jnp.bfloat16)
    d_rows = jnp.einsum(
        "sjcf,djf->sjcd", d_gate_up, gate_and_up, preferred_element_type=jnp.float32
    ).astype(jnp.bfloat16)
    d_returned = lax.all_to_all(d_rows, "expert", split_axis=0, concat_axis=0, tiled=True).reshape(
        E * CAP, MODEL_WIDTH
    )
    d_n_two = jnp.einsum(
        "te,de->td", d_logits, router_full, preferred_element_type=jnp.float32
    ) + jnp.sum(
        d_returned[targets].reshape(rows_local, TOP, MODEL_WIDTH).astype(jnp.float32), axis=1
    )
    first_part = jnp.einsum(
        "sjcd,sjcf->djf", arrived, d_gate_up, preferred_element_type=jnp.float32
    )
    second = jnp.einsum("sjcd,sjcf->djf", d_arrived, activated, preferred_element_type=jnp.float32)
    grad_experts = lax.psum_scatter(
        jnp.concatenate([first_part, second], axis=2).astype(jnp.bfloat16),
        "shard",
        scatter_dimension=0,
        tiled=True,
    ).astype(jnp.float32)
    grad_gain_two = jnp.sum(d_n_two * z_two, axis=0)
    dz_two = d_n_two * gain_two.astype(jnp.float32)
    dh_one = dy_wide + r_two * (dz_two - z_two * jnp.mean(dz_two * z_two, axis=-1, keepdims=True))
    dh_narrow = dh_one.astype(jnp.bfloat16)
    grad_output = jnp.einsum(
        "tk,td->kd", attention_mixed, dh_narrow, preferred_element_type=jnp.float32
    )
    mixed_gradient = jnp.einsum(
        "td,kd->tk", dh_narrow, output_full, preferred_element_type=jnp.float32
    ).astype(jnp.bfloat16)
    grad_four_dims = mixed_gradient.reshape(
        sequence_count, DEVICE_TOKENS, KEY_VALUE_HEADS, group_width, HEAD_SIZE
    )
    row_difference = jnp.sum(
        grad_four_dims.astype(jnp.float32)
        * attention_mixed.reshape(
            sequence_count, DEVICE_TOKENS, KEY_VALUE_HEADS, group_width, HEAD_SIZE
        ).astype(jnp.float32),
        axis=-1,
    )
    row_difference = jnp.transpose(row_difference, (0, 2, 3, 1))

    def grad_step(block_index, loop_state):
        d_query_sum, d_key_rows = loop_state
        scores, keys_block, values_block = scores_for(block_index)
        attn_probs = jnp.exp(scores - log_total[..., None])
        d_probs = jnp.einsum(
            "nqjgd,nkjd->njgqk", grad_four_dims, values_block, preferred_element_type=jnp.float32
        )
        d_scores = (attn_probs * (d_probs - row_difference[..., None])).astype(jnp.bfloat16)
        d_query_sum = (
            d_query_sum
            + jnp.einsum(
                "njgqk,nkjd->nqjgd", d_scores, keys_block, preferred_element_type=jnp.float32
            )
            * scale_factor
        )
        key_grad = (
            jnp.einsum(
                "njgqk,nqjgd->nkjd", d_scores, query_four_dims, preferred_element_type=jnp.float32
            )
            * scale_factor
        )
        value_grad = jnp.einsum(
            "njgqk,nqjgd->nkjd",
            attn_probs.astype(jnp.bfloat16),
            grad_four_dims,
            preferred_element_type=jnp.float32,
        )
        update = jnp.concatenate(
            [
                key_grad.reshape(sequence_count, block_of_keys, key_value_width),
                value_grad.reshape(sequence_count, block_of_keys, key_value_width),
            ],
            axis=2,
        )
        d_key_rows = lax.dynamic_update_slice_in_dim(
            d_key_rows, update, block_index * block_of_keys, 1
        )
        return (d_query_sum, d_key_rows)

    start_grads = (
        jnp.zeros(
            (sequence_count, DEVICE_TOKENS, KEY_VALUE_HEADS, group_width, HEAD_SIZE), jnp.float32
        ),
        jnp.zeros((sequence_count, seq_length, 2 * key_value_width), jnp.float32),
    )
    d_query_sum, d_key_rows = lax.fori_loop(0, total_of_block, grad_step, start_grads)
    owned_keys = (
        lax.psum_scatter(d_key_rows.astype(jnp.bfloat16), "shard", scatter_dimension=1, tiled=True)
        .astype(jnp.float32)
        .reshape(rows_local, 2 * key_value_width)
    )
    d_query = (
        reverse_rotation(
            d_query_sum.reshape(rows_local, QUERY_HEADS, HEAD_SIZE), cosine_table, sines_table
        )
        .reshape(rows_local, QUERY_HEADS * HEAD_SIZE)
        .astype(jnp.bfloat16)
    )
    key_gradient = (
        reverse_rotation(
            owned_keys[:, :key_value_width].reshape(rows_local, KEY_VALUE_HEADS, HEAD_SIZE),
            cosine_table,
            sines_table,
        )
        .reshape(rows_local, key_value_width)
        .astype(jnp.bfloat16)
    )
    value_gradient = owned_keys[:, key_value_width:].astype(jnp.bfloat16)
    grad_query = jnp.einsum("td,tk->dk", normed_first, d_query, preferred_element_type=jnp.float32)
    grad_key = jnp.einsum(
        "td,tk->dk", normed_first, key_gradient, preferred_element_type=jnp.float32
    )
    grad_value = jnp.einsum(
        "td,tk->dk", normed_first, value_gradient, preferred_element_type=jnp.float32
    )
    d_n_one = (
        jnp.einsum("tk,dk->td", d_query, query_full, preferred_element_type=jnp.float32)
        + jnp.einsum("tk,dk->td", key_gradient, key_complete, preferred_element_type=jnp.float32)
        + jnp.einsum("tk,dk->td", value_gradient, value_full, preferred_element_type=jnp.float32)
    )
    grad_gain_one = jnp.sum(d_n_one * z_one, axis=0)
    dz_one = d_n_one * gain_one.astype(jnp.float32)
    grad_inputs = dh_one + r_one * (
        dz_one - z_one * jnp.mean(dz_one * z_one, axis=-1, keepdims=True)
    )
    totals = (
        lax.psum_scatter(
            grad_gain_one.astype(jnp.bfloat16), "shard", scatter_dimension=0, tiled=True
        ).astype(jnp.float32),
        lax.psum_scatter(
            grad_query.astype(jnp.bfloat16), "shard", scatter_dimension=0, tiled=True
        ).astype(jnp.float32),
        lax.psum_scatter(
            grad_key.astype(jnp.bfloat16), "shard", scatter_dimension=0, tiled=True
        ).astype(jnp.float32),
        lax.psum_scatter(
            grad_value.astype(jnp.bfloat16), "shard", scatter_dimension=0, tiled=True
        ).astype(jnp.float32),
        lax.psum_scatter(
            grad_output.astype(jnp.bfloat16), "shard", scatter_dimension=0, tiled=True
        ).astype(jnp.float32),
        lax.psum_scatter(
            grad_router.astype(jnp.bfloat16), "shard", scatter_dimension=0, tiled=True
        ).astype(jnp.float32),
        lax.psum_scatter(
            grad_gain_two.astype(jnp.bfloat16), "shard", scatter_dimension=0, tiled=True
        ).astype(jnp.float32),
    )
    totals = (
        lax.psum(totals[0].astype(jnp.bfloat16), "expert").astype(jnp.float32),
        lax.psum(totals[1].astype(jnp.bfloat16), "expert").astype(jnp.float32),
        lax.psum(totals[2].astype(jnp.bfloat16), "expert").astype(jnp.float32),
        lax.psum(totals[3].astype(jnp.bfloat16), "expert").astype(jnp.float32),
        lax.psum(totals[4].astype(jnp.bfloat16), "expert").astype(jnp.float32),
        lax.psum(totals[5].astype(jnp.bfloat16), "expert").astype(jnp.float32),
        lax.psum(totals[6].astype(jnp.bfloat16), "expert").astype(jnp.float32),
    )
    return (
        outputs,
        grad_inputs,
        totals[0],
        totals[1],
        totals[2],
        totals[3],
        totals[4],
        totals[6],
        totals[5],
        grad_experts,
    )


def fits(shards, groups):
    if groups != 4 or shards != KEY_VALUE_HEADS or shards % 2 or E % groups:
        return False
    extra = E // groups % shards
    return E // groups > shards and extra > 0 and FF % (shards // extra * LANES) == 0


def alternating(depth):
    order = []
    low, high = 0, depth - 1
    while low <= high:
        order.append(high)
        if low != high:
            order.append(low)
        low, high = low + 1, high - 1
    return order


def sent(source, target, send, receive, group, shard):
    return pltpu.make_async_remote_copy(
        src_ref=source,
        dst_ref=target,
        send_sem=send,
        recv_sem=receive,
        device_id=(group, shard),
        device_id_type=pl.DeviceIdType.MESH,
    )


class Place:
    def __init__(self, shards, groups):
        self.group, self.shard = lax.axis_index("expert"), lax.axis_index("shard")
        self.shards, self.groups = shards, groups
        self.depth = shards // 2
        self.spot, self.core = self.shard // 2, self.shard % 2
        self.first = self.group + 1 - 2 * (self.group % 2)
        self.second = (self.group + 2) % 4
        self.corner = (self.first + 2) % 4
        self.partner = self.shard + 1 - 2 * self.core

    def greet(self, wide, whole_line, corner=False):
        barrier = pltpu.get_barrier_semaphore()

        def signal(group, shard):
            pl.semaphore_signal(
                barrier, inc=1, device_id=(group, shard), device_id_type=pl.DeviceIdType.MESH
            )

        more = (2 if wide else 0) + (1 if corner else 0)
        if wide:
            signal(self.first, self.shard)
            signal(self.second, self.shard)
        if corner:
            signal(self.corner, self.shard)
        if whole_line:
            for i in range(1, self.shards):
                signal(self.group, (self.shard + i) % self.shards)
            pl.semaphore_wait(barrier, more + self.shards - 1)
            return
        signal(self.group, self.partner)
        inside = (self.spot > 0) & (self.spot < self.depth - 1)

        @pl.when(self.spot > 0)
        def _():
            signal(self.group, self.shard - 2)

        @pl.when(self.spot < self.depth - 1)
        def _():
            signal(self.group, self.shard + 2)

        @pl.when(inside)
        def _():
            pl.semaphore_wait(barrier, more + 3)

        @pl.when(jnp.logical_not(inside))
        def _():
            pl.semaphore_wait(barrier, more + 2)


class Exchange:
    @staticmethod
    def scratch(block, dtype, pieces, n):
        dma = pltpu.SemaphoreType.DMA
        return [pltpu.VMEM(block, dtype), dma((2, pieces)), dma((n, pieces)), dma((n, pieces))]

    def __init__(self, at, plan, source, target, stage, own, out, come):
        self.at, self.source, self.target = at, source, target
        self.stage, self.own, self.out, self.come = stage, own, out, come
        self.take, self.give, self.parts = plan.take, plan.give, plan.parts

    def copies(self, i):
        at = self.at
        to = (at.shard + i) % at.shards
        for k, (taken, given) in enumerate(zip(self.take(to), self.give(at.shard))):
            yield sent(
                self.source.at[taken],
                self.target.at[given],
                self.out.at[i, k],
                self.come.at[i, k],
                at.group,
                to,
            )

    def keep(self, way):
        here = self.at.shard
        for k, (taken, given) in enumerate(zip(self.take(here), self.give(here))):
            held = self.stage.at[self.parts[k]]
            if way == 0:
                yield pltpu.make_async_copy(self.source.at[taken], held, self.own.at[0, k])
            else:
                yield pltpu.make_async_copy(held, self.target.at[given], self.own.at[1, k])

    def start(self):
        for copy in self.keep(0):
            copy.start()
        for i in range(self.at.shards - 1, 0, -1):
            for copy in self.copies(i):
                copy.start()
        for copy in self.keep(0):
            copy.wait()
        for copy in self.keep(1):
            copy.start()

    def wait(self):
        for copy in self.keep(1):
            copy.wait()
        for i in range(1, self.at.shards):
            for copy in self.copies(i):
                copy.wait()


class Rows:
    def __init__(self, array):
        self.shape, self.block, self.count = array.shape, array.shape[1:], 1
        self.parts = [...]

    def take(self, i):
        return [i]

    def give(self, me):
        return [me]


class Experts:
    def __init__(self, shape, shards, experts_here, back, sixths, shared):
        self.back, self.sixths = back, sixths
        self.cut_thirds = (0, 3) if shared else (0, 0)
        self.whole, self.extra = divmod(experts_here, shards)
        self.shards = shards
        self.cuts = shards // self.extra if self.extra else 1
        self.width = FF // self.cuts
        rows = shape[1]
        held = 3 * (FF * self.whole + (self.width if self.extra else 0))
        self.shape = (experts_here, rows, 3 * FF) if back else (shards, rows, held)
        self.block = (rows, held)
        self.parts = [cut for _, cut in self.owner_cuts()]
        self.count = len(self.parts)

    def owner_cuts(self):
        cuts = []
        first, last = self.sixths
        for i in range(self.whole if last > first else 0):
            start = 3 * i * FF + first * FF // 2
            cuts.append((i, pl.ds(start, (last - first) * FF // 2)))
        start = self.whole * 3 * FF
        for k in range(*self.cut_thirds):
            cuts.append((k, pl.ds(start + k * self.width, self.width)))
        return [(k, (slice(None), cut)) for k, cut in cuts]

    def owner(self, i):
        return [(i, *cut) for _, cut in self.owner_cuts()]

    def outside(self, i):
        cuts = []
        first, last = self.sixths
        for k in range(self.whole if last > first else 0):
            here = pl.ds(first * FF // 2, (last - first) * FF // 2)
            cuts.append((i * self.whole + k, slice(None), here))
        for k in range(*self.cut_thirds):
            expert = self.whole * self.shards + i // self.cuts
            start = pl.multiple_of(k * FF + i % self.cuts * self.width, 128)
            cuts.append((expert, slice(None), pl.ds(start, self.width)))
        return cuts

    def take(self, i):
        return self.owner(i) if self.back else self.outside(i)

    def give(self, me):
        return self.outside(me) if self.back else self.owner(me)


def quarter(ref, group, size, axis):
    here = pl.ds(pl.multiple_of(group * size, 16) if axis else group * size, size)
    return ref.at[:, here] if axis else ref.at[here]


class Spread:
    @staticmethod
    def scratch():
        return [pltpu.SemaphoreType.DMA((4,)), pltpu.SemaphoreType.DMA((4,))]

    def __init__(self, at, source, target, axis, out, come):
        self.at, self.source, self.out, self.come = at, source, out, come
        self.target = quarter(target, at.group, source.shape[axis], axis)

    def copies(self):
        at = self.at
        for i, peer in ((3, at.corner), (1, at.first), (2, at.second)):
            yield sent(
                self.source, self.target, self.out.at[i], self.come.at[i], peer, at.shard
            )

    def own(self):
        return pltpu.make_async_copy(self.source, self.target, self.come.at[0])

    def start(self):
        self.own().start()
        for copy in self.copies():
            copy.start()

    def wait(self):
        self.own().wait()
        for copy in self.copies():
            copy.wait()


class Across:
    @staticmethod
    def scratch(shape, dtype, axis=0):
        block = shape[:axis] + (shape[axis] // 4,) + shape[axis + 1 :]
        dma = pltpu.SemaphoreType.DMA
        return [pltpu.VMEM((4,) + block, dtype), pltpu.VMEM(block, dtype), dma((4,)), dma((4,))]

    def __init__(self, at, source, axis, held, mine, out, come):
        self.at, self.source, self.axis, self.held, self.mine = at, source, axis, held, mine
        self.out, self.come = out, come

    def part(self, group):
        return quarter(self.source, group, self.mine.shape[self.axis], self.axis)

    def copies(self):
        at = self.at
        for i, peer in ((3, at.corner), (1, at.first), (2, at.second)):
            yield sent(
                self.part(peer),
                self.held.at[i],
                self.out.at[i],
                self.come.at[i],
                peer,
                at.shard,
            )

    def own(self):
        return pltpu.make_async_copy(self.part(self.at.group), self.held.at[0], self.come.at[0])

    def start(self):
        self.own().start()
        for copy in self.copies():
            copy.start()

    def add(self):
        self.own().wait()
        for copy in self.copies():
            copy.wait()
        total = self.held[0].astype(jnp.float32)
        for i in range(1, 4):
            total = total + self.held[i].astype(jnp.float32)
        self.mine[...] = total.astype(self.mine.dtype)


class Gather:
    @staticmethod
    def scratch(array, wide, shards):
        steps = shards // 2 - 1
        marks = 1 + 2 * steps
        dma = pltpu.SemaphoreType.DMA
        turns = 2 if wide else 1
        return [
            dma((1,)),
            dma((2 * steps,)),
            dma((2 * steps,)),
            dma((turns, marks)),
            dma((turns, marks)),
            dma((turns, marks)),
            dma((turns, marks)),
            dma((5 if wide else 1, marks)),
            dma((5 if wide else 1, marks)),
        ]

    def __init__(self, at, wide, block, out, *sems):
        self.at, self.wide, self.block, self.out = at, wide, block, out
        self.own, self.z_out, self.z_in, self.p_out, self.p_in = sems[:5]
        self.h_out, self.h_in, self.c_out, self.c_in = sems[5:]
        self.steps = at.depth - 1
        self.events = [(0, 0)]
        for t in range(self.steps):
            self.events += [(1, t), (2, t)]

    def when(self, event, body):
        kind, t = event
        if kind == 0:
            body()
        elif kind == 1:
            pl.when(self.at.spot - 1 - t >= 0)(body)
        else:
            pl.when(self.at.spot + 1 + t < self.at.depth)(body)

    def origin(self, event):
        kind, t = event
        return self.at.shard + (0, -2 * (t + 1), 2 * (t + 1))[kind]

    def slot(self, group, shard):
        index = group * self.at.shards + shard if self.wide else shard
        return self.out.at[:, index]

    def half(self, ref, which):
        rows = ref.shape[1]
        cut = rows // 32 * 16
        return ref.at[:, pl.ds(0, cut)] if which == 0 else ref.at[:, pl.ds(cut, rows - cut)]

    def line(self, step, direction, shard):
        at = self.at
        k = direction * self.steps + step
        ref = self.slot(at.group, shard)
        source = self.block if step == 0 else ref
        to = at.shard + (2, -2)[direction]
        return sent(source, ref, self.z_out.at[k], self.z_in.at[k], at.group, to)

    def side(self, k, which):
        at, event = self.at, self.events[k]
        ref = self.slot(at.group, self.origin(event))
        source = self.block if event[0] == 0 else ref
        group = (at.first, at.second)[which]
        return sent(source, ref, self.p_out.at[which, k], self.p_in.at[which, k], group, at.shard)

    def turn(self, k, which):
        at = self.at
        shard = self.origin(self.events[k])
        held = self.half(self.slot((at.first, at.second)[which], shard), which)
        group = (at.second, at.first)[which]
        return sent(held, held, self.h_out.at[which, k], self.h_in.at[which, k], group, at.shard)

    def across(self, k, kind):
        at, event = self.at, self.events[k]
        shard = self.origin(event)
        if kind < 3:
            ref = self.slot((at.group, at.first, at.second)[kind], shard)
        else:
            ref = self.half(self.slot(at.corner, shard), kind - 3)
        source = self.block if kind == 0 and event[0] == 0 else ref
        return sent(
            source, ref, self.c_out.at[kind, k], self.c_in.at[kind, k], at.group, at.partner
        )

    def keep(self):
        here = self.slot(self.at.group, self.at.shard)
        return pltpu.make_async_copy(self.block, here, self.own.at[0])

    def onward(self, event, act):
        kind, t = event
        for direction in range(2):
            if kind and direction != kind - 1:
                continue
            step = 0 if kind == 0 else t + 1
            if step >= self.steps:
                continue
            ahead = self.at.spot < self.at.depth - 1 if direction == 0 else self.at.spot > 0
            pl.when(ahead)(
                lambda step=step, direction=direction: act(
                    self.line(step, direction, self.origin(event))
                )
            )

    def lines(self, k):
        event = self.events[k]

        def body():
            kind, t = event
            if kind:
                self.line(t, kind - 1, self.origin(event)).wait_recv()
            self.onward(event, lambda copy: copy.start())
            if self.wide:
                self.side(k, 0).start()
                self.side(k, 1).start()
            self.across(k, 0).start()
            if kind == 0:
                self.keep().start()

        self.when(event, body)

    def sides(self, k):
        def body():
            for which in range(2):
                self.side(k, which).wait_recv()
                self.turn(k, which).start()
                self.across(k, 1 + which).start()

        if self.wide:
            self.when(self.events[k], body)

    def turns(self, k):
        def body():
            for which in range(2):
                self.turn(k, which).wait_recv()
                self.across(k, 3 + which).start()

        if self.wide:
            self.when(self.events[k], body)

    def finish(self, k):
        event = self.events[k]

        def body():
            if event[0] == 0:
                self.keep().wait()
            self.onward(event, lambda copy: copy.wait_send())
            for kind in range(5 if self.wide else 1):
                copy = self.across(k, kind)
                copy.wait_send()
                copy.wait_recv()
            if self.wide:
                for which in range(2):
                    self.side(k, which).wait_send()
                    self.turn(k, which).wait_send()

        self.when(event, body)


class Reduce:
    @staticmethod
    def scratch(parts, wide, shards):
        depth = shards // 2
        block = (parts.shape[0],) + parts.shape[2:]
        kinds = 4 if wide else 1
        dma = pltpu.SemaphoreType.DMA
        out = [
            pltpu.VMEM((kinds, depth) + block, parts.dtype),
            pltpu.VMEM((kinds, depth) + block, parts.dtype),
            pltpu.VMEM((2, depth) + block, parts.dtype),
            dma((kinds, depth)),
            dma((kinds, depth)),
            dma((kinds, depth)),
            dma((2, depth)),
            dma((2, depth)),
        ]
        if wide:
            cut = block[1] // 32 * 16
            out += [
                pltpu.VMEM((depth, block[0], cut, block[2]), parts.dtype),
                pltpu.VMEM((depth, block[0], block[1] - cut, block[2]), parts.dtype),
                pltpu.VMEM((2, depth) + block, parts.dtype),
                dma((2, depth)),
                dma((2, depth)),
                dma((2, depth)),
                dma((2, depth)),
            ]
        return out

    def __init__(self, at, wide, parts, total, *scratch):
        self.at, self.wide, self.parts, self.total = at, wide, parts, total
        self.mine, self.accs, self.z_buf, self.own = scratch[:4]
        self.c_out, self.c_in, self.z_out, self.z_in = scratch[4:8]
        if wide:
            self.h_buf, self.p_buf = scratch[8:10], scratch[10]
            self.h_out, self.h_in, self.p_out, self.p_in = scratch[11:]
        self.order = alternating(at.depth)
        self.kinds = (3, 1, 2, 0) if wide else (0,)
        self.columns = (at.group, at.first, at.second, at.corner)

    def place(self, kind, q, core):
        shard = 2 * q + core
        return self.columns[kind] * self.at.shards + shard if self.wide else shard

    def load(self, kind, q):
        return pltpu.make_async_copy(
            self.parts.at[:, self.place(kind, q, self.at.core)],
            self.mine.at[kind, q],
            self.own.at[kind, q],
        )

    def across(self, kind, q):
        return sent(
            self.parts.at[:, self.place(kind, q, 1 - self.at.core)],
            self.accs.at[kind, q],
            self.c_out.at[kind, q],
            self.c_in.at[kind, q],
            self.at.group,
            self.at.partner,
        )

    def span(self, which):
        rows = self.accs.shape[3]
        cut = rows // 32 * 16
        return pl.ds(0, cut) if which == 0 else pl.ds(cut, rows - cut)

    def turn(self, q, which):
        return sent(
            self.accs.at[3, q, :, self.span(which)],
            self.h_buf[which].at[q],
            self.h_out.at[which, q],
            self.h_in.at[which, q],
            (self.at.first, self.at.second)[which],
            self.at.shard,
        )

    def side(self, q, which):
        return sent(
            self.accs.at[1 + which, q],
            self.p_buf.at[which, q],
            self.p_out.at[which, q],
            self.p_in.at[which, q],
            (self.at.first, self.at.second)[which],
            self.at.shard,
        )

    def line(self, q, direction):
        return sent(
            self.accs.at[0, q],
            self.z_buf.at[direction, q],
            self.z_out.at[direction, q],
            self.z_in.at[direction, q],
            self.at.group,
            self.at.shard + (2, -2)[direction],
        )

    def add(self, kind, q, *others):
        value = self.accs[kind, q].astype(jnp.float32)
        for other in others:
            value = value + other.astype(jnp.float32)
        self.accs[kind, q] = value.astype(self.accs.dtype)

    def pair(self, kind, q):
        self.load(kind, q).wait()
        self.across(kind, q).wait_recv()
        self.add(kind, q, self.mine[kind, q])

    def begin(self):
        for kind in self.kinds:
            for q in self.order:
                self.load(kind, q).start()
                self.across(kind, q).start()

    def corners(self):
        for q in self.order:
            self.pair(3, q)
            self.turn(q, 0).start()
            self.turn(q, 1).start()

    def sides(self):
        for q in self.order:
            for which in range(2):
                kind = 2 - which
                self.pair(kind, q)
                self.turn(q, which).wait_recv()
                span = self.span(which)
                value = self.accs[kind, q, :, span].astype(jnp.float32)
                value = value + self.h_buf[which][q].astype(jnp.float32)
                self.accs[kind, q, :, span] = value.astype(self.accs.dtype)
                self.side(q, kind - 1).start()

    def lines(self, q):
        at = self.at
        self.pair(0, q)
        if self.wide:
            self.side(q, 0).wait_recv()
            self.side(q, 1).wait_recv()
            self.add(0, q, self.p_buf[0, q], self.p_buf[1, q])
        for direction in range(2):

            @pl.when(q > at.spot if direction == 0 else q < at.spot)
            def _(direction=direction):
                @pl.when(at.spot > 0 if direction == 0 else at.spot < at.depth - 1)
                def _():
                    self.line(q, direction).wait_recv()
                    self.add(0, q, self.z_buf[direction, q])

                self.line(q, direction).start()

    def finish(self):
        at, total = self.at, self.total
        for q in range(at.depth):

            @pl.when(q == at.spot)
            def _(q=q):
                total[...] = self.accs[0, q].astype(jnp.float32)
                for direction in range(2):
                    if q > 0 if direction == 0 else q < at.depth - 1:
                        self.line(q, direction).wait_recv()
                        total[...] = total[...] + self.z_buf[direction, q].astype(jnp.float32)

            for kind in self.kinds:
                self.across(kind, q).wait_send()
            if self.wide:
                for which in range(2):
                    self.turn(q, which).wait_send()
                    self.side(q, which).wait_send()
            for direction in range(2):

                @pl.when(q > at.spot if direction == 0 else q < at.spot)
                def _(q=q, direction=direction):
                    self.line(q, direction).wait_send()


def cut_refs(refs, sizes):
    out, start = [], 0
    for size in sizes:
        out.append(refs[start : start + size])
        start += size
    return out


def gather_body(shards, groups, wides, plans, sizes, *refs):
    count = len(wides) + len(plans)
    ins, outs = refs[:count], refs[count : 2 * count]
    scratch = cut_refs(refs[2 * count :], sizes)
    at = Place(shards, groups)
    at.greet(any(wides), len(plans) > 0)
    gathers = [Gather(at, wide, ins[i], outs[i], *scratch[i]) for i, wide in enumerate(wides)]
    moves = [
        Exchange(at, plan, ins[i], outs[i], *scratch[i])
        for i, plan in enumerate(plans, len(wides))
    ]
    marks = range(len(gathers[0].events))
    for k in marks:
        for g in gathers:
            g.lines(k)
    for m in moves:
        m.start()
    for step in (Gather.sides, Gather.turns, Gather.finish):
        for k in marks:
            for g in gathers:
                step(g, k)
    for m in moves:
        m.wait()


def gathered(arrays, wides, shards, groups, identity, swapped=(), plans=()):
    shapes = [
        jax.ShapeDtypeStruct(
            (a.shape[0], shards * (groups if wide else 1)) + a.shape[1:], a.dtype
        )
        for a, wide in zip(arrays, wides)
    ] + [jax.ShapeDtypeStruct(p.shape, a.dtype) for a, p in zip(swapped, plans)]
    moved = sum(s.size * s.dtype.itemsize for s in shapes)
    scratch = [Gather.scratch(a, wide, shards) for a, wide in zip(arrays, wides)]
    scratch += [Exchange.scratch(p.block, a.dtype, p.count, shards) for a, p in zip(swapped, plans)]
    return pl.pallas_call(
        functools.partial(
            gather_body, shards, groups, tuple(wides), tuple(plans), tuple(len(s) for s in scratch)
        ),
        out_shape=shapes,
        in_specs=[pl.BlockSpec(memory_space=pltpu.VMEM)] * len(arrays)
        + [pl.BlockSpec(memory_space=pl.ANY)] * len(swapped),
        out_specs=[pl.BlockSpec(memory_space=pl.ANY)] * len(shapes),
        scratch_shapes=[s for some in scratch for s in some],
        compiler_params=pltpu.CompilerParams(collective_id=identity, has_side_effects=True),
        cost_estimate=pl.CostEstimate(flops=0, bytes_accessed=20 * moved, transcendentals=0),
    )(*arrays, *swapped)


def reduce_body(shards, groups, wides, plans, sizes, *refs):
    count = len(wides) + len(plans)
    ins, outs = refs[:count], refs[count + len(plans) : 2 * count + len(plans)]
    scratch = cut_refs(refs[2 * count + len(plans) :], sizes)
    at = Place(shards, groups)
    at.greet(any(wides), len(plans) > 0)
    sums = [Reduce(at, wide, ins[i], outs[i], *scratch[i]) for i, wide in enumerate(wides)]
    moves = [
        Exchange(at, plan, ins[i], outs[i], *scratch[i])
        for i, plan in enumerate(plans, len(wides))
    ]
    for r in sums:
        r.begin()
    for m in moves:
        m.start()
    for r in sums:
        if r.wide:
            r.corners()
    for r in sums:
        if r.wide:
            r.sides()
        for q in r.order:
            r.lines(q)
    for r in sums:
        r.finish()
    for m in moves:
        m.wait()


def reduced(arrays, wides, shards, groups, identity, swapped=(), plans=(), held=()):
    shapes = [
        jax.ShapeDtypeStruct((a.shape[0],) + a.shape[2:], jnp.float32) for a in arrays
    ] + [jax.ShapeDtypeStruct(p.shape, a.dtype) for a, p in zip(swapped, plans)]
    operands = (*arrays, *swapped, *held)
    moved = sum(a.size * a.dtype.itemsize for a in operands)
    scratch = [Reduce.scratch(a, wide, shards) for a, wide in zip(arrays, wides)]
    scratch += [Exchange.scratch(p.block, a.dtype, p.count, shards) for a, p in zip(swapped, plans)]
    return pl.pallas_call(
        functools.partial(
            reduce_body, shards, groups, tuple(wides), tuple(plans), tuple(len(s) for s in scratch)
        ),
        out_shape=shapes,
        in_specs=[pl.BlockSpec(memory_space=pl.ANY)] * len(operands),
        out_specs=[pl.BlockSpec(memory_space=pltpu.VMEM)] * len(arrays)
        + [pl.BlockSpec(memory_space=pl.ANY)] * len(swapped),
        scratch_shapes=[s for some in scratch for s in some],
        input_output_aliases={
            len(arrays) + len(swapped) + i: len(arrays) + i for i in range(len(held))
        },
        compiler_params=pltpu.CompilerParams(
            collective_id=identity, has_side_effects=True, vmem_limit_bytes=64 * 1024 * 1024 - 65536
        ),
        cost_estimate=pl.CostEstimate(flops=0, bytes_accessed=20 * moved, transcendentals=0),
    )(*operands)


PAIR = 256
TILE = 320


def experts_body(shards, groups, plans, shape, sizes, *refs):
    ids, routes, router, n_block, c_from, w_cut, w_pieces = refs[:7]
    n_from, y_to, d_to, g_to, g_back = refs[7:12]
    rows_n, rows_c, weights, picks, slot_w, slot_d, act_rows, gu_rows, y_rows, d_rows = refs[12:22]
    n_buf, c_buf, y_buf, d_buf, g_buf, n_sem, c_sem, w_sem, y_sem, d_sem, g_sem = refs[22:33]
    scratch = cut_refs(refs[33:], sizes)
    units, pairs, slots, tokens, extra = shape
    f32, bf16 = jnp.float32, jnp.bfloat16
    whole = 2 * slots
    chunk = weights.shape[1]
    width_all = n_block.shape[2]
    at = Place(shards, groups)
    at.greet(True, True)
    gather = Gather(at, True, n_block, n_from, *scratch[0])
    bring_weights = Exchange(at, plans[0], w_pieces, weights, *scratch[1])
    back_cut = Exchange(at, plans[1], g_buf, g_back, *scratch[2])

    def bring(p, slot):
        return (
            pltpu.make_async_copy(n_from.at[0, pl.ds(2 * p, 2)], n_buf.at[slot], n_sem.at[slot]),
            pltpu.make_async_copy(c_from.at[0, pl.ds(2 * p, 2)], c_buf.at[slot], c_sem.at[slot]),
        )

    split = units[-1][0]
    cut = pl.ds(split, weights.shape[2] - split)
    cut_copy = pltpu.make_async_copy(w_cut.at[:, :, cut], weights.at[:, :, cut], w_sem.at[0])
    cut_copy.start()
    marks = range(len(gather.events))
    for k in marks:
        gather.lines(k)
    bring_weights.start()
    for step in (Gather.sides, Gather.turns, Gather.finish):
        for k in marks:
            step(gather, k)
    for copy in bring(0, 0):
        copy.start()
    row = lax.broadcasted_iota(jnp.int32, (PAIR, PAIR), 0)
    column = lax.broadcasted_iota(jnp.int32, (PAIR, PAIR), 1)
    upto = ((row <= column) & (row // tokens == column // tokens)).astype(bf16)
    names = lax.broadcasted_iota(jnp.int32, (router.shape[0], PAIR), 0)
    lanes = lax.broadcasted_iota(jnp.int32, (1, PAIR), 1)
    places = lax.broadcasted_iota(jnp.int32, (whole, PAIR), 0)
    sixteen = lax.broadcasted_iota(jnp.int32, (16, PAIR), 0)

    def dispatch(p, _):
        slot = p % 2
        for copy in bring(p, slot):
            copy.wait()

        @pl.when(p + 1 < pairs)
        def _():
            for copy in bring(p + 1, 1 - slot):
                copy.start()

        n = n_buf[slot].reshape(PAIR, n_buf.shape[3])
        c = c_buf[slot].reshape(PAIR, c_buf.shape[3])
        named = routes[p]
        logits = lax.dot_general(
            router[...], n, (((1,), (1,)), ((), ())), preferred_element_type=f32
        )
        hit = names == named[0:1]
        for j in range(1, TOP):
            hit = hit | (names == named[j : j + 1])
        masked = jnp.where(hit, logits, MASKED)
        top = jnp.max(masked, axis=0, keepdims=True)
        raised = jnp.where(hit, jnp.exp(masked - top), 0.0)
        share = raised / jnp.sum(raised, axis=0, keepdims=True)
        hits = []
        for u in range(len(units)):
            mine = hit & (names == ids[u])
            hits.append(jnp.sum(jnp.where(mine, 1.0, 0.0), axis=0, keepdims=True))
        both = jnp.zeros((16, PAIR), f32)
        for u in range(len(units)):
            both = jnp.where(sixteen == u, hits[u], both)
        ranks = jnp.dot(both.astype(bf16), upto, preferred_element_type=f32)
        for u in range(len(units)):
            weight = jnp.sum(
                jnp.where(hit & (names == ids[u]), share, 0.0), axis=0, keepdims=True
            )
            place = jnp.where(
                hits[u] > 0.5,
                ranks[u : u + 1].astype(jnp.int32) - 1 + lanes // tokens * slots,
                -1,
            )
            pick = (places == place).astype(f32)
            here = pl.ds(pl.multiple_of(p * whole, 16), whole)
            slot_w[u, here] = jnp.sum(pick * weight, axis=1, keepdims=True)
            picks[p, u * whole : (u + 1) * whole] = pick.astype(bf16)
        here = pl.ds(pl.multiple_of(p * whole, 16), whole)
        sent_n = jnp.dot(picks[p], n, preferred_element_type=f32).astype(bf16)
        sent_c = jnp.dot(picks[p], c, preferred_element_type=f32).astype(bf16)
        for u in range(len(units)):
            rows_n[u, here] = sent_n[u * whole : (u + 1) * whole]
            rows_c[u, here] = sent_c[u * whole : (u + 1) * whole]
        return 0

    lax.fori_loop(0, pairs, dispatch, 0)
    turned = (((1,), (1,)), ((), ()))
    summed = (((0,), (0,)), ((), ()))
    deep = 2 * chunk

    def columns(start, width):
        return weights[:, :, pl.ds(start, width)].reshape(width_all, width)

    def products(u):
        start, width = units[u]
        first = start // 3
        held_a, held_g = pl.ds(first, width), pl.ds(2 * first, 2 * width)

        def tile(i, _):
            here = pl.ds(pl.multiple_of(i * TILE, 16), TILE)
            parts = jnp.dot(rows_n[u, here], columns(start, 2 * width), preferred_element_type=f32)
            down = columns(start + 2 * width, width)
            plain = jnp.dot(rows_c[u, here], down, preferred_element_type=f32)
            gate, up = parts[:, :width], parts[:, width:]
            sig = jax.nn.sigmoid(gate)
            act = gate * sig * up
            w = slot_w[u, here]
            slot_d[u, here] = jnp.sum(act * plain, axis=1, keepdims=True)
            act_w = (act * w).astype(bf16)
            da = plain * w
            d_gate = (da * up * sig * (1.0 + gate * (1.0 - sig))).astype(bf16)
            d_up = (da * gate * sig).astype(bf16)
            act_rows[here, held_a] = act_w
            gu_rows[here, pl.ds(2 * first, width)] = d_gate
            gu_rows[here, pl.ds(2 * first + width, width)] = d_up
            y_rows[u, here] = lax.dot_general(
                act_w, down, turned, preferred_element_type=f32
            ).astype(bf16)
            d_rows[u, here] = lax.dot_general(
                gu_rows[here, held_g],
                columns(start, 2 * width),
                turned,
                preferred_element_type=f32,
            ).astype(bf16)
            return 0

        lax.fori_loop(0, pairs * whole // TILE, tile, 0)

        def grads(i, _):
            here = pl.ds(pl.multiple_of(i * deep, deep), deep)
            value = lax.dot_general(
                rows_n[u, :, here], gu_rows[:, held_g], summed, preferred_element_type=f32
            )
            g_buf[pl.ds(2 * i, 2), :, pl.ds(start, 2 * width)] = value.astype(bf16).reshape(
                2, chunk, 2 * width
            )
            value = lax.dot_general(
                rows_c[u, :, here], act_rows[:, held_a], summed, preferred_element_type=f32
            )
            g_buf[pl.ds(2 * i, 2), :, pl.ds(start + 2 * width, width)] = value.astype(
                bf16
            ).reshape(2, chunk, width)
            return 0

        lax.fori_loop(0, width_all // deep, grads, 0)

    cut_copy.wait()
    products(len(units) - 1)
    back_cut.start()
    bring_weights.wait()
    for u in range(len(units) - 1):
        products(u)
    rest = pl.ds(0, split)
    g_copy = pltpu.make_async_copy(g_buf.at[:, :, rest], g_to.at[:, :, rest], g_sem.at[0])
    g_copy.start()

    def put(p, slot):
        return (
            pltpu.make_async_copy(y_buf.at[slot], y_to.at[pl.ds(2 * p, 2)], y_sem.at[slot]),
            pltpu.make_async_copy(d_buf.at[slot], d_to.at[pl.ds(2 * p, 2)], d_sem.at[slot]),
        )

    d_buf[:, :, tokens:] = jnp.zeros((2, 2, extra, d_buf.shape[3]), bf16)

    def combine(p, _):
        slot = p % 2

        @pl.when(p >= 2)
        def _():
            for copy in put(p - 2, slot):
                copy.wait()

        here = pl.ds(pl.multiple_of(p * whole, 16), whole)
        pick = picks[p]
        both = [y_rows[u, here] for u in range(len(units))]
        y = lax.dot_general(pick, jnp.concatenate(both), summed, preferred_element_type=f32)
        both = [d_rows[u, here] for u in range(len(units))]
        d = lax.dot_general(pick, jnp.concatenate(both), summed, preferred_element_type=f32)
        d_w = jnp.zeros((TOP, PAIR), f32)
        for u in range(len(units)):
            pick = picks[p, u * whole : (u + 1) * whole]
            back = jnp.sum(pick.astype(f32) * slot_d[u, here], axis=0, keepdims=True)
            d_w = d_w + jnp.where(routes[p] == ids[u], back, 0.0)
        high = d_w.astype(bf16)
        low = (d_w - high.astype(f32)).astype(bf16)
        y_buf[slot] = y.astype(bf16).reshape(y_buf.shape[1:])
        d_buf[slot, :, :tokens] = d.astype(bf16).reshape(2, tokens, d.shape[1])
        both = jnp.concatenate([high.astype(f32), low.astype(f32)], axis=0).astype(bf16)
        for i in range(2):
            d_buf[slot, i, tokens:, :tokens] = both[:, i * tokens : (i + 1) * tokens]
        for copy in put(p, slot):
            copy.start()
        return 0

    lax.fori_loop(0, pairs, combine, 0)
    for p in range(pairs - 2, pairs):
        for copy in put(p, p % 2):
            copy.wait()
    g_copy.wait()
    back_cut.wait()


def experts(
    ids, routes, router, n_block, c_all, w_cut, w_pieces, units, slots, extra, shards, groups, plans
):
    _, tokens, width = n_block.shape
    blocks = shards * groups
    pairs = blocks // 2
    rows = pairs * 2 * slots
    count = len(units)
    hidden = sum(w for _, w in units)
    bf16, f32 = jnp.bfloat16, jnp.float32
    owned = w_cut.shape
    dma = pltpu.SemaphoreType.DMA
    any_space, vmem = pl.BlockSpec(memory_space=pl.ANY), pl.BlockSpec(memory_space=pltpu.VMEM)
    scratch = [
        Gather.scratch(n_block, True, shards),
        Exchange.scratch(plans[0].block, bf16, plans[0].count, shards),
        Exchange.scratch(plans[1].block, bf16, plans[1].count, shards),
    ]
    return pl.pallas_call(
        functools.partial(
            experts_body,
            shards,
            groups,
            tuple(plans),
            (tuple(units), pairs, slots, tokens, extra),
            tuple(len(s) for s in scratch),
        ),
        out_shape=[
            jax.ShapeDtypeStruct((1, blocks, tokens, width), bf16),
            jax.ShapeDtypeStruct((blocks, tokens, width), bf16),
            jax.ShapeDtypeStruct((blocks, tokens + extra, width), bf16),
            jax.ShapeDtypeStruct(owned, bf16),
            jax.ShapeDtypeStruct(plans[1].shape, bf16),
        ],
        in_specs=[pl.BlockSpec(memory_space=pltpu.SMEM)] + [vmem] * 3 + [any_space] * 3,
        out_specs=[any_space] * 5,
        scratch_shapes=[
            pltpu.VMEM((count, rows, width), bf16),
            pltpu.VMEM((count, rows, width), bf16),
            pltpu.VMEM(owned, bf16),
            pltpu.VMEM((pairs, count * 2 * slots, PAIR), bf16),
            pltpu.VMEM((count, rows, 1), f32),
            pltpu.VMEM((count, rows, 1), f32),
            pltpu.VMEM((rows, hidden), bf16),
            pltpu.VMEM((rows, 2 * hidden), bf16),
            pltpu.VMEM((count, rows, width), bf16),
            pltpu.VMEM((count, rows, width), bf16),
            pltpu.VMEM((2, 2, tokens, width), bf16),
            pltpu.VMEM((2, 2, tokens, width), bf16),
            pltpu.VMEM((2, 2, tokens, width), bf16),
            pltpu.VMEM((2, 2, tokens + extra, width), bf16),
            pltpu.VMEM(owned, bf16),
            dma((2,)),
            dma((2,)),
            dma((1,)),
            dma((2,)),
            dma((2,)),
            dma((1,)),
        ]
        + [s for some in scratch for s in some],
        compiler_params=pltpu.CompilerParams(
            collective_id=2, has_side_effects=True, vmem_limit_bytes=67_000_000
        ),
        cost_estimate=pl.CostEstimate(
            flops=18 * rows * width * hidden,
            bytes_accessed=200 * 1024 * 1024,
            transcendentals=rows * hidden,
        ),
    )(ids, routes, router, n_block, c_all, w_cut, w_pieces)


def turned_lanes(values, cosine, sine):
    lane = lax.broadcasted_iota(jnp.int32, values.shape, 1)
    half = HEAD_SIZE // 2
    other = jnp.where(
        lane % HEAD_SIZE < half,
        pltpu.roll(values, LANES - half, 1),
        pltpu.roll(values, half, 1),
    )
    return values * cosine + other * sine


def causal(rows, columns, first_row):
    row = lax.broadcasted_iota(jnp.int32, (rows, columns), 0) + first_row
    return lax.broadcasted_iota(jnp.int32, (rows, columns), 1) <= row


NT = (((1,), (1,)), ((), ()))
TN = (((0,), (0,)), ((), ()))


def product(a, b, dims):
    return lax.dot_general(a, b, dims, preferred_element_type=jnp.float32)


def front_body(shards, groups, plans, sizes, *refs):
    x, small, routes, far, w_output, cosine, sine, qkv_cut, experts_cut = refs[:9]
    small_all, routes_all, far_all, qkv_own, piece, normed, turned, log_sums, mixed = refs[9:18]
    attended, x_all, parts, qkv_quarter = refs[18:22]
    scratch = cut_refs(refs[22:], sizes)
    f32, bf16 = jnp.float32, jnp.bfloat16
    at = Place(shards, groups)
    at.greet(True, True, True)
    gathers = [
        Gather(at, False, x, x_all, *scratch[0]),
        Gather(at, False, small, small_all, *scratch[1]),
        Gather(at, True, routes, routes_all, *scratch[2]),
    ]
    quarter_cut = quarter(qkv_cut, at.group, qkv_quarter.shape[1], 1)
    qkv_move = Exchange(at, plans[0], quarter_cut, qkv_quarter, *scratch[3])
    qkv_spread = Spread(at, qkv_quarter, qkv_own, 1, *scratch[7])
    beside = Gather(at, True, far, far_all, *scratch[8])
    piece_move = Exchange(at, plans[1], experts_cut, piece, *scratch[4])
    sums = [
        Reduce(at, False, parts.at[pl.ds(j, 1)], attended.at[pl.ds(j, 1)], *scratch[5 + j])
        for j in range(2)
    ]
    marks = range(len(gathers[0].events))
    for k in marks:
        for g in gathers:
            g.lines(k)
        if k == 0:
            qkv_move.start()
    beside.lines(0)
    qkv_move.wait()
    qkv_spread.start()
    for step in (Gather.sides, Gather.turns, Gather.finish):
        for k in marks:
            for g in gathers:
                step(g, k)
    qkv_spread.wait()

    width = x.shape[2]
    length = shards * DEVICE_TOKENS
    tile = 256
    at_lane = lax.broadcasted_iota(jnp.int32, (16, LANES), 1)
    at_row = lax.broadcasted_iota(jnp.int32, (16, LANES), 0)
    one_hot = ((at_lane == E) & (at_row == 0)).astype(bf16)
    gain = product(one_hot, small_all[0].reshape(width, LANES), NT)[0:1]
    per = length // tile

    def project(t):
        j, i = divmod(t, per)
        count = tile // DEVICE_TOKENS
        rows = x_all[j, i * count : (i + 1) * count].reshape(tile, width).astype(f32)
        rate = lax.rsqrt(jnp.mean(rows * rows, axis=-1, keepdims=True) + EPSILON)
        n = (rows * rate * gain).astype(bf16)
        here = slice(i * tile, (i + 1) * tile)
        normed[j, here] = n
        qkv = jnp.dot(n, qkv_own[...].reshape(width, -1), preferred_element_type=f32)
        for lanes in (0, LANES):
            turned[j, here, lanes : lanes + LANES] = turned_lanes(
                qkv[:, lanes : lanes + LANES], cosine[here], sine[here]
            ).astype(bf16)
        turned[j, here, 2 * LANES :] = qkv[:, 2 * LANES :].astype(bf16)

    waiting = list(marks)[1:]
    for t in range(2 * per):
        project(t)
        for k in waiting[:2]:
            beside.lines(k)
        waiting = waiting[2:]
    for k in waiting:
        beside.lines(k)
    piece_move.start()
    waiting = list(marks)
    ratio = QUERY_HEADS // KEY_VALUE_HEADS
    scale = 1.0 / HEAD_SIZE
    for j in range(2):
        key = turned[j, :, ratio * HEAD_SIZE : (ratio + 1) * HEAD_SIZE]
        value = turned[j, :, (ratio + 1) * HEAD_SIZE :]
        for i in range(per):
            here = slice(i * tile, (i + 1) * tile)
            seen = (i + 1) * tile
            outs, logs = [], []
            for h in range(ratio):
                query = turned[j, here, h * HEAD_SIZE : (h + 1) * HEAD_SIZE]
                scores = product(query, key[:seen], NT) * scale
                scores = jnp.where(causal(tile, seen, i * tile), scores, MASKED)
                top = jnp.max(scores, axis=-1, keepdims=True)
                raised = jnp.exp(scores - top)
                total = jnp.sum(raised, axis=-1, keepdims=True)
                logs.append(top + jnp.log(total))
                probs = (raised * (1.0 / total)).astype(bf16)
                outs.append(jnp.dot(probs, value[:seen], preferred_element_type=f32))
            mixed[j, here] = jnp.concatenate(outs, axis=1).astype(bf16)
            for h in range(ratio):
                log_sums[j, here, h : h + 1] = logs[h]
            out = jnp.dot(mixed[j, here], w_output[...], preferred_element_type=f32).astype(bf16)
            count = tile // DEVICE_TOKENS
            parts[j, i * count : (i + 1) * count] = out.reshape(count, DEVICE_TOKENS, width)
            for k in waiting[:2]:
                beside.sides(k)
            waiting = waiting[2:]
        sums[j].begin()
    for k in waiting:
        beside.sides(k)
    for q in sums[0].order:
        for s in sums:
            s.lines(q)
    for k in marks:
        beside.turns(k)
    for s in sums:
        s.finish()
    for k in marks:
        beside.finish(k)
    piece_move.wait()


def front(
    x, small, routes, far, w_output, cosine, sine, qkv_cut, experts_cut, shards, groups, plan
):
    f32, bf16 = jnp.float32, jnp.bfloat16
    sequences, rows, width = x.shape
    length = shards * rows
    own_rows, columns = qkv_cut.shape[1:]
    quarter_shape = (shards, own_rows // groups, columns)
    plans = (Rows(jax.ShapeDtypeStruct(quarter_shape, bf16)), plan)
    block = jax.ShapeDtypeStruct((1, shards, rows, width), bf16)
    scratch = [
        Gather.scratch(x, False, shards),
        Gather.scratch(small, False, shards),
        Gather.scratch(routes, True, shards),
        Exchange.scratch(plans[0].block, bf16, plans[0].count, shards),
        Exchange.scratch(plans[1].block, bf16, plans[1].count, shards),
        Reduce.scratch(block, False, shards),
        Reduce.scratch(block, False, shards),
        Spread.scratch(),
        Gather.scratch(far, True, shards),
    ]
    any_space, vmem = pl.BlockSpec(memory_space=pl.ANY), pl.BlockSpec(memory_space=pltpu.VMEM)
    queries = w_output.shape[0]
    return pl.pallas_call(
        functools.partial(
            front_body, shards, groups, plans, tuple(len(s) for s in scratch)
        ),
        out_shape=[
            jax.ShapeDtypeStruct((1, shards) + small.shape[1:], bf16),
            jax.ShapeDtypeStruct((1, shards * groups) + routes.shape[1:], routes.dtype),
            jax.ShapeDtypeStruct((1, shards * groups) + far.shape[1:], bf16),
            jax.ShapeDtypeStruct(qkv_cut.shape, bf16),
            jax.ShapeDtypeStruct(plan.shape, bf16),
            jax.ShapeDtypeStruct((sequences, length, width), bf16),
            jax.ShapeDtypeStruct((sequences, length, columns), bf16),
            jax.ShapeDtypeStruct((sequences, length, LANES), f32),
            jax.ShapeDtypeStruct((sequences, length, queries), bf16),
            jax.ShapeDtypeStruct((sequences, rows, width), f32),
        ],
        in_specs=[vmem] * 7 + [any_space] * 2,
        out_specs=[vmem, any_space, any_space, vmem, any_space, vmem, vmem, vmem, vmem, vmem],
        scratch_shapes=[
            pltpu.VMEM((sequences, shards, rows, width), bf16),
            pltpu.VMEM((sequences, shards, rows, width), bf16),
            pltpu.VMEM(quarter_shape, bf16),
        ]
        + [s for some in scratch for s in some],
        compiler_params=pltpu.CompilerParams(
            collective_id=0, has_side_effects=True, vmem_limit_bytes=60 * 1024 * 1024
        ),
        cost_estimate=pl.CostEstimate(
            flops=4 * 10**9, bytes_accessed=100 * 10**6, transcendentals=3 * 10**6
        ),
    )(x, small, routes, far, w_output, cosine, sine, qkv_cut, experts_cut)


def rear_body(shards, groups, plans, sizes, *refs):
    dh, w_output, normed, qkv_own, turned, log_sums, mixed, cosine, sine = refs[:9]
    grad_small, grads, _ = refs[9:12]
    d_normed, small_line, qkv_sum, small_sum, output_sum, experts_out = refs[12:18]
    dh_all, parts, d_qkv, d_keys, d_values, grad_qkv, swapped, grad_output = refs[18:26]
    scratch = cut_refs(refs[26:], sizes)
    f32, bf16 = jnp.float32, jnp.bfloat16
    at = Place(shards, groups)
    at.greet(True, True, True)
    gather = Gather(at, False, dh, dh_all, *scratch[0])
    experts_moves = [
        Exchange(at, plans[i], grads, experts_out, *scratch[(1, 12)[i]])
        for i in range(len(plans) - 1)
    ]
    sums = [
        Reduce(at, False, parts.at[pl.ds(j, 1)], d_normed.at[pl.ds(j, 1)], *scratch[3 + j])
        for j in range(2)
    ]
    small = Reduce(at, False, grad_small, small_line, *scratch[5])
    of_qkv = Across(at, grad_qkv, 1, *scratch[6])
    of_small = Across(at, small_line, 0, *scratch[7])
    of_output = Across(at, grad_output, 0, *scratch[8])
    qkv_move = Exchange(at, plans[-1], of_qkv.mine, swapped, *scratch[2])
    spreads = [
        Spread(at, swapped, qkv_sum, 1, *scratch[9]),
        Spread(at, of_small.mine, small_sum, 0, *scratch[10]),
        Spread(at, of_output.mine, output_sum, 0, *scratch[11]),
    ]
    small.begin()
    marks = range(len(gather.events))
    for k in marks:
        gather.lines(k)
    for q in small.order:
        small.lines(q)
    experts_moves[0].start()
    small.finish()
    of_small.start()
    for k in marks:
        gather.finish(k)

    width = dh.shape[2]
    length = shards * DEVICE_TOKENS
    tile = 256
    ratio = QUERY_HEADS // KEY_VALUE_HEADS
    scale = 1.0 / HEAD_SIZE
    total = jnp.zeros((ratio * HEAD_SIZE, width), f32)
    for j in range(2):
        total = total + product(mixed[j], dh_all[j].reshape(length, width), TN)
    grad_output[...] = total.astype(bf16).reshape(grad_output.shape)
    of_output.start()
    for j in range(2):
        d_mixed = product(dh_all[j].reshape(length, width), w_output[...], NT).astype(bf16)
        key = turned[j, :, ratio * HEAD_SIZE : (ratio + 1) * HEAD_SIZE]
        value = turned[j, :, (ratio + 1) * HEAD_SIZE :]
        d_keys[...] = jnp.zeros_like(d_keys)
        d_values[...] = jnp.zeros_like(d_values)
        d_queries = []
        for i in range(length // tile):
            here = slice(i * tile, (i + 1) * tile)
            seen = (i + 1) * tile
            row = []
            for h in range(ratio):
                head = slice(h * HEAD_SIZE, (h + 1) * HEAD_SIZE)
                query = turned[j, here, head]
                d_out = d_mixed[here, head]
                scores = product(query, key[:seen], NT) * scale
                scores = jnp.where(causal(tile, seen, i * tile), scores, MASKED)
                probs = jnp.exp(scores - log_sums[j, here, h : h + 1])
                delta = jnp.sum(
                    d_out.astype(f32) * mixed[j, here, head].astype(f32), axis=-1, keepdims=True
                )
                d_scores = probs * (product(d_out, value[:seen], NT) - delta)
                d_scores = d_scores.astype(bf16)
                row.append(jnp.dot(d_scores, key[:seen], preferred_element_type=f32) * scale)
                d_keys[:seen] = d_keys[:seen] + product(d_scores, query, TN) * scale
                d_values[:seen] = d_values[:seen] + product(probs.astype(bf16), d_out, TN)
            d_queries.append(jnp.concatenate(row, axis=1))
        d_query = jnp.concatenate(d_queries, axis=0)
        last = jnp.concatenate([d_query[:, LANES:], d_keys[...]], axis=1)
        d_qkv[j, :, :LANES] = turned_lanes(d_query[:, :LANES], cosine[...], -sine[...]).astype(bf16)
        d_qkv[j, :, LANES : 2 * LANES] = turned_lanes(last, cosine[...], -sine[...]).astype(bf16)
        d_qkv[j, :, 2 * LANES :] = d_values[...].astype(bf16)
        out = product(d_qkv[j], qkv_own[...].reshape(width, -1), NT).astype(bf16)
        parts[j] = out.reshape(shards, DEVICE_TOKENS, width)
        sums[j].begin()
    cut = 2 * grad_qkv.shape[1]
    for i in range(width // cut):
        here = slice(i * cut, (i + 1) * cut)
        value = product(normed[0, :, here], d_qkv[0], TN) + product(
            normed[1, :, here], d_qkv[1], TN
        )
        grad_qkv[2 * i : 2 * i + 2] = value.astype(bf16).reshape(2, cut // 2, -1)
    of_qkv.start()
    order = sums[0].order
    for step, q in enumerate(order):
        for s in sums:
            s.lines(q)
        if step == min(1, len(order) - 1):
            of_small.add()
            spreads[1].start()
            of_output.add()
            spreads[2].start()
            of_qkv.add()
            qkv_move.start()
    for m in experts_moves[1:]:
        m.start()
    qkv_move.wait()
    spreads[0].start()
    for s in sums:
        s.finish()
    for s in spreads:
        s.wait()
    for m in experts_moves:
        m.wait()


def rear(
    dh, w_output, normed, qkv_own, turned, log_sums, mixed, cosine, sine, grad_small, grads, held,
    shards, groups, plans,
):
    f32, bf16 = jnp.float32, jnp.bfloat16
    sequences, rows, width = dh.shape
    length = shards * rows
    queries = w_output.shape[0]
    block = jax.ShapeDtypeStruct((1, shards, rows, width), bf16)
    small_shape = grad_small.shape[:1] + grad_small.shape[2:]
    output_shape = (groups, queries // groups, width)
    own_rows, columns = qkv_own.shape[1:]
    quarter_shape = (shards, own_rows // groups, columns)
    qkv_plan = Rows(jax.ShapeDtypeStruct(quarter_shape, bf16))
    scratch = [
        Gather.scratch(dh, False, shards),
        Exchange.scratch(plans[0].block, bf16, plans[0].count, shards),
        Exchange.scratch(qkv_plan.block, bf16, qkv_plan.count, shards),
        Reduce.scratch(block, False, shards),
        Reduce.scratch(block, False, shards),
        Reduce.scratch(grad_small, False, shards),
        Across.scratch(qkv_own.shape, bf16, 1),
        Across.scratch(small_shape, f32),
        Across.scratch(output_shape, bf16),
        Spread.scratch(),
        Spread.scratch(),
        Spread.scratch(),
    ] + [Exchange.scratch(p.block, bf16, p.count, shards) for p in plans[1:]]
    any_space, vmem = pl.BlockSpec(memory_space=pl.ANY), pl.BlockSpec(memory_space=pltpu.VMEM)
    return pl.pallas_call(
        functools.partial(
            rear_body, shards, groups, (*plans, qkv_plan), tuple(len(s) for s in scratch)
        ),
        out_shape=[
            jax.ShapeDtypeStruct(dh.shape, f32),
            jax.ShapeDtypeStruct(small_shape, f32),
            jax.ShapeDtypeStruct(qkv_own.shape, bf16),
            jax.ShapeDtypeStruct(small_shape, f32),
            jax.ShapeDtypeStruct(output_shape, bf16),
            jax.ShapeDtypeStruct(held.shape, bf16),
        ],
        in_specs=[vmem] * 9 + [any_space] * 3,
        out_specs=[vmem] * 2 + [any_space] * 4,
        scratch_shapes=[
            pltpu.VMEM((sequences, shards, rows, width), bf16),
            pltpu.VMEM((sequences, shards, rows, width), bf16),
            pltpu.VMEM(turned.shape, bf16),
            pltpu.VMEM((length, HEAD_SIZE), f32),
            pltpu.VMEM((length, HEAD_SIZE), f32),
            pltpu.VMEM(qkv_own.shape, bf16),
            pltpu.VMEM(quarter_shape, bf16),
            pltpu.VMEM(output_shape, bf16),
        ]
        + [s for some in scratch for s in some],
        input_output_aliases={11: 5},
        compiler_params=pltpu.CompilerParams(
            collective_id=5, has_side_effects=True, vmem_limit_bytes=64 * 1024 * 1024 - 65536
        ),
        cost_estimate=pl.CostEstimate(
            flops=8 * 10**9, bytes_accessed=100 * 10**6, transcendentals=3 * 10**6
        ),
    )(
        dh, w_output, normed, qkv_own, turned, log_sums, mixed, cosine, sine, grad_small, grads,
        held,
    )


def local(
    inputs,
    cotangent,
    routes,
    attn_gain,
    w_query,
    key_matrix,
    value_matrix,
    w_output,
    moe_gain,
    w_router,
    w_experts,
):
    f32, bf16 = jnp.float32, jnp.bfloat16
    shards, groups = lax.axis_size("shard"), lax.axis_size("expert")
    shard, group = lax.axis_index("shard"), lax.axis_index("expert")
    tokens = inputs.shape[0]
    own_rows = attn_gain.shape[0]
    sequences = tokens // DEVICE_TOKENS
    length = shards * DEVICE_TOKENS
    experts_here = E // groups
    blocks = groups * shards
    ratio = QUERY_HEADS // KEY_VALUE_HEADS
    query_width, key_width = ratio * HEAD_SIZE, HEAD_SIZE

    small = jnp.concatenate([w_router, attn_gain[:, None], moe_gain[:, None]], axis=1)
    small = jnp.pad(small, ((0, 0), (0, LANES - E - 2)))
    qkv_cut = jnp.transpose(
        jnp.concatenate(
            [
                w_query.reshape(own_rows, shards, query_width),
                key_matrix.reshape(own_rows, shards, key_width),
                value_matrix.reshape(own_rows, shards, key_width),
            ],
            axis=2,
        ),
        (1, 0, 2),
    )
    experts_cut = jnp.transpose(w_experts, (1, 0, 2))
    cosine, sine = angle_tables(jnp.arange(length, dtype=f32))
    twice = LANES // HEAD_SIZE
    cosine = jnp.tile(cosine, (1, 2 * twice))
    sine = jnp.tile(jnp.concatenate([-sine, sine], axis=1), (1, twice))
    (
        small_all,
        routes_all,
        c_all,
        qkv_own,
        cut_own,
        normed,
        turned,
        log_sums,
        mixed,
        attended,
    ) = front(
        inputs.reshape(sequences, DEVICE_TOKENS, MODEL_WIDTH),
        small[None],
        jnp.transpose(routes)[None],
        cotangent[None],
        w_output,
        cosine,
        sine,
        qkv_cut,
        experts_cut,
        shards,
        groups,
        Experts(experts_cut.shape, shards, experts_here, False, (0, 0), True),
    )
    small = small_all.reshape(MODEL_WIDTH, LANES)
    router_pad = jnp.where(jnp.arange(LANES) < E, small, 0)
    router, gain_one, gain_two = small[:, :E], small[:, E].astype(f32), small[:, E + 1].astype(f32)
    inputs_wide = inputs.astype(f32)
    h_one = inputs_wide + attended.reshape(tokens, MODEL_WIDTH)
    r_two = lax.rsqrt(jnp.mean(h_one * h_one, axis=-1, keepdims=True) + EPSILON)
    z_two = h_one * r_two
    n_two = (z_two * gain_two).astype(bf16)

    whole, extra = divmod(experts_here, shards)
    cuts = shards // extra
    owned = [(group * experts_here + shard * whole + i, i * 3 * FF, FF) for i in range(whole)]
    owned.append(
        (group * experts_here + whole * shards + shard // cuts, whole * 3 * FF, FF // cuts)
    )
    slots = -(-CAP // 8) * 8
    routes_pairs = jnp.transpose(
        routes_all.reshape(blocks // 2, 2, TOP, tokens), (0, 2, 1, 3)
    ).reshape(blocks // 2, TOP, 2 * tokens)
    _, o_sums, d_sums, grads, grad_experts = experts(
        jnp.stack([expert for expert, _, _ in owned]).astype(jnp.int32),
        routes_pairs,
        jnp.transpose(router_pad)[: -(-E // 16) * 16],
        n_two[None],
        c_all,
        cut_own,
        experts_cut,
        [(start, width) for _, start, width in owned],
        slots,
        2 * TOP,
        shards,
        groups,
        [
            Experts(experts_cut.shape, shards, experts_here, False, (0, 6), False),
            Experts(cut_own.shape, shards, experts_here, True, (0, 0), True),
        ],
    )
    back, moe_sum, grad_experts = reduced(
        [d_sums[None], o_sums[None]],
        (True, True),
        shards,
        groups,
        3,
        [grads],
        [Experts(grads.shape, shards, experts_here, True, (0, 4), False)],
        [grad_experts],
    )
    back = back[0]
    outputs = (h_one + moe_sum[0]).astype(bf16)

    logits = jnp.dot(n_two, router, preferred_element_type=f32)
    picks = (routes[:, :, None] == jnp.arange(E, dtype=jnp.int32)).astype(f32)
    weights = jax.nn.softmax(jnp.sum(picks * logits[:, None, :], axis=-1), axis=-1)
    carried = back[tokens:, :tokens]
    d_weights = jnp.transpose(carried[:TOP] + carried[TOP:])
    d_chosen = weights * (d_weights - jnp.sum(weights * d_weights, axis=-1, keepdims=True))
    d_logits = jnp.sum(picks * d_chosen[:, :, None], axis=1).astype(bf16)
    grad_router = jnp.einsum("td,te->de", n_two, d_logits, preferred_element_type=f32)
    d_n_two = jnp.einsum("te,de->td", d_logits, router, preferred_element_type=f32)
    d_n_two = d_n_two + back[:tokens]
    grad_gain_two = jnp.sum(d_n_two * z_two, axis=0)
    dz_two = d_n_two * gain_two
    dh_one = cotangent.astype(f32) + r_two * (
        dz_two - z_two * jnp.mean(dz_two * z_two, axis=-1, keepdims=True)
    )
    grad_small = jnp.concatenate([grad_router, grad_gain_two[:, None]], axis=1).astype(bf16)
    grad_small = jnp.pad(grad_small, ((0, 0), (0, LANES - E - 1)))
    grad_small = jnp.transpose(
        grad_small.reshape(shards, groups, own_rows // groups, LANES), (1, 0, 2, 3)
    )
    dh_rows = dh_one.astype(bf16).reshape(sequences, DEVICE_TOKENS, MODEL_WIDTH)
    d_n_one, _, grad_qkv, grad_small, grad_output, grad_experts = rear(
        dh_rows,
        w_output,
        normed,
        qkv_own,
        turned,
        log_sums,
        mixed,
        cosine,
        sine,
        grad_small,
        grads,
        grad_experts,
        shards,
        groups,
        [Experts(grads.shape, shards, experts_here, True, (4, 6), False)],
    )
    grad_output = grad_output.reshape(own_rows, MODEL_WIDTH).astype(f32)
    grad_small = grad_small.reshape(own_rows, LANES)
    grad_experts = jnp.transpose(grad_experts, (1, 0, 2)).astype(f32)

    def columns(start, width):
        part = jnp.transpose(grad_qkv[:, :, start : start + width], (1, 0, 2))
        return part.reshape(own_rows, shards * width).astype(f32)

    grad_query = columns(0, query_width)
    grad_key = columns(query_width, key_width)
    grad_value = columns(query_width + key_width, key_width)
    grad_gain_one = (
        jnp.sum(grad_query * w_query.astype(f32), axis=1)
        + jnp.sum(grad_key * key_matrix.astype(f32), axis=1)
        + jnp.sum(grad_value * value_matrix.astype(f32), axis=1)
    ) / attn_gain.astype(f32)
    r_one = lax.rsqrt(jnp.mean(inputs_wide * inputs_wide, axis=-1, keepdims=True) + EPSILON)
    z_one = inputs_wide * r_one
    dz_one = d_n_one.reshape(tokens, MODEL_WIDTH) * gain_one
    grad_inputs = dh_one + r_one * (
        dz_one - z_one * jnp.mean(dz_one * z_one, axis=-1, keepdims=True)
    )
    return (
        outputs,
        grad_inputs,
        grad_gain_one,
        grad_query,
        grad_key,
        grad_value,
        grad_output,
        grad_small[:, E],
        grad_small[:, :E],
        grad_experts,
    )


def solution(mesh):
    return jax.shard_map(
        local if fits(mesh.shape["shard"], mesh.shape["expert"]) else general,
        mesh=mesh,
        in_specs=(
            P(("expert", "shard"), None),
            P(("expert", "shard"), None),
            P(("expert", "shard"), None),
            P("shard"),
            P("shard", None),
            P("shard", None),
            P("shard", None),
            P("shard", None),
            P("shard"),
            P("shard", None),
            P("shard", "expert", None),
        ),
        out_specs=(
            P(("expert", "shard"), None),
            P(("expert", "shard"), None),
            P("shard"),
            P("shard", None),
            P("shard", None),
            P("shard", None),
            P("shard", None),
            P("shard"),
            P("shard", None),
            P("shard", "expert", None),
        ),
        check_vma=False,
    )
```
